32 devices in a mesh: grp: 2 (over x), gx: 4 (over z), gy: 4 (over y, core).
Axes of the slice: x: 2, y: 2, z: 4, core: 2. Of those that a mesh axis runs over, the one named last changes fastest.
Arguments:
- state: float32 [2, 3, 144, 192, 90], P('grp', None, 'gx', 'gy'), may hold values from -6 to 6
- courant: float32 [2, 144, 192, 90], P('grp', 'gx', 'gy'), may hold values from 0.15 to 0.5
- vert_inverse: float32 [2, 90, 90], P('grp'), may hold values from -0.1 to 0.65, as said below
- interp_index: int32 [144, 192, 4], P('gx', 'gy'), may hold values from 0 to 8
- interp_weight: float32 [144, 192, 4], P('gx', 'gy'), may hold values from 0.2 to 1
- restrict_index: int32 [48, 64, 9], P('gx', 'gy'), may hold values from 0 to 8
- restrict_weight: float32 [48, 64, 9], P('gx', 'gy'), may hold values from 0.2 to 1
Outputs:
- new_state: float32 [2, 3, 144, 192, 90], P('grp', None, 'gx', 'gy')
The draws below stay inside these ranges and needn't reach their ends.
Inputs may be any that keep to these rules, and one draw needn't show every extreme that they name: `vert_inverse`: each matrix's diagonal lies in 0.5 to 0.65, its neighbours on the diagonal beside it in 0.05 to 0.12, the rest is small.
All inputs are finite; a program needn't handle non-finite values.
Results may differ from the reference program's by a relative error of at most 0.0001.
Values sent between devices are 32-bit elements; how exact they have to be, the bound alone decides.
A program may use at most 128 MiB of HBM per device.

```python
import math
import jax
import jax.numpy as jnp
from jax import lax

LEV = 90
SUBS = 4
BAND = 5
NK = 9
NX = 144
NY = 192
FX = 48
FY = 64
OX = 72
OY = 96


def draw_vert_inverse(key, part):
    keys = jax.random.split(key, 3)
    diagonal = jax.random.uniform(keys[0], (2, LEV), jnp.float32, 0.5, 0.65)
    beside = jax.random.uniform(keys[1], (2, LEV - 1), jnp.float32, 0.05, 0.12)
    beside = jnp.pad(beside, ((0, 0), (0, 1)))
    upper = beside[:, :, None] * jnp.eye(LEV, k=1, dtype=jnp.float32)[None]
    noise = jax.random.normal(keys[2], (2, LEV, LEV), jnp.float32) * (0.01 / jnp.sqrt(1.0 * LEV))
    noise = jnp.clip(noise, -0.02, 0.02)
    matrix = diagonal[:, :, None] * jnp.eye(LEV, dtype=jnp.float32)[None] + upper + jnp.swapaxes(upper, 1, 2) + noise
    return matrix.astype(jnp.float32)


def plant(array, key, least, largest):
    spot = [jax.random.randint(jax.random.fold_in(key, axis), (), 0, length) for axis, length in enumerate(array.shape)]
    longest = array.shape.index(max(array.shape))
    neighbour = spot[:longest] + [(spot[longest] + 1) % array.shape[longest]] + spot[longest + 1:]
    return array.at[tuple(spot)].set(least).at[tuple(neighbour)].set(largest)


def level_of(own_key, extent, cuts, smallest, largest):
    loudness, own = 1.0, jax.random.fold_in(own_key, 6)
    for dim, blocks in cuts:
        steps = jnp.exp(jax.random.uniform(jax.random.fold_in(own, dim), (blocks,), jnp.float32, smallest / len(cuts), largest / len(cuts)))
        loudness = loudness * jnp.repeat(steps, extent[dim] // blocks).reshape([-1 if axis == dim else 1 for axis in range(len(extent))])
    return loudness


def bell_draw(stream_key, shape, deviation, reach, cuts=(), kind=jnp.bfloat16):
    values = deviation * jax.random.normal(stream_key, shape, jnp.float32)
    if cuts:
        values = values * level_of(stream_key, shape, cuts, -0.22, 0.18)
    return jnp.clip(values, -reach, reach).astype(kind)


def setup_inputs(seed: int = 0) -> dict:
    key_of = jax.random.split(jax.random.key(seed), 8)
    state = bell_draw(key_of[0], (2, 3, NX, NY, LEV), 1.0, 6.0, ((0, 2), (2, 4), (3, 4)), jnp.float32)
    courant = jnp.clip(jnp.exp(math.log(0.5) - 1.2039728 * jax.random.uniform(key_of[1], (2, NX, NY, LEV), jnp.float32) ** level_of(key_of[1], (2, NX, NY, LEV), ((0, 2), (1, 4), (2, 4)), -0.2, 0.2)), 0.15, 0.5)
    vert_inverse = draw_vert_inverse(jax.random.fold_in(key_of[7], 71), 0)
    interp_index = plant(jax.random.randint(key_of[3], (NX, NY, 4), 0, 9), jax.random.fold_in(key_of[3], 1), 0, 8).astype(jnp.int32)
    interp_weight = jnp.clip(0.2 + 0.8 * jax.random.uniform(key_of[4], (NX, NY, 4), jnp.float32) ** level_of(key_of[4], (NX, NY, 4), ((0, 4), (1, 4)), -0.2, 0.2), 0.2, 1.0)
    restrict_index = plant(jax.random.randint(key_of[5], (FX, FY, NK), 0, 9), jax.random.fold_in(key_of[5], 1), 0, 8).astype(jnp.int32)
    restrict_weight = jnp.clip(0.2 + 0.8 * jax.random.uniform(key_of[6], (FX, FY, NK), jnp.float32) ** level_of(key_of[6], (FX, FY, NK), ((0, 4), (1, 4)), -0.2, 0.2), 0.2, 1.0)
    return dict(state=state, courant=courant, vert_inverse=vert_inverse, interp_index=interp_index, interp_weight=interp_weight, restrict_index=restrict_index, restrict_weight=restrict_weight)


FEEDBACK = 0.5


def slope_x(field):
    return 0.5 * (field[..., 2:, 1:-1, :] - field[..., :-2, 1:-1, :])


def slope_y(field):
    return 0.5 * (field[..., 1:-1, 2:, :] - field[..., 1:-1, :-2, :])


def padded(field):
    return jnp.pad(field, ((1, 1), (1, 1), (0, 0)))


def vertical(pressure, inverse):
    return jnp.einsum("xyk,kl->xyl", pressure, inverse, precision=lax.Precision.HIGHEST)


def substeps(fields, speed, inverse):
    pressure, wind_x, wind_y = fields[0], fields[1], fields[2]
    running = jnp.zeros_like(fields)
    for substep in range(SUBS):
        rimmed = padded(pressure)
        wind_x = wind_x - speed * slope_x(rimmed)
        wind_y = wind_y - speed * slope_y(rimmed)
        pressure = pressure - speed * (slope_x(padded(wind_x)) + slope_y(padded(wind_y)))
        pressure = vertical(pressure, inverse)
        running = running + jnp.stack([pressure, wind_x, wind_y])
    return jnp.stack([pressure, wind_x, wind_y]), running / SUBS


def weighted_sum(source, child_rows, child_cols, weight):
    shares = weight / jnp.sum(weight, axis=-1, keepdims=True)
    summed = jnp.zeros((source.shape[0],) + child_rows.shape[:2] + (source.shape[-1],), jnp.float32)
    for term in range(child_rows.shape[2]):
        summed = summed + shares[None, :, :, term, None] * source[:, child_rows[:, :, term], child_cols[:, :, term], :]
    return summed


def reference(state, courant, vert_inverse, interp_index, interp_weight, restrict_index, restrict_weight):
    parent_end, parent_mean = substeps(state[0], courant[0], vert_inverse[0])
    nest_end, nest_mean = substeps(state[1], courant[1], vert_inverse[1])
    fine_x = jnp.arange(NX, dtype=jnp.int32)
    fine_y = jnp.arange(NY, dtype=jnp.int32)
    source_x = jnp.clip((OX - 1 + fine_x // 3)[:, None, None] + interp_index // 3, OX, OX + FX - 1).astype(jnp.int32)
    source_y = jnp.clip((OY - 1 + fine_y // 3)[None, :, None] + interp_index % 3, OY, OY + FY - 1).astype(jnp.int32)
    boundary = weighted_sum(parent_end, source_x, source_y, interp_weight)
    coarse_x = jnp.arange(FX, dtype=jnp.int32)
    coarse_y = jnp.arange(FY, dtype=jnp.int32)
    child_x = (3 * coarse_x)[:, None, None] + restrict_index // 3
    child_y = (3 * coarse_y)[None, :, None] + restrict_index % 3
    footprint = weighted_sum(nest_mean, child_x, child_y, restrict_weight)
    restricted = jnp.zeros_like(parent_end).at[:, OX:OX + FX, OY:OY + FY, :].set(footprint)
    column_x = fine_x[:, None]
    column_y = fine_y[None, :]
    edge_depth = jnp.minimum(jnp.minimum(column_x, NX - 1 - column_x), jnp.minimum(column_y, NY - 1 - column_y)).astype(jnp.float32)
    relax_weight = jnp.maximum(1.0 - edge_depth / BAND, 0.0)[None, :, :, None]
    nest_new = nest_end + relax_weight * (boundary - nest_end)
    region = ((column_x >= OX) & (column_x < OX + FX) & (column_y >= OY) & (column_y < OY + FY)).astype(jnp.float32)[None, :, :, None]
    parent_new = parent_end + FEEDBACK * region * (restricted - parent_end)
    return jnp.stack([parent_new, nest_new])
```

```python
import functools

import jax
import jax.numpy as jnp
from jax import lax
from jax.experimental import pallas as pl
from jax.experimental.pallas import tpu as pltpu
from jax.sharding import PartitionSpec as P

SUBS = 4
BAND = 5
FEEDBACK = 0.5
MESH = pl.DeviceIdType.MESH
F32 = jnp.float32
XB, YB = 2, 8


def split(a):
    high = a.astype(jnp.bfloat16)
    return high, (a - high.astype(F32)).astype(jnp.bfloat16)


def dot(a, b):
    return jnp.dot(a, b, preferred_element_type=F32)


def dot3(a, b_high, b_low):
    a_high, a_low = split(a)
    return dot(a_high, b_high) + (dot(a_low, b_high) + dot(a_high, b_low))


def third(t):
    return (t * 11) >> 5


def kernel(
    cx, cy,
    state, courant, *rest,
):
    small, (
    S,
    C, inverse, iidx, iwgt, ridx, rwgt, mean, wr, wx, wy, sx0, sy0, rx0, ry0, sx, sy, rx, ry, rst, fb, xstrip, ystrip,
    load_sem, halo_send, halo_recv, strip_send, strip_recv, fb_send, fb_recv,
    q0, q1, q2, q3, q_send, q_recv,
    ) = rest[:5], rest[5:]
    g, a, b = lax.axis_index("grp"), lax.axis_index("gx"), lax.axis_index("gy")
    nx, ny, lev = state.shape[2], state.shape[3], state.shape[4]
    tx, ty = nx // 3, ny // 3
    fx, fy = cx // 2, cy // 2

    barrier = pltpu.get_barrier_semaphore()
    greeted = []

    def greet(on, device):
        greeted.append(on)

        @pl.when(on)
        def _():
            pl.semaphore_signal(barrier, inc=1, device_id=device, device_id_type=MESH)

    greet(a > 0, (g, a - 1, b))
    greet(a < cx - 1, (g, a + 1, b))
    greet(b > 0, (g, a, b - 1))
    greet(b < cy - 1, (g, a, b + 1))
    for i in range(-1, 4):
        for j in range(-1, 4):
            child_a, child_b = 3 * (a - fx) + i, 3 * (b - fy) + j
            greet(
                (g == 0) & (a >= fx) & (b >= fy) & (child_a >= 0) & (child_a < cx)
                & (child_b >= 0) & (child_b < cy),
                (1, child_a, child_b),
            )

    def parents(place, first, count):
        own = first + place // 3
        return (
            (place >= 0, own),
            ((place % 3 == 0) & (place > 0), own - 1),
            ((place % 3 == 2) & (own + 1 < count), own + 1),
        )

    for on_a, parent_a in parents(a, fx, cx):
        for on_b, parent_b in parents(b, fy, cy):
            greet((g == 1) & on_a & on_b, (0, parent_a, parent_b))

    def route(at_a, at_b):
        to_a, to_b = fx + at_a // 3, fy + at_b // 3
        far = (at_a != to_a) & (at_b != to_b)
        direct = (at_a == to_a) & (at_b == to_b)
        by_nest = (at_a % 3 == 1) & (at_b == to_b) & (at_a != to_a)
        over = jnp.logical_not(direct | by_nest)
        along_a = over & (at_a % 3 == 1) & far
        along_b = over & (at_a % 3 == 0) & far
        last = over & jnp.logical_not(along_a | along_b)
        return to_a, to_b, direct, by_nest, over, along_a, along_b, last

    to_a, to_b, direct, by_nest, over, along_a, along_b, last = route(a, b)
    parent, nest = g == 0, g == 1
    mid_a = 3 * (a - fx) + 1
    comes = (a >= fx) & (mid_a < cx)
    middle = route(mid_a, b)
    relay1, relay3 = parent & comes & middle[5], nest & comes & middle[3]
    relay2 = []
    for j in range(3):
        side_b = 3 * (b - fy) + j
        relay2.append((parent & (b >= fy) & (side_b < cy) & route(a, side_b)[6], side_b))
    greet(nest & over, (0, a, b))
    greet(parent & over, (1, a, b))
    greet(parent & along_a, (0, to_a, b))
    greet(relay1, (0, mid_a, b))
    greet(parent & along_b, (0, a, to_b))
    for on, side_b in relay2:
        greet(on, (0, a, side_b))
        greet(on, (0, to_a, b))
    greet(nest & by_nest, (1, to_a, b))
    greet(relay3, (1, mid_a, b))
    greet(parent & last, (0, to_a, to_b))
    greet(relay1, (0, a, to_b))
    greet(relay3, (0, a, b))
    greet(nest & direct, (0, a, b))
    for i in range(3):
        for j in range(3):
            from_a, from_b = 3 * (a - fx) + i, 3 * (b - fy) + j
            on = parent & (a >= fx) & (b >= fy) & (from_a < cx) & (from_b < cy)
            _, _, f_direct, f_nest, _, f_a, f_b, f_last = route(from_a, from_b)
            greet(on & f_direct, (1, a, b))
            greet(on & f_nest, (1, a, from_b))
            greet(on & f_a, (0, a, from_b))
            greet(on & f_b, (0, from_a, b))
            greet(on & f_last, (0, from_a, from_b))

    loads = [
        pltpu.make_async_copy(
            state.at[0], S.at[:, pl.ds(XB, nx), pl.ds(YB, ny), :], load_sem.at[0]
        ),
        pltpu.make_async_copy(
            courant.at[0], C.at[pl.ds(1, nx), pl.ds(YB, ny), :], load_sem.at[1]
        ),
    ]
    for n, (src, dst) in enumerate(zip(small, (inverse, iidx, iwgt, ridx, rwgt))):
        loads.append(pltpu.make_async_copy(src, dst, load_sem.at[2 + n]))
    for copy in loads:
        copy.start()
    zrow = jnp.zeros((2, ny, lev), F32)
    S[0, 0:2, YB : YB + ny, :] = zrow
    S[0, XB + nx : XB + nx + 2, YB : YB + ny, :] = zrow
    S[1, 0:2, YB : YB + ny, :] = zrow
    S[1, XB + nx : XB + nx + 2, YB : YB + ny, :] = zrow
    C[0:1, YB : YB + ny, :] = zrow[0:1]
    C[nx + 1 : nx + 2, YB : YB + ny, :] = zrow[0:1]
    zcol = jnp.zeros((nx, 8, lev), F32)
    for c in (0, 2):
        S[c, XB : XB + nx, 0:YB, :] = zcol
        S[c, XB : XB + nx, YB + ny : YB + ny + 8, :] = zcol
    C[1 : 1 + nx, 0:YB, :] = zcol
    C[1 : 1 + nx, YB + ny : YB + ny + 8, :] = zcol
    for copy in loads:
        copy.wait()
    m_high, m_low = split(inverse[:, 0, :])
    pl.semaphore_wait(barrier, sum(on.astype(jnp.int32) for on in greeted))

    dirs = (
        (a > 0, a < cx - 1, (g, a - 1, b)),
        (a < cx - 1, a > 0, (g, a + 1, b)),
        (b > 0, b < cy - 1, (g, a, b - 1)),
        (b < cy - 1, b > 0, (g, a, b + 1)),
    )

    def halo_copy(k, d):
        if k == 0:
            src, dst = (sx0, rx0) if d < 2 else (sy0, ry0)
            src, dst = src.at[d % 2], dst.at[d % 2]
        else:
            src, dst = (sx, rx) if d < 2 else (sy, ry)
            src, dst = src.at[k - 1, d % 2], dst.at[k - 1, d % 2]
        return pltpu.make_async_remote_copy(
            src_ref=src, dst_ref=dst,
            send_sem=halo_send.at[k, d], recv_sem=halo_recv.at[k, d],
            device_id=dirs[d][2], device_id_type=MESH,
        )

    def exchange(k):
        cols = slice(YB, YB + ny)
        rows = slice(XB, XB + nx)
        last_x, last_y = XB + nx, YB + ny
        if k == 0:
            sx0[0, 0:2] = S[0, XB : XB + 2, cols, :]
            sx0[0, 2:3] = S[1, XB : XB + 1, cols, :]
            sx0[0, 3:4] = C[1:2, cols, :]
            sx0[1, 0:2] = S[0, last_x - 2 : last_x, cols, :]
            sx0[1, 2:3] = S[1, last_x - 1 : last_x, cols, :]
            sx0[1, 3:4] = C[nx : nx + 1, cols, :]
            sy0[0, :, 0:2] = S[0, rows, YB : YB + 2, :]
            sy0[0, :, 2:3] = S[2, rows, YB : YB + 1, :]
            sy0[0, :, 3:4] = C[1 : 1 + nx, YB : YB + 1, :]
            sy0[1, :, 0:2] = S[0, rows, last_y - 2 : last_y, :]
            sy0[1, :, 2:3] = S[2, rows, last_y - 1 : last_y, :]
            sy0[1, :, 3:4] = C[1 : 1 + nx, last_y - 1 : last_y, :]
        else:
            sx[k - 1, 0] = S[0, XB : XB + 2, cols, :]
            sx[k - 1, 1] = S[0, last_x - 2 : last_x, cols, :]
            sy[k - 1, 0] = S[0, rows, YB : YB + 2, :]
            sy[k - 1, 1] = S[0, rows, last_y - 2 : last_y, :]
        for d in range(4):
            @pl.when(dirs[d][0])
            def _():
                halo_copy(k, d).start()
        if k == 0:
            @pl.when(g == 1)
            def _():
                restrict_weights()
        if k == 1:
            @pl.when((g == 1) & ((a == 0) | (a == cx - 1) | (b == 0) | (b == cy - 1)))
            def _():
                boundary_weights()
        for d in range(4):
            @pl.when(dirs[d][1])
            def _():
                halo_copy(k, d).wait_recv()
                if d < 2:
                    got = rx0.at[d] if k == 0 else rx.at[k - 1, d]
                    at = last_x if d == 0 else XB - 2
                    S[0, at : at + 2, cols, :] = got[0:2]
                    if k == 0:
                        at = last_x if d == 0 else XB - 1
                        S[1, at : at + 1, cols, :] = got[2:3]
                        C[at - 1 : at, cols, :] = got[3:4]
                else:
                    got = ry0.at[d - 2] if k == 0 else ry.at[k - 1, d - 2]
                    at = last_y if d == 2 else YB - 2
                    S[0, rows, at : at + 2, :] = got[:, 0:2]
                    if k == 0:
                        at = last_y if d == 2 else YB - 1
                        S[2, rows, at : at + 1, :] = got[:, 2:3]
                        C[1 : 1 + nx, at : at + 1, :] = got[:, 3:4]

    def add_mean(k, c, x, value):
        mean[c, x] = value if k == 0 else mean[c, x] + value

    def winds(k):
        def u_row(r, _):
            slope = 0.5 * (S[0, r + 1, YB : YB + ny, :] - S[0, r - 1, YB : YB + ny, :])
            S[1, r, YB : YB + ny, :] = S[1, r, YB : YB + ny, :] - C[r - 1, YB : YB + ny, :] * slope
            return 0

        u_row(XB - 1, 0)
        u_row(XB + nx, 0)

        cols, wide = slice(YB, YB + ny), slice(YB - 1, YB + ny + 1)
        group = 4

        def rows(i, _):
            new = []
            for j in range(group):
                x = i * group + j
                r = x + XB
                slope = 0.5 * (S[0, r + 1, cols, :] - S[0, r - 1, cols, :])
                u = S[1, r, cols, :] - C[x + 1, cols, :] * slope
                slope = 0.5 * (S[0, r, YB : YB + ny + 2, :] - S[0, r, YB - 2 : YB + ny, :])
                v = S[2, r, wide, :] - C[x + 1, wide, :] * slope
                new.append((x, u, v))
            for x, u, v in new:
                S[1, x + XB, cols, :] = u
                S[2, x + XB, wide, :] = v
                add_mean(k, 1, x, u)
                add_mean(k, 2, x, v[1 : ny + 1])
            return 0

        lax.fori_loop(0, nx // group, rows, 0)

    def press(k):
        group = 12

        def rows(i, _):
            parts = []
            for j in range(group):
                x = i * group + j
                r = x + XB
                div = 0.5 * (S[1, r + 1, YB : YB + ny, :] - S[1, r - 1, YB : YB + ny, :]) + 0.5 * (
                    S[2, r, YB + 1 : YB + ny + 1, :] - S[2, r, YB - 1 : YB + ny - 1, :]
                )
                parts.append(S[0, r, YB : YB + ny, :] - C[x + 1, YB : YB + ny, :] * div)
            solved = dot3(jnp.concatenate(parts, axis=0), m_high, m_low)
            for j in range(group):
                x = i * group + j
                new = solved[j * ny : (j + 1) * ny]
                S[0, x + XB, YB : YB + ny, :] = new
                add_mean(k, 0, x, new)
            return 0

        lax.fori_loop(0, nx // group, rows, 0)

    def hop(src, dst, device, send, recv):
        return pltpu.make_async_remote_copy(
            src_ref=src, dst_ref=dst, send_sem=send, recv_sem=recv,
            device_id=device, device_id_type=MESH,
        )

    def home(src, c, i, j, device, send):
        n = 3 * i + j
        return hop(src, fb.at[n, c], device, send, fb_recv.at[n, c])

    def fb_copies(c):
        mine, sem = rst.at[c], fb_send.at[c]
        return (
            (direct, home(mine, c, a % 3, b % 3, (0, a, b), sem)),
            (by_nest, hop(mine, q3.at[c], (1, to_a, b), sem, q_recv.at[5, c])),
            (over, hop(mine, q0.at[c], (0, a, b), sem, q_recv.at[0, c])),
        )

    def fb_start(c):
        for on, copy in fb_copies(c):
            @pl.when(on)
            def _():
                copy.start()

    def relays(c):
        sem0 = q_send.at[0, c]
        yield parent & over, q0.at[c], 0, (
            (along_a, hop(q0.at[c], q1.at[c], (0, to_a, b), sem0, q_recv.at[1, c])),
            (along_b, hop(q0.at[c], q2.at[b % 3, c], (0, a, to_b), sem0,
                          q_recv.at[2 + b % 3, c])),
            (last, home(q0.at[c], c, a % 3, b % 3, (0, to_a, to_b), sem0)),
        )
        yield relay1, q1.at[c], 1, (
            (relay1, home(q1.at[c], c, 1, b % 3, (0, a, to_b), q_send.at[1, c])),
        )
        for j, (on, side_b) in enumerate(relay2):
            yield on, q2.at[j, c], 2 + j, (
                (on, home(q2.at[j, c], c, 0, j, (0, to_a, b), q_send.at[2 + j, c])),
            )
        yield relay3, q3.at[c], 5, (
            (relay3, home(q3.at[c], c, 1, b % 3, (0, a, b), q_send.at[5, c])),
        )

    def pass_on():
        for c in (1, 2, 0):
            for here, buffer, n, onward in relays(c):
                @pl.when(here)
                def _():
                    hop(buffer, buffer, (g, a, b), q_send.at[n, c], q_recv.at[n, c]).wait_recv()
                    for on, copy in onward:
                        @pl.when(on)
                        def _():
                            copy.start()

    def passed_on():
        for c in (1, 2, 0):
            for here, buffer, n, onward in relays(c):
                @pl.when(here)
                def _():
                    hop(buffer, buffer, (g, a, b), q_send.at[n, c], q_recv.at[n, c]).wait_send()

    def restrict(comps):
        def rows(u, _):
            new = []
            for c in comps:
                total = None
                for t in range(9):
                    part = wr[u, t] * mean[c, 3 * u + t // 3, pl.ds(t % 3, ty, stride=3), :]
                    total = part if total is None else total + part
                new.append((c, total))
            for c, total in new:
                rst[c, u] = total
            return 0

        lax.fori_loop(0, tx, rows, 0)

    def restrict_weights():
        terms = range(ridx.shape[0])
        w = [rwgt[k] for k in terms]
        scale = (1.0 / SUBS) / row_sum(w)
        shares = [part * scale for part in w]
        index = [ridx[k] for k in terms]
        for t in range(9):
            at = row_sum([jnp.where(index[k] == t, shares[k], 0.0) for k in terms]).T
            for u in range(tx):
                wr[u, t] = jnp.broadcast_to(at[:, u : u + 1], (ty, lev))

    def boundary_weights():
        share = iwgt[...] / jnp.sum(iwgt[...], axis=1, keepdims=True)
        share = share.reshape(nx * 4, ny).T
        index = iidx[...].astype(F32).reshape(nx * 4, ny).T.astype(jnp.int32)
        over = third(index)
        shape = index.shape
        x3 = (lax.broadcasted_iota(jnp.int32, shape, 1) * 171) >> 11
        y3 = (lax.broadcasted_iota(jnp.int32, shape, 0) * 171) >> 9
        source_x = jnp.clip(a * tx + x3 + over - 1, 0, cx * tx - 1)
        source_y = jnp.clip(b * ty + y3 + (index - 3 * over) - 1, 0, cy * ty - 1)

        def spread(cells, parts, x, depth):
            places = lax.broadcasted_iota(jnp.int32, (cells.shape[0], depth), 1)
            total = jnp.zeros(places.shape, F32)
            for n in range(4 * x, 4 * x + 4):
                total = total + jnp.where(places == cells[:, n : n + 1], parts[:, n : n + 1], 0.0)
            return total

        def y_weights(col, strip0):
            cells = (source_x - (a * tx - 1)) * 8 + source_y - (b * ty + strip0)
            cells, parts = cells[col : col + 8], share[col : col + 8]
            for x in range(nx):
                wy[8 * x : 8 * x + 8] = spread(cells, parts, x, 8 * (tx + 2))

        def x_weights(first, strip0):
            wide = ty + 16
            cells = (source_x - (a * tx + strip0)) * wide + source_y - (b * ty - 8)
            for i in range(BAND):
                wx[ny * i : ny * i + ny] = spread(cells, share, first + i, 3 * wide)

        @pl.when(b == 0)
        def _():
            y_weights(0, 0)

        @pl.when(b == cy - 1)
        def _():
            y_weights(ny - 8, ty - 8)

        @pl.when(a == 0)
        def _():
            x_weights(0, 0)

        @pl.when(a == cx - 1)
        def _():
            x_weights(nx - BAND, tx - 3)

    def row_sum(rows):
        total = rows[0]
        for row in rows[1:]:
            total = total + row
        return total

    for k in range(SUBS):
        exchange(k)
        winds(k)
        if k == SUBS - 1:
            @pl.when(g == 1)
            def _():
                restrict((1, 2))
                fb_start(1)
                fb_start(2)
        press(k)

    x_windows = {-1: (0, 8, 24), 0: (0, ty + 8, 8), 1: (ty - 8, 2 * ty + 8, 0),
                 2: (2 * ty - 8, ny, 0), 3: (ny - 8, ny, 0)}
    y_windows = {-1: (0, 1, tx + 1), 0: (0, tx + 1, 1), 1: (tx - 1, 2 * tx + 1, 0),
                 2: (2 * tx - 1, nx, 0), 3: (nx - 1, nx, 0)}
    kinds = {-1: 1, 0: 0, 1: 0, 2: 0, 3: 2}

    def strip_copies():
        for side in range(2):
            edge = 0 if side == 0 else cx - 1
            at = XB if side == 0 else XB + tx * (edge % 3) + tx - 3
            for j in range(-1, 4):
                lo, hi, dst = x_windows[j]
                child = 3 * (b - fy) + j
                on = (a == fx + edge // 3) & (b >= fy) & (child >= 0) & (child < cy)
                yield on, pltpu.make_async_remote_copy(
                    src_ref=S.at[:, pl.ds(at, 3), pl.ds(YB + lo, hi - lo), :],
                    dst_ref=xstrip.at[:, :, pl.ds(dst, hi - lo), :],
                    send_sem=strip_send.at[0, side, j + 1], recv_sem=strip_recv.at[0, kinds[j]],
                    device_id=(1, edge, child), device_id_type=MESH,
                )
            edge = 0 if side == 0 else cy - 1
            at = YB if side == 0 else YB + ty * (edge % 3) + ty - 8
            for i in range(-1, 4):
                lo, hi, dst = y_windows[i]
                child = 3 * (a - fx) + i
                on = (b == fy + edge // 3) & (a >= fx) & (child >= 0) & (child < cx)
                yield on, pltpu.make_async_remote_copy(
                    src_ref=S.at[:, pl.ds(XB + lo, hi - lo), pl.ds(at, 8), :],
                    dst_ref=ystrip.at[:, pl.ds(dst, hi - lo), :, :],
                    send_sem=strip_send.at[1, side, i + 1], recv_sem=strip_recv.at[1, kinds[i]],
                    device_id=(1, child, edge), device_id_type=MESH,
                )

    def strip_wait(axis, kind, lo, hi, dst):
        if axis == 0:
            ref = xstrip.at[:, :, pl.ds(dst, hi - lo), :]
        else:
            ref = ystrip.at[:, pl.ds(dst, hi - lo), :, :]
        pltpu.make_async_remote_copy(
            src_ref=ref, dst_ref=ref, send_sem=strip_send.at[0, 0, 0],
            recv_sem=strip_recv.at[axis, kind], device_id=(g, a, b), device_id_type=MESH,
        ).wait_recv()

    def wait_strips(axis, place, count, windows):
        for i in range(3):
            @pl.when(place % 3 == i)
            def _():
                strip_wait(axis, 0, *windows[i])

        @pl.when((place % 3 == 2) & (place < count - 1))
        def _():
            strip_wait(axis, 1, *windows[-1])

        @pl.when((place % 3 == 0) & (place > 0))
        def _():
            strip_wait(axis, 2, *windows[3])

    def relax_at(x, y):
        gx, gy = a * nx + x, b * ny + y
        depth = jnp.minimum(
            jnp.minimum(gx, nx * cx - 1 - gx), jnp.minimum(gy, ny * cy - 1 - gy)
        ).astype(F32)
        return jnp.maximum(1.0 - depth / BAND, 0.0)

    def mixed(weights, source):
        w_high, w_low = split(weights)
        s_high, s_low = split(source)
        return dot(w_high, s_high) + (dot(w_low, s_high) + dot(w_high, s_low))

    def y_edge(col):
        shape = (nx, 8, lev)
        relax = relax_at(
            lax.broadcasted_iota(jnp.int32, shape, 0), col + lax.broadcasted_iota(jnp.int32, shape, 1)
        )
        for c in range(3):
            bound = mixed(wy[...], ystrip[c].reshape(8 * (tx + 2), lev)).reshape(shape)
            at = (c, slice(XB, XB + nx), slice(YB + col, YB + col + 8), slice(None))
            now = S[at]
            S[at] = now + relax * (bound - now)

    def x_edge(first):
        shape = (BAND, ny, lev)
        relax = relax_at(
            first + lax.broadcasted_iota(jnp.int32, shape, 0), lax.broadcasted_iota(jnp.int32, shape, 1)
        )
        for c in range(3):
            bound = mixed(wx[...], xstrip[c].reshape(3 * (ty + 16), lev)).reshape(shape)
            now = mean[c, 0:BAND]
            S[c, XB + first : XB + first + BAND, YB : YB + ny, :] = now + relax * (bound - now)

    @pl.when(g == 1)
    def _():
        restrict((0,))
        fb_start(0)
        pass_on()
        x_low, x_high = a == 0, a == cx - 1
        y_low, y_high = b == 0, b == cy - 1

        @pl.when(x_low)
        def _():
            for c in range(3):
                mean[c, 0:BAND] = S[c, XB : XB + BAND, YB : YB + ny, :]

        @pl.when(x_high)
        def _():
            for c in range(3):
                mean[c, 0:BAND] = S[c, XB + nx - BAND : XB + nx, YB : YB + ny, :]

        @pl.when(x_low | x_high)
        def _():
            xstrip_pad = jnp.zeros((3, 3, 8, lev), F32)

            @pl.when(y_low)
            def _():
                xstrip[:, :, 0:8, :] = xstrip_pad

            if (cy - 1) % 3 == 2:

                @pl.when(y_high)
                def _():
                    xstrip[:, :, ty + 8 : ty + 16, :] = xstrip_pad

        @pl.when(y_low | y_high)
        def _():
            @pl.when(x_low)
            def _():
                ystrip[:, 0:1] = jnp.zeros((3, 1, 8, lev), F32)

            if (cx - 1) % 3 == 2:

                @pl.when(x_high)
                def _():
                    ystrip[:, tx + 1 : tx + 2] = jnp.zeros((3, 1, 8, lev), F32)

            wait_strips(1, a, cx, y_windows)

        @pl.when(y_low)
        def _():
            y_edge(0)

        @pl.when(y_high)
        def _():
            y_edge(ny - 8)

        @pl.when(x_low | x_high)
        def _():
            wait_strips(0, b, cy, x_windows)

        @pl.when(x_low)
        def _():
            x_edge(0)

        @pl.when(x_high)
        def _():
            x_edge(nx - BAND)

        for c in range(3):
            hop(rst.at[c], rst.at[c], (g, a, b), fb_send.at[c], q_recv.at[0, c]).wait_send()

    @pl.when(g == 0)
    def _():
        for on, copy in strip_copies():
            @pl.when(on)
            def _():
                copy.start()
        pass_on()
        for on, copy in strip_copies():
            @pl.when(on)
            def _():
                copy.wait_send()
        for i in range(3):
            for j in range(3):
                there = (
                    (a >= fx) & (b >= fy) & (3 * (a - fx) + i < cx) & (3 * (b - fy) + j < cy)
                )

                @pl.when(there)
                def _():
                    for c in (1, 2, 0):
                        piece = fb.at[3 * i + j, c]
                        pltpu.make_async_remote_copy(
                            src_ref=piece, dst_ref=piece, send_sem=fb_send.at[c],
                            recv_sem=fb_recv.at[3 * i + j, c], device_id=(g, a, b),
                            device_id_type=MESH,
                        ).wait_recv()
                        at = (c, slice(XB + i * tx, XB + (i + 1) * tx),
                              slice(YB + j * ty, YB + (j + 1) * ty), slice(None))
                        now = S[at]
                        S[at] = now + FEEDBACK * (piece[...] - now)

    for k in range(SUBS):
        for d in range(4):
            @pl.when(dirs[d][0])
            def _():
                halo_copy(k, d).wait_send()
    passed_on()


def per_device(
    state, courant, vert_inverse, interp_index, interp_weight, restrict_index, restrict_weight
):
    cx, cy = lax.axis_size("gx"), lax.axis_size("gy")
    _, _, nx, ny, lev = state.shape
    tx, ty = nx // 3, ny // 3
    vmem = lambda *shape: pltpu.VMEM(shape, F32)
    dma = pltpu.SemaphoreType.DMA
    anywhere = pl.BlockSpec(memory_space=pltpu.HBM)
    inside = pl.BlockSpec(memory_space=pltpu.VMEM)
    padded = pl.pallas_call(
        functools.partial(kernel, cx, cy),
        out_shape=vmem(3, nx + 4, ny + 16, lev),
        in_specs=[anywhere] * 7,
        out_specs=inside,
        scratch_shapes=[
            vmem(nx + 2, ny + 16, lev),
            vmem(lev, 1, lev),
            pltpu.VMEM((nx, 4, ny), jnp.int32),
            vmem(nx, 4, ny),
            pltpu.VMEM((9, tx, ty), jnp.int32),
            vmem(9, tx, ty),
            vmem(3, nx, ny, lev),
            vmem(tx, 9, ty, lev),
            vmem(BAND * ny, 3 * (ty + 16)),
            vmem(nx * 8, 8 * (tx + 2)),
            vmem(2, 4, ny, lev),
            vmem(2, nx, 4, lev),
            vmem(2, 4, ny, lev),
            vmem(2, nx, 4, lev),
            vmem(SUBS - 1, 2, 2, ny, lev),
            vmem(SUBS - 1, 2, nx, 2, lev),
            vmem(SUBS - 1, 2, 2, ny, lev),
            vmem(SUBS - 1, 2, nx, 2, lev),
            vmem(3, tx, ty, lev),
            vmem(9, 3, tx, ty, lev),
            vmem(3, 3, ty + 16, lev),
            vmem(3, tx + 2, 8, lev),
            dma((7,)),
            dma((SUBS, 4)),
            dma((SUBS, 4)),
            dma((2, 2, 5)),
            dma((2, 3)),
            dma((3,)),
            dma((9, 3)),
            vmem(3, tx, ty, lev),
            vmem(3, tx, ty, lev),
            vmem(3, 3, tx, ty, lev),
            vmem(3, tx, ty, lev),
            dma((6, 3)),
            dma((6, 3)),
        ],
        compiler_params=pltpu.CompilerParams(
            has_side_effects=True, collective_id=0, vmem_limit_bytes=67043328 - 4 * (3 * (nx + 4) * (ny + 16) * 128) - 2**14
        ),
        name="nest_step",
    )(
        state, courant, vert_inverse.transpose(1, 0, 2),
        interp_index.transpose(0, 2, 1), interp_weight.transpose(0, 2, 1),
        restrict_index.transpose(2, 0, 1), restrict_weight.transpose(2, 0, 1),
    )
    return padded[None, :, XB : XB + nx, YB : YB + ny, :]


def solution(mesh):
    return jax.shard_map(
        per_device,
        mesh=mesh,
        in_specs=(
            P("grp", None, "gx", "gy", None),
            P("grp", "gx", "gy", None),
            P("grp", None, None),
            P("gx", "gy", None),
            P("gx", "gy", None),
            P("gx", "gy", None),
            P("gx", "gy", None),
        ),
        out_specs=P("grp", None, "gx", "gy", None),
        check_vma=False,
    )
```

```python
import functools

import jax
import jax.numpy as jnp
from jax import lax
from jax.experimental import pallas as pl
from jax.experimental.pallas import tpu as pltpu
from jax.sharding import PartitionSpec as P

SUBS = 4
BAND = 5
FEEDBACK = 0.5
MESH = pl.DeviceIdType.MESH
F32 = jnp.float32
XB, YB = 2, 8


def split(a):
    high = a.astype(jnp.bfloat16)
    return high, (a - high.astype(F32)).astype(jnp.bfloat16)


def dot(a, b):
    return jnp.dot(a, b, preferred_element_type=F32)


def dot3(a, b_high, b_low):
    a_high, a_low = split(a)
    return dot(a_high, b_high) + (dot(a_low, b_high) + dot(a_high, b_low))


def third(t):
    return (t * 11) >> 5


def kernel(
    cx, cy,
    state, courant, *rest,
):
    small, (
    S,
    C, inverse, iidx, iwgt, ridx, rwgt, mean, wr, wx, wy, sx0, sy0, rx0, ry0, sx, sy, rx, ry, rst, fb, xstrip, ystrip,
    load_sem, halo_send, halo_recv, strip_send, strip_recv, fb_send, fb_recv,
    q0, q1, q2, xpack, ypack, q_send, q_recv,
    ) = rest[:5], rest[5:]
    g, a, b = lax.axis_index("grp"), lax.axis_index("gx"), lax.axis_index("gy")
    nx, ny, lev = state.shape[2], state.shape[3], state.shape[4]
    tx, ty = nx // 3, ny // 3
    fx, fy = cx // 2, cy // 2
    quarter, slot = tx // 4, lev // 3

    barrier = pltpu.get_barrier_semaphore()
    greeted = []

    def greet(on, device):
        greeted.append(on)

        @pl.when(on)
        def _():
            pl.semaphore_signal(barrier, inc=1, device_id=device, device_id_type=MESH)

    greet(a > 0, (g, a - 1, b))
    greet(a < cx - 1, (g, a + 1, b))
    greet(b > 0, (g, a, b - 1))
    greet(b < cy - 1, (g, a, b + 1))
    for i in range(-1, 4):
        for j in range(-1, 4):
            child_a, child_b = 3 * (a - fx) + i, 3 * (b - fy) + j
            greet(
                (g == 0) & (a >= fx) & (b >= fy) & (child_a >= 0) & (child_a < cx)
                & (child_b >= 0) & (child_b < cy),
                (1, child_a, child_b),
            )

    def parents(place, first, count):
        own = first + place // 3
        return (
            (place >= 0, own),
            ((place % 3 == 0) & (place > 0), own - 1),
            ((place % 3 == 2) & (own + 1 < count), own + 1),
        )

    for on_a, parent_a in parents(a, fx, cx):
        for on_b, parent_b in parents(b, fy, cy):
            greet((g == 1) & on_a & on_b, (0, parent_a, parent_b))

    def route(at_a, at_b):
        to_a, to_b = fx + at_a // 3, fy + at_b // 3
        far = (at_a != to_a) & (at_b != to_b)
        direct = (at_a == to_a) & (at_b == to_b)
        over = jnp.logical_not(direct)
        along_a = over & (at_a % 3 == 1) & far
        along_b = over & (at_a % 3 == 0) & far
        last = over & jnp.logical_not(along_a | along_b)
        return to_a, to_b, direct, over, along_a, along_b, last

    to_a, to_b, direct, over, along_a, along_b, last = route(a, b)
    parent, nest = g == 0, g == 1
    mid_a = 3 * (a - fx) + 1
    comes = (a >= fx) & (mid_a < cx)
    relay1 = parent & comes & route(mid_a, b)[4]
    relay2 = []
    for j in range(3):
        side_b = 3 * (b - fy) + j
        relay2.append((parent & (b >= fy) & (side_b < cy) & route(a, side_b)[5], side_b))
    greet(nest & over, (0, a, b))
    greet(parent & over, (1, a, b))
    greet(parent & along_a, (0, to_a, b))
    greet(relay1, (0, mid_a, b))
    greet(parent & along_b, (0, a, to_b))
    for on, side_b in relay2:
        greet(on, (0, a, side_b))
        greet(on, (0, to_a, b))
    greet(parent & last, (0, to_a, to_b))
    greet(relay1, (0, a, to_b))
    for i in range(3):
        for j in range(3):
            from_a, from_b = 3 * (a - fx) + i, 3 * (b - fy) + j
            on = parent & (a >= fx) & (b >= fy) & (from_a < cx) & (from_b < cy)
            f_a, f_b, f_last = route(from_a, from_b)[4:]
            greet(on & f_a, (0, a, from_b))
            greet(on & f_b, (0, from_a, b))
            greet(on & f_last, (0, from_a, from_b))

    loads = [
        pltpu.make_async_copy(
            state.at[0], S.at[:, pl.ds(XB, nx), pl.ds(YB, ny), :], load_sem.at[0]
        ),
        pltpu.make_async_copy(
            courant.at[0], C.at[pl.ds(1, nx), pl.ds(YB, ny), :], load_sem.at[1]
        ),
    ]
    for n, (src, dst) in enumerate(zip(small, (inverse, iidx, iwgt, ridx, rwgt))):
        loads.append(pltpu.make_async_copy(src, dst, load_sem.at[2 + n]))
    for copy in loads:
        copy.start()
    zrow = jnp.zeros((2, ny, lev), F32)
    S[0, 0:2, YB : YB + ny, :] = zrow
    S[0, XB + nx : XB + nx + 2, YB : YB + ny, :] = zrow
    S[1, 0:2, YB : YB + ny, :] = zrow
    S[1, XB + nx : XB + nx + 2, YB : YB + ny, :] = zrow
    C[0:1, YB : YB + ny, :] = zrow[0:1]
    C[nx + 1 : nx + 2, YB : YB + ny, :] = zrow[0:1]
    zcol = jnp.zeros((nx, 8, lev), F32)
    for c in (0, 2):
        S[c, XB : XB + nx, 0:YB, :] = zcol
        S[c, XB : XB + nx, YB + ny : YB + ny + 8, :] = zcol
    C[1 : 1 + nx, 0:YB, :] = zcol
    C[1 : 1 + nx, YB + ny : YB + ny + 8, :] = zcol
    with jax.named_scope("loads"):
        for copy in loads:
            copy.wait()
    m_high, m_low = split(inverse[:, 0, :])
    with jax.named_scope("greet"):
        pl.semaphore_wait(barrier, sum(on.astype(jnp.int32) for on in greeted))

    dirs = (
        (a > 0, a < cx - 1, (g, a - 1, b)),
        (a < cx - 1, a > 0, (g, a + 1, b)),
        (b > 0, b < cy - 1, (g, a, b - 1)),
        (b < cy - 1, b > 0, (g, a, b + 1)),
    )

    def halo_copy(k, d):
        if k == 0:
            src, dst = (sx0, rx0) if d < 2 else (sy0, ry0)
            src, dst = src.at[d % 2], dst.at[d % 2]
        else:
            src, dst = (sx, rx) if d < 2 else (sy, ry)
            src, dst = src.at[k - 1, d % 2], dst.at[k - 1, d % 2]
        return pltpu.make_async_remote_copy(
            src_ref=src, dst_ref=dst,
            send_sem=halo_send.at[d], recv_sem=halo_recv.at[k % 2, d],
            device_id=dirs[d][2], device_id_type=MESH,
        )

    def halo_sent(k):
        for d in range(4):
            @pl.when(dirs[d][0])
            def _():
                halo_copy(k, d).wait_send()

    def exchange(k):
        cols = slice(YB, YB + ny)
        rows = slice(XB, XB + nx)
        last_x, last_y = XB + nx, YB + ny
        if k == 0:
            sx0[0, 0:2] = S[0, XB : XB + 2, cols, :]
            sx0[0, 2:3] = S[1, XB : XB + 1, cols, :]
            sx0[0, 3:4] = C[1:2, cols, :]
            sx0[1, 0:2] = S[0, last_x - 2 : last_x, cols, :]
            sx0[1, 2:3] = S[1, last_x - 1 : last_x, cols, :]
            sx0[1, 3:4] = C[nx : nx + 1, cols, :]
            sy0[0, :, 0:2] = S[0, rows, YB : YB + 2, :]
            sy0[0, :, 2:3] = S[2, rows, YB : YB + 1, :]
            sy0[0, :, 3:4] = C[1 : 1 + nx, YB : YB + 1, :]
            sy0[1, :, 0:2] = S[0, rows, last_y - 2 : last_y, :]
            sy0[1, :, 2:3] = S[2, rows, last_y - 1 : last_y, :]
            sy0[1, :, 3:4] = C[1 : 1 + nx, last_y - 1 : last_y, :]
        else:
            sx[k - 1, 0] = S[0, XB : XB + 2, cols, :]
            sx[k - 1, 1] = S[0, last_x - 2 : last_x, cols, :]
            sy[k - 1, 0] = S[0, rows, YB : YB + 2, :]
            sy[k - 1, 1] = S[0, rows, last_y - 2 : last_y, :]
        if k > 0:
            halo_sent(k - 1)
        for d in range(4):
            @pl.when(dirs[d][0])
            def _():
                halo_copy(k, d).start()
        if k == 0:
            @pl.when(g == 1)
            def _():
                with jax.named_scope("restrict_weights"):
                    restrict_weights()
        if k == 1:
            @pl.when((g == 1) & ((a == 0) | (a == cx - 1) | (b == 0) | (b == cy - 1)))
            def _():
                with jax.named_scope("boundary_weights"):
                    boundary_weights()
        for d in range(4):
            @pl.when(dirs[d][1])
            def _():
                halo_copy(k, d).wait_recv()
                if d < 2:
                    got = rx0.at[d] if k == 0 else rx.at[k - 1, d]
                    at = last_x if d == 0 else XB - 2
                    S[0, at : at + 2, cols, :] = got[0:2]
                    if k == 0:
                        at = last_x if d == 0 else XB - 1
                        S[1, at : at + 1, cols, :] = got[2:3]
                        C[at - 1 : at, cols, :] = got[3:4]
                else:
                    got = ry0.at[d - 2] if k == 0 else ry.at[k - 1, d - 2]
                    at = last_y if d == 2 else YB - 2
                    S[0, rows, at : at + 2, :] = got[:, 0:2]
                    if k == 0:
                        at = last_y if d == 2 else YB - 1
                        S[2, rows, at : at + 1, :] = got[:, 2:3]
                        C[1 : 1 + nx, at : at + 1, :] = got[:, 3:4]

    def add_mean(k, c, x, value):
        mean[c, x] = value if k == 0 else mean[c, x] + value

    def winds(k):
        def u_row(r, _):
            slope = 0.5 * (S[0, r + 1, YB : YB + ny, :] - S[0, r - 1, YB : YB + ny, :])
            S[1, r, YB : YB + ny, :] = S[1, r, YB : YB + ny, :] - C[r - 1, YB : YB + ny, :] * slope
            return 0

        u_row(XB - 1, 0)
        u_row(XB + nx, 0)

        cols, wide = slice(YB, YB + ny), slice(YB - 1, YB + ny + 1)
        group = 4

        def rows(i, _):
            new = []
            for j in range(group):
                x = i * group + j
                r = x + XB
                slope = 0.5 * (S[0, r + 1, cols, :] - S[0, r - 1, cols, :])
                u = S[1, r, cols, :] - C[x + 1, cols, :] * slope
                slope = 0.5 * (S[0, r, YB : YB + ny + 2, :] - S[0, r, YB - 2 : YB + ny, :])
                v = S[2, r, wide, :] - C[x + 1, wide, :] * slope
                new.append((x, u, v))
            for x, u, v in new:
                S[1, x + XB, cols, :] = u
                S[2, x + XB, wide, :] = v
                add_mean(k, 1, x, u)
                add_mean(k, 2, x, v[1 : ny + 1])
            return 0

        lax.fori_loop(0, nx // group, rows, 0)

    def press(k):
        group = 12

        def rows(i, _):
            parts = []
            for j in range(group):
                x = i * group + j
                r = x + XB
                div = 0.5 * (S[1, r + 1, YB : YB + ny, :] - S[1, r - 1, YB : YB + ny, :]) + 0.5 * (
                    S[2, r, YB + 1 : YB + ny + 1, :] - S[2, r, YB - 1 : YB + ny - 1, :]
                )
                parts.append(S[0, r, YB : YB + ny, :] - C[x + 1, YB : YB + ny, :] * div)
            solved = dot3(jnp.concatenate(parts, axis=0), m_high, m_low)
            for j in range(group):
                x = i * group + j
                new = solved[j * ny : (j + 1) * ny]
                S[0, x + XB, YB : YB + ny, :] = new
                add_mean(k, 0, x, new)
            return 0

        lax.fori_loop(0, nx // group, rows, 0)

    def hop(src, dst, device, send, recv):
        return pltpu.make_async_remote_copy(
            src_ref=src, dst_ref=dst, send_sem=send, recv_sem=recv,
            device_id=device, device_id_type=MESH,
        )

    def home(src, c, i, j, device, send):
        n = 3 * i + j
        return hop(src, fb.at[n, c], device, send, fb_recv.at[n, min(c, 1)])

    def fb_copies(c):
        mine, sem = rst.at[c], fb_send.at[min(c, 1)]
        straight = home(mine, c, a % 3, b % 3, (0, to_a, to_b), sem)
        if c == 0:
            return ((nest, straight),)
        return (
            (direct, straight),
            (over, hop(mine, q0.at[c - 1], (0, a, b), sem, q_recv.at[0, c - 1])),
        )

    def fb_start(c):
        for on, copy in fb_copies(c):
            @pl.when(on)
            def _():
                copy.start()

    def relays(c):
        n = c - 1
        sem0 = q_send.at[0]
        yield parent & over, q0, 0, (
            (along_a, hop(q0.at[n], q1.at[n], (0, to_a, b), sem0, q_recv.at[1, n])),
            (along_b, hop(q0.at[n], q2.at[b % 3, n], (0, a, to_b), sem0,
                          q_recv.at[2 + b % 3, n])),
            (last, home(q0.at[n], c, a % 3, b % 3, (0, to_a, to_b), sem0)),
        )
        yield relay1, q1, 1, (
            (relay1, home(q1.at[n], c, 1, b % 3, (0, a, to_b), q_send.at[1])),
        )
        for j, (on, side_b) in enumerate(relay2):
            yield on, q2.at[j], 2 + j, (
                (on, home(q2.at[j, n], c, 0, j, (0, to_a, b), q_send.at[2 + j])),
            )

    def pass_on():
        for stages in zip(relays(1), relays(2)):
            for n, (here, buffer, stage, onward) in enumerate(stages):
                @pl.when(here)
                def _():
                    piece = buffer.at[n]
                    hop(piece, piece, (g, a, b), q_send.at[stage], q_recv.at[stage, n]).wait_recv()
                    for on, copy in onward:
                        @pl.when(on)
                        def _():
                            copy.start()

    def passed_on():
        for here, buffer, stage, _ in relays(1):
            @pl.when(here)
            def _():
                hop(buffer, buffer, (g, a, b), q_send.at[stage], q_recv.at[0, 0]).wait_send()

    def restrict(comps):
        def mixed_row(c, u):
            total = None
            for t in range(9):
                part = wr[u, t] * mean[c, 3 * u + t // 3, pl.ds(t % 3, ty, stride=3), :]
                total = part if total is None else total + part
            return total

        def rows(i, _):
            new = []
            spare = jnp.zeros((ty, 128 - lev - slot), F32)
            for c in comps:
                guest = mixed_row(c, 3 * quarter + i)
                for m in range(3):
                    new.append((c, 3 * i + m, mixed_row(c, 3 * i + m), guest[:, m * slot : (m + 1) * slot]))
            for c, u, own, part in new:
                rst[c, u] = jnp.concatenate([own, part, spare], axis=1)
            return 0

        lax.fori_loop(0, quarter, rows, 0)

    def restrict_weights():
        terms = range(ridx.shape[0])
        w = [rwgt[k] for k in terms]
        scale = (1.0 / SUBS) / row_sum(w)
        shares = [part * scale for part in w]
        index = [ridx[k] for k in terms]
        for t in range(9):
            at = row_sum([jnp.where(index[k] == t, shares[k], 0.0) for k in terms]).T
            for u in range(tx):
                wr[u, t] = jnp.broadcast_to(at[:, u : u + 1], (ty, lev))

    def boundary_weights():
        share = iwgt[...] / jnp.sum(iwgt[...], axis=1, keepdims=True)
        share = share.reshape(nx * 4, ny).T
        index = iidx[...].astype(F32).reshape(nx * 4, ny).T.astype(jnp.int32)
        over = third(index)
        shape = index.shape
        x3 = (lax.broadcasted_iota(jnp.int32, shape, 1) * 171) >> 11
        y3 = (lax.broadcasted_iota(jnp.int32, shape, 0) * 171) >> 9
        source_x = jnp.clip(a * tx + x3 + over - 1, 0, cx * tx - 1)
        source_y = jnp.clip(b * ty + y3 + (index - 3 * over) - 1, 0, cy * ty - 1)

        def spread(cells, parts, x, depth):
            places = lax.broadcasted_iota(jnp.int32, (cells.shape[0], depth), 1)
            total = jnp.zeros(places.shape, F32)
            for n in range(4 * x, 4 * x + 4):
                total = total + jnp.where(places == cells[:, n : n + 1], parts[:, n : n + 1], 0.0)
            return total

        def y_weights(col, strip0):
            cells = (source_x - (a * tx - 1)) * 4 + source_y - (b * ty + strip0)
            cells, parts = cells[col : col + 8], share[col : col + 8]
            for x in range(nx):
                wy[8 * x : 8 * x + 8] = spread(cells, parts, x, 4 * (tx + 2))

        def x_weights(first, strip0):
            wide = ty + 16
            cells = (source_x - (a * tx + strip0)) * wide + source_y - (b * ty - 8)
            for i in range(BAND):
                wx[ny * i : ny * i + ny] = spread(cells, share, first + i, 3 * wide)

        @pl.when(b == 0)
        def _():
            y_weights(0, 0)

        @pl.when(b == cy - 1)
        def _():
            y_weights(ny - 8, ty - 4)

        @pl.when(a == 0)
        def _():
            x_weights(0, 0)

        @pl.when(a == cx - 1)
        def _():
            x_weights(nx - BAND, tx - 3)

    def row_sum(rows):
        total = rows[0]
        for row in rows[1:]:
            total = total + row
        return total

    x_windows = {-1: (0, 8, 24), 0: (0, ty + 8, 8), 1: (ty - 8, 2 * ty + 8, 0),
                 2: (2 * ty - 8, ny, 0), 3: (ny - 8, ny, 0)}
    y_windows = {-1: (0, 1, tx + 1), 0: (0, tx + 1, 1), 1: (tx - 1, 2 * tx + 1, 0),
                 2: (2 * tx - 1, nx, 0), 3: (nx - 1, nx, 0)}
    kinds = {-1: 1, 0: 0, 1: 0, 2: 0, 3: 2}

    def x_side(side):
        edge = 0 if side == 0 else cx - 1
        at = XB if side == 0 else XB + tx * (edge % 3) + tx - 3
        return edge, (a == fx + edge // 3) & (b >= fy), at

    def y_side(side):
        edge = 0 if side == 0 else cy - 1
        at = YB if side == 0 else YB + ty * (edge % 3) + ty - 4
        return edge, (b == fy + edge // 3) & (a >= fx), at

    def strip_pack(comps):
        for side in range(2):
            _, on, x_at = x_side(side)

            @pl.when(on)
            def _():
                for c in comps:
                    xpack[c] = S[c, x_at : x_at + 3, YB : YB + ny, :]

            _, on, y_at = y_side(side)

            @pl.when(on)
            def _():
                for c in comps:
                    ypack[c] = S[c, XB : XB + nx, y_at : y_at + 4, :]

    def strip_copies(comps):
        for side in range(2):
            edge, here, _ = x_side(side)
            for j in range(-1, 4):
                lo, hi, dst = x_windows[j]
                child = 3 * (b - fy) + j
                yield here & (child >= 0) & (child < cy), pltpu.make_async_remote_copy(
                    src_ref=xpack.at[comps, :, pl.ds(lo, hi - lo), :],
                    dst_ref=xstrip.at[comps, :, pl.ds(dst, hi - lo), :],
                    send_sem=strip_send.at[0, j + 1], recv_sem=strip_recv.at[0, kinds[j]],
                    device_id=(1, edge, child), device_id_type=MESH,
                )
            edge, here, _ = y_side(side)
            for i in range(-1, 4):
                lo, hi, dst = y_windows[i]
                child = 3 * (a - fx) + i
                yield here & (child >= 0) & (child < cx), pltpu.make_async_remote_copy(
                    src_ref=ypack.at[comps, pl.ds(lo, hi - lo)],
                    dst_ref=ystrip.at[comps, pl.ds(dst, hi - lo)],
                    send_sem=strip_send.at[1, i + 1], recv_sem=strip_recv.at[1, kinds[i]],
                    device_id=(1, child, edge), device_id_type=MESH,
                )

    def strip_start(comps):
        for on, copy in strip_copies(comps):
            @pl.when(on)
            def _():
                copy.start()

    def strips_sent():
        for on, copy in strip_copies(slice(0, 3)):
            @pl.when(on)
            def _():
                copy.wait_send()

    def strip_wait(axis, kind, lo, hi, dst):
        if axis == 0:
            ref = xstrip.at[:, :, pl.ds(dst, hi - lo), :]
        else:
            ref = ystrip.at[:, pl.ds(dst, hi - lo), :, :]
        pltpu.make_async_remote_copy(
            src_ref=ref, dst_ref=ref, send_sem=strip_send.at[0, 0],
            recv_sem=strip_recv.at[axis, kind], device_id=(g, a, b), device_id_type=MESH,
        ).wait_recv()

    def wait_strips(axis, place, count, windows):
        for i in range(3):
            @pl.when(place % 3 == i)
            def _():
                strip_wait(axis, 0, *windows[i])

        @pl.when((place % 3 == 2) & (place < count - 1))
        def _():
            strip_wait(axis, 1, *windows[-1])

        @pl.when((place % 3 == 0) & (place > 0))
        def _():
            strip_wait(axis, 2, *windows[3])

    def relax_at(x, y):
        gx, gy = a * nx + x, b * ny + y
        depth = jnp.minimum(
            jnp.minimum(gx, nx * cx - 1 - gx), jnp.minimum(gy, ny * cy - 1 - gy)
        ).astype(F32)
        return jnp.maximum(1.0 - depth / BAND, 0.0)

    def mixed(weights, source):
        w_high, w_low = split(weights)
        s_high, s_low = split(source)
        return dot(w_high, s_high) + (dot(w_low, s_high) + dot(w_high, s_low))

    def y_edge(col):
        shape = (nx, 8, lev)
        relax = relax_at(
            lax.broadcasted_iota(jnp.int32, shape, 0), col + lax.broadcasted_iota(jnp.int32, shape, 1)
        )
        for c in range(3):
            bound = mixed(wy[...], ystrip[c].reshape(4 * (tx + 2), lev)).reshape(shape)
            at = (c, slice(XB, XB + nx), slice(YB + col, YB + col + 8), slice(None))
            now = S[at]
            S[at] = now + relax * (bound - now)

    def x_edge(first):
        shape = (BAND, ny, lev)
        relax = relax_at(
            first + lax.broadcasted_iota(jnp.int32, shape, 0), lax.broadcasted_iota(jnp.int32, shape, 1)
        )
        for c in range(3):
            bound = mixed(wx[...], xstrip[c].reshape(3 * (ty + 16), lev)).reshape(shape)
            now = mean[c, 0:BAND]
            S[c, XB + first : XB + first + BAND, YB : YB + ny, :] = now + relax * (bound - now)

    for k in range(SUBS):
        with jax.named_scope(f"exchange{k}"):
            exchange(k)
        with jax.named_scope(f"winds{k}"):
            winds(k)
        if k == SUBS - 1:
            @pl.when(g == 1)
            def _():
                with jax.named_scope("restrict_winds"):
                    restrict((1, 2))
                fb_start(1)
                fb_start(2)

            @pl.when(g == 0)
            def _():
                strip_pack((1, 2))
                strip_start(slice(1, 3))
        with jax.named_scope(f"press{k}"):
            press(k)

    def take(i, j, comps):
        first, count = comps[0], len(comps)
        with jax.named_scope(f"piece{i}{j}{first}"):
            piece = fb.at[3 * i + j, first : first + count]
            pltpu.make_async_remote_copy(
                src_ref=piece, dst_ref=piece, send_sem=fb_send.at[0],
                recv_sem=fb_recv.at[3 * i + j, min(first, 1)], device_id=(g, a, b),
                device_id_type=MESH,
            ).wait_recv()
        for c in comps:
            got = fb[3 * i + j, c]
            parts = got.reshape(quarter, 3, ty, 128)[:, :, :, lev : lev + slot]
            guest = jnp.concatenate([parts[:, m] for m in range(3)], axis=2)

            def blend(u, count, value):
                first = XB + i * tx + u
                at = (c, slice(first, first + count), slice(YB + j * ty, YB + (j + 1) * ty), slice(None))
                now = S[at]
                S[at] = now + FEEDBACK * (value - now)

            blend(0, 3 * quarter, got[:, :, :lev])
            blend(3 * quarter, quarter, guest)

    @pl.when(g == 1)
    def _():
        with jax.named_scope("restrict_pressure"):
            restrict((0,))
        fb_start(0)
        halo_sent(SUBS - 1)
        x_low, x_high = a == 0, a == cx - 1
        y_low, y_high = b == 0, b == cy - 1

        @pl.when(x_low)
        def _():
            for c in range(3):
                mean[c, 0:BAND] = S[c, XB : XB + BAND, YB : YB + ny, :]

        @pl.when(x_high)
        def _():
            for c in range(3):
                mean[c, 0:BAND] = S[c, XB + nx - BAND : XB + nx, YB : YB + ny, :]

        @pl.when(x_low | x_high)
        def _():
            xstrip_pad = jnp.zeros((3, 3, 8, lev), F32)

            @pl.when(y_low)
            def _():
                xstrip[:, :, 0:8, :] = xstrip_pad

            if (cy - 1) % 3 == 2:

                @pl.when(y_high)
                def _():
                    xstrip[:, :, ty + 8 : ty + 16, :] = xstrip_pad

        @pl.when(y_low | y_high)
        def _():
            @pl.when(x_low)
            def _():
                ystrip[:, 0:1] = jnp.zeros((3, 1, 4, lev), F32)

            if (cx - 1) % 3 == 2:

                @pl.when(x_high)
                def _():
                    ystrip[:, tx + 1 : tx + 2] = jnp.zeros((3, 1, 4, lev), F32)

            with jax.named_scope("wait_y"):
                wait_strips(1, a, cx, y_windows)

        @pl.when(y_low)
        def _():
            with jax.named_scope("y_low"):
                y_edge(0)

        @pl.when(y_high)
        def _():
            with jax.named_scope("y_high"):
                y_edge(ny - 8)

        @pl.when(x_low | x_high)
        def _():
            with jax.named_scope("wait_x"):
                wait_strips(0, b, cy, x_windows)

        @pl.when(x_low)
        def _():
            with jax.named_scope("x_low_edge"):
                x_edge(0)

        @pl.when(x_high)
        def _():
            with jax.named_scope("x_high_edge"):
                x_edge(nx - BAND)

        for part, comps in ((1, slice(1, 3)), (0, slice(0, 1))):
            piece = rst.at[comps]
            hop(piece, piece, (g, a, b), fb_send.at[part], q_recv.at[0, 0]).wait_send()

    @pl.when(g == 0)
    def _():
        strip_pack((0,))
        strip_start(slice(0, 1))
        with jax.named_scope("pass_parent"):
            pass_on()
        halo_sent(SUBS - 1)
        passed_on()
        winds_of, pressure_of = (1, 2), (0,)
        order = [((2, j), winds_of) for j in (2, 1, 0)] + [((2, j), pressure_of) for j in (2, 1, 0)]
        order += [((1, 2), winds_of)] + [((i, j), pressure_of) for i in (1, 0) for j in (2, 1, 0)]
        order += [(at, winds_of) for at in ((1, 1), (1, 0), (0, 2), (0, 1), (0, 0))]
        for (i, j), comps in order:
            there = (a >= fx) & (b >= fy) & (3 * (a - fx) + i < cx) & (3 * (b - fy) + j < cy)

            @pl.when(there)
            def _():
                take(i, j, comps)

        strips_sent()


def per_device(
    state, courant, vert_inverse, interp_index, interp_weight, restrict_index, restrict_weight
):
    cx, cy = lax.axis_size("gx"), lax.axis_size("gy")
    _, _, nx, ny, lev = state.shape
    tx, ty = nx // 3, ny // 3
    packed = (3 * (tx // 4), ty, 128)
    vmem = lambda *shape: pltpu.VMEM(shape, F32)
    dma = pltpu.SemaphoreType.DMA
    anywhere = pl.BlockSpec(memory_space=pltpu.HBM)
    inside = pl.BlockSpec(memory_space=pltpu.VMEM)
    padded = pl.pallas_call(
        functools.partial(kernel, cx, cy),
        out_shape=vmem(3, nx + 4, ny + 16, lev),
        in_specs=[anywhere] * 7,
        out_specs=inside,
        scratch_shapes=[
            vmem(nx + 2, ny + 16, lev),
            vmem(lev, 1, lev),
            pltpu.VMEM((nx, 4, ny), jnp.int32),
            vmem(nx, 4, ny),
            pltpu.VMEM((9, tx, ty), jnp.int32),
            vmem(9, tx, ty),
            vmem(3, nx, ny, lev),
            vmem(tx, 9, ty, lev),
            vmem(BAND * ny, 3 * (ty + 16)),
            vmem(nx * 8, 4 * (tx + 2)),
            vmem(2, 4, ny, lev),
            vmem(2, nx, 4, lev),
            vmem(2, 4, ny, lev),
            vmem(2, nx, 4, lev),
            vmem(SUBS - 1, 2, 2, ny, lev),
            vmem(SUBS - 1, 2, nx, 2, lev),
            vmem(SUBS - 1, 2, 2, ny, lev),
            vmem(SUBS - 1, 2, nx, 2, lev),
            vmem(3, *packed),
            vmem(9, 3, *packed),
            vmem(3, 3, ty + 16, lev),
            vmem(3, tx + 2, 4, lev),
            dma((7,)),
            dma((4,)),
            dma((2, 4)),
            dma((2, 5)),
            dma((2, 3)),
            dma((2,)),
            dma((9, 2)),
            vmem(2, *packed),
            vmem(2, *packed),
            vmem(3, 2, *packed),
            vmem(3, 3, ny, lev),
            vmem(3, nx, 4, lev),
            dma((5,)),
            dma((5, 2)),
        ],
        compiler_params=pltpu.CompilerParams(
            has_side_effects=True, collective_id=0, vmem_limit_bytes=67043328 - 4 * (3 * (nx + 4) * (ny + 16) * 128) - 2**14
        ),
        name="nest_step",
    )(
        state, courant, vert_inverse.transpose(1, 0, 2),
        interp_index.transpose(0, 2, 1), interp_weight.transpose(0, 2, 1),
        restrict_index.transpose(2, 0, 1), restrict_weight.transpose(2, 0, 1),
    )
    return padded[None, :, XB : XB + nx, YB : YB + ny, :]


def solution(mesh):
    return jax.shard_map(
        per_device,
        mesh=mesh,
        in_specs=(
            P("grp", None, "gx", "gy", None),
            P("grp", "gx", "gy", None),
            P("grp", None, None),
            P("gx", "gy", None),
            P("gx", "gy", None),
            P("gx", "gy", None),
            P("gx", "gy", None),
        ),
        out_specs=P("grp", None, "gx", "gy", None),
        check_vma=False,
    )
```

```python
import functools

import jax
import jax.numpy as jnp
from jax import lax
from jax.experimental import pallas as pl
from jax.experimental.pallas import tpu as pltpu
from jax.sharding import PartitionSpec as P

SUBS = 4
BAND = 5
FEEDBACK = 0.5
MESH = pl.DeviceIdType.MESH
F32 = jnp.float32
XB, YB = 2, 8


def split(a):
    high = a.astype(jnp.bfloat16)
    return high, (a - high.astype(F32)).astype(jnp.bfloat16)


def dot(a, b):
    return jnp.dot(a, b, preferred_element_type=F32)


def dot3(a, b_high, b_low):
    a_high, a_low = split(a)
    return dot(a_high, b_high) + (dot(a_low, b_high) + dot(a_high, b_low))


def third(t):
    return (t * 11) >> 5


def kernel(
    cx, cy,
    state, courant, *rest,
):
    small, (
    S,
    C, inverse, iidx, iwgt, ridx, rwgt, saved, racc, wr, wx, wy, sx0, sy0, rx0, ry0, sx, sy, rx, ry, rst, fb, xstrip, ystrip,
    load_sem, halo_send, halo_recv, strip_send, strip_recv, fb_send, fb_recv,
    q0, xpack, ypack, q_send, q_recv,
    ) = rest[:5], rest[5:]
    g, a, b = lax.axis_index("grp"), lax.axis_index("gx"), lax.axis_index("gy")
    nx, ny, lev = state.shape[2], state.shape[3], state.shape[4]
    tx, ty = nx // 3, ny // 3
    fx, fy = cx // 2, cy // 2
    quarter, slot = tx // 4, lev // 3

    barrier = pltpu.get_barrier_semaphore()
    greeted = []

    def greet(on, device):
        greeted.append(on)

        @pl.when(on)
        def _():
            pl.semaphore_signal(barrier, inc=1, device_id=device, device_id_type=MESH)

    greet(a > 0, (g, a - 1, b))
    greet(a < cx - 1, (g, a + 1, b))
    greet(b > 0, (g, a, b - 1))
    greet(b < cy - 1, (g, a, b + 1))
    for i in range(-1, 4):
        for j in range(-1, 4):
            child_a, child_b = 3 * (a - fx) + i, 3 * (b - fy) + j
            greet(
                (g == 0) & (a >= fx) & (b >= fy) & (child_a >= 0) & (child_a < cx)
                & (child_b >= 0) & (child_b < cy),
                (1, child_a, child_b),
            )

    def parents(place, first, count):
        own = first + place // 3
        return (
            (place >= 0, own),
            ((place % 3 == 0) & (place > 0), own - 1),
            ((place % 3 == 2) & (own + 1 < count), own + 1),
        )

    for on_a, parent_a in parents(a, fx, cx):
        for on_b, parent_b in parents(b, fy, cy):
            greet((g == 1) & on_a & on_b, (0, parent_a, parent_b))

    def route(at_a, at_b):
        to_a, to_b = fx + at_a // 3, fy + at_b // 3
        return to_a, to_b, (at_a % 3 == 0) & (at_a != to_a)

    to_a, to_b, via = route(a, b)
    parent, nest = g == 0, g == 1
    greet(nest & via, (0, a, to_b))
    relayed = []
    for j in range(3):
        from_b = 3 * (b - fy) + j
        on = parent & (b >= fy) & (from_b < cy) & via
        relayed.append(on)
        greet(on, (1, a, from_b))
    greet(relayed[0], (0, to_a, b))
    for i in range(3):
        from_a = 3 * (a - fx) + i
        greet(parent & (a >= fx) & (b >= fy) & (from_a < cx) & route(from_a, 0)[2], (0, from_a, b))

    loads = [
        pltpu.make_async_copy(
            state.at[0], S.at[:, pl.ds(XB, nx), pl.ds(YB, ny), :], load_sem.at[0]
        ),
        pltpu.make_async_copy(
            courant.at[0], C.at[pl.ds(1, nx), pl.ds(YB, ny), :], load_sem.at[1]
        ),
    ]
    for n, (src, dst) in enumerate(zip(small, (inverse, iidx, iwgt, ridx, rwgt))):
        loads.append(pltpu.make_async_copy(src, dst, load_sem.at[2 + n]))
    for copy in loads:
        copy.start()
    zrow = jnp.zeros((2, ny, lev), F32)
    S[0, 0:2, YB : YB + ny, :] = zrow
    S[0, XB + nx : XB + nx + 2, YB : YB + ny, :] = zrow
    S[1, 0:2, YB : YB + ny, :] = zrow
    S[1, XB + nx : XB + nx + 2, YB : YB + ny, :] = zrow
    C[0:1, YB : YB + ny, :] = zrow[0:1]
    C[nx + 1 : nx + 2, YB : YB + ny, :] = zrow[0:1]
    zcol = jnp.zeros((nx, 8, lev), F32)
    for c in (0, 2):
        S[c, XB : XB + nx, 0:YB, :] = zcol
        S[c, XB : XB + nx, YB + ny : YB + ny + 8, :] = zcol
    C[1 : 1 + nx, 0:YB, :] = zcol
    C[1 : 1 + nx, YB + ny : YB + ny + 8, :] = zcol
    with jax.named_scope("loads"):
        for copy in loads:
            copy.wait()
    m_high, m_low = split(inverse[:, 0, :])
    with jax.named_scope("greet"):
        pl.semaphore_wait(barrier, sum(on.astype(jnp.int32) for on in greeted))

    dirs = (
        (a > 0, a < cx - 1, (g, a - 1, b)),
        (a < cx - 1, a > 0, (g, a + 1, b)),
        (b > 0, b < cy - 1, (g, a, b - 1)),
        (b < cy - 1, b > 0, (g, a, b + 1)),
    )

    def halo_copy(k, d):
        if k == 0:
            src, dst = (sx0, rx0) if d < 2 else (sy0, ry0)
            src, dst = src.at[d % 2], dst.at[d % 2]
        else:
            src, dst = (sx, rx) if d < 2 else (sy, ry)
            src, dst = src.at[k - 1, d % 2], dst.at[k - 1, d % 2]
        return pltpu.make_async_remote_copy(
            src_ref=src, dst_ref=dst,
            send_sem=halo_send.at[d], recv_sem=halo_recv.at[k % 2, d],
            device_id=dirs[d][2], device_id_type=MESH,
        )

    def halo_sent(k):
        for d in range(4):
            @pl.when(dirs[d][0])
            def _():
                halo_copy(k, d).wait_send()

    def send_edges(k):
        cols = slice(YB, YB + ny)
        rows = slice(XB, XB + nx)
        last_x, last_y = XB + nx, YB + ny
        if k == 0:
            sx0[0, 0:2] = S[0, XB : XB + 2, cols, :]
            sx0[0, 2:3] = S[1, XB : XB + 1, cols, :]
            sx0[0, 3:4] = C[1:2, cols, :]
            sx0[1, 0:2] = S[0, last_x - 2 : last_x, cols, :]
            sx0[1, 2:3] = S[1, last_x - 1 : last_x, cols, :]
            sx0[1, 3:4] = C[nx : nx + 1, cols, :]
            sy0[0, :, 0:2] = S[0, rows, YB : YB + 2, :]
            sy0[0, :, 2:3] = S[2, rows, YB : YB + 1, :]
            sy0[0, :, 3:4] = C[1 : 1 + nx, YB : YB + 1, :]
            sy0[1, :, 0:2] = S[0, rows, last_y - 2 : last_y, :]
            sy0[1, :, 2:3] = S[2, rows, last_y - 1 : last_y, :]
            sy0[1, :, 3:4] = C[1 : 1 + nx, last_y - 1 : last_y, :]
        else:
            sx[k - 1, 0] = S[0, XB : XB + 2, cols, :]
            sx[k - 1, 1] = S[0, last_x - 2 : last_x, cols, :]
            sy[k - 1, 0] = S[0, rows, YB : YB + 2, :]
            sy[k - 1, 1] = S[0, rows, last_y - 2 : last_y, :]
        if k > 0:
            halo_sent(k - 1)
        for d in range(4):
            @pl.when(dirs[d][0])
            def _():
                halo_copy(k, d).start()

    def receive(k, which):
        cols = slice(YB, YB + ny)
        rows = slice(XB, XB + nx)
        last_x, last_y = XB + nx, YB + ny
        for d in which:
            @pl.when(dirs[d][1])
            def _():
                halo_copy(k, d).wait_recv()
                if d < 2:
                    got = rx0.at[d] if k == 0 else rx.at[k - 1, d]
                    at = last_x if d == 0 else XB - 2
                    S[0, at : at + 2, cols, :] = got[0:2]
                    if k == 0:
                        at = last_x if d == 0 else XB - 1
                        S[1, at : at + 1, cols, :] = got[2:3]
                        C[at - 1 : at, cols, :] = got[3:4]
                else:
                    got = ry0.at[d - 2] if k == 0 else ry.at[k - 1, d - 2]
                    at = last_y if d == 2 else YB - 2
                    S[0, rows, at : at + 2, :] = got[:, 0:2]
                    if k == 0:
                        at = last_y if d == 2 else YB - 1
                        S[2, rows, at : at + 1, :] = got[:, 2:3]
                        C[1 : 1 + nx, at : at + 1, :] = got[:, 3:4]

    cols = slice(YB, YB + ny)

    def u_row(r):
        slope = 0.5 * (S[0, r + 1, cols, :] - S[0, r - 1, cols, :])
        return S[1, r, cols, :] - C[r - 1, cols, :] * slope

    def v_row(r):
        mid = slice(YB + 1, YB + ny - 1)
        slope = 0.5 * (S[0, r, YB + 2 : YB + ny, :] - S[0, r, YB : YB + ny - 2, :])
        return S[2, r, mid, :] - C[r - 1, mid, :] * slope

    def inner_winds():
        group = 4

        def some(us, vs):
            new = [(1, r, cols, u_row(r)) for r in us]
            new += [(2, r, slice(YB + 1, YB + ny - 1), v_row(r)) for r in vs]
            for c, r, at, value in new:
                S[c, r, at, :] = value

        def rows(i, _):
            some(*[[XB + 2 + i * group + j for j in range(group)]] * 2)
            return 0

        first, last = XB, XB + nx - 1
        some((first + 1, last - 1), (first, first + 1, last - 1, last))
        lax.fori_loop(0, (nx - 4) // group, rows, 0)

    def edge_winds_x():
        new = [(r, u_row(r)) for r in (XB - 1, XB, XB + nx - 1, XB + nx)]
        for r, value in new:
            S[1, r, cols, :] = value

    def edge_winds_y():
        rows = slice(XB, XB + nx)
        for y in (YB - 1, YB + ny - 1):
            slope = 0.5 * (S[0, rows, y + 1 : y + 3, :] - S[0, rows, y - 1 : y + 1, :])
            S[2, rows, y : y + 2, :] = S[2, rows, y : y + 2, :] - C[1 : 1 + nx, y : y + 2, :] * slope

    def forced(r, y, width):
        at = slice(y, y + width)
        div = 0.5 * (S[1, r + 1, at, :] - S[1, r - 1, at, :]) + 0.5 * (
            S[2, r, y + 1 : y + width + 1, :] - S[2, r, y - 1 : y + width - 1, :]
        )
        return S[0, r, at, :] - C[r - 1, at, :] * div

    def solved(parts):
        return dot3(jnp.concatenate(parts, axis=0), m_high, m_low)

    def inner_pressure():
        group = 8

        def rows(i, _):
            first = XB + 2 + i * group
            new = solved([forced(first + j, YB, ny) for j in range(group)])
            for j in range(group):
                S[0, first + j, YB + 2 : YB + ny - 2, :] = new[j * ny + 2 : (j + 1) * ny - 2]
            return 0

        lax.fori_loop(0, (nx - 4) // group, rows, 0)

    def edge_pressure():
        rows = (XB, XB + 1, XB + nx - 2, XB + nx - 1)
        parts = [forced(r, YB, ny) for r in rows]
        sides = [(r, y) for y in (YB, YB + ny - 8) for r in range(XB + 2, XB + nx - 2)]
        parts += [forced(r, y, 8) for r, y in sides]
        new = solved(parts)
        for n, r in enumerate(rows):
            S[0, r, cols, :] = new[n * ny : (n + 1) * ny]
        base = len(rows) * ny
        for n, (r, y) in enumerate(sides):
            skip = 0 if y == YB else 6
            S[0, r, y + skip : y + skip + 2, :] = new[base + 8 * n + skip : base + 8 * n + skip + 2]

    def hop(src, dst, device, send, recv):
        return pltpu.make_async_remote_copy(
            src_ref=src, dst_ref=dst, send_sem=send, recv_sem=recv,
            device_id=device, device_id_type=MESH,
        )

    chunks = ((1, slice(3, 3 * quarter)), (1, slice(0, 3)), (2, slice(0, 3 * quarter)))

    def home(src, c, part, i, j, device, send):
        n = 3 * i + j
        return hop(src, fb.at[n, c, part], device, send, fb_recv.at[n, min(c, 1)])

    def pressure_home():
        whole = slice(0, 3 * quarter)
        return home(rst.at[0], 0, whole, a % 3, b % 3, (0, to_a, to_b), fb_send.at[0])

    def fb_start(n):
        c, part = chunks[n]
        mine, sem = rst.at[c, part], fb_send.at[1]

        @pl.when(jnp.logical_not(via))
        def _():
            home(mine, c, part, a % 3, b % 3, (0, to_a, to_b), sem).start()

        @pl.when(via)
        def _():
            hop(mine, q0.at[b % 3, c - 1, part], (0, a, to_b), sem, q_recv.at[b % 3, n]).start()

    def pass_on():
        for n, (c, part) in enumerate(chunks):
            for j in range(3):
                @pl.when(relayed[j])
                def _():
                    piece = q0.at[j, c - 1, part]
                    hop(piece, piece, (g, a, b), q_send.at[j], q_recv.at[j, n]).wait_recv()
                    home(piece, c, part, 0, j, (0, to_a, b), q_send.at[j]).start()

    def passed_on():
        for j in range(3):
            @pl.when(relayed[j])
            def _():
                hop(q0.at[j], q0.at[j], (g, a, b), q_send.at[j], q_recv.at[0, 0]).wait_send()

    def rows_of(i):
        if i == 0:
            return 0, tx - 1, 1, 2
        return tuple(4 * i - 1 + m for m in range(4))

    def mixed_row(c, u):
        total = None
        for t in range(9):
            part = wr[u, t] * S[c, XB + 3 * u + t // 3, pl.ds(YB + t % 3, ty, stride=3), :]
            total = part if total is None else total + part
        return total

    def gather_mean(k):
        def rows(u, _):
            new = [mixed_row(c, u) for c in range(3)]
            for c in range(3):
                racc[c, u] = new[c] if k == 0 else racc[c, u] + new[c]
            return 0

        lax.fori_loop(0, tx, rows, 0)

    def restrict(c, groups):
        spare = jnp.zeros((ty, 128 - lev - slot), F32)
        for i in groups:
            own = [racc[c, u] + mixed_row(c, u) for u in rows_of(i)]
            for m in range(3):
                part = own[3][:, m * slot : (m + 1) * slot]
                rst[c, 3 * i + m] = jnp.concatenate([own[m], part, spare], axis=1)

    def restrict_weights():
        terms = range(ridx.shape[0])
        w = [rwgt[k] for k in terms]
        scale = (1.0 / SUBS) / row_sum(w)
        shares = [part * scale for part in w]
        index = [ridx[k] for k in terms]
        for t in range(9):
            at = row_sum([jnp.where(index[k] == t, shares[k], 0.0) for k in terms]).T
            for u in range(tx):
                wr[u, t] = jnp.broadcast_to(at[:, u : u + 1], (ty, lev))

    def boundary_weights():
        share = iwgt[...] / jnp.sum(iwgt[...], axis=1, keepdims=True)
        share = share.reshape(nx * 4, ny).T
        index = iidx[...].astype(F32).reshape(nx * 4, ny).T.astype(jnp.int32)
        over = third(index)
        shape = index.shape
        x3 = (lax.broadcasted_iota(jnp.int32, shape, 1) * 171) >> 11
        y3 = (lax.broadcasted_iota(jnp.int32, shape, 0) * 171) >> 9
        source_x = jnp.clip(a * tx + x3 + over - 1, 0, cx * tx - 1)
        source_y = jnp.clip(b * ty + y3 + (index - 3 * over) - 1, 0, cy * ty - 1)

        def spread(cells, parts, x, depth):
            places = lax.broadcasted_iota(jnp.int32, (cells.shape[0], depth), 1)
            total = jnp.zeros(places.shape, F32)
            for n in range(4 * x, 4 * x + 4):
                total = total + jnp.where(places == cells[:, n : n + 1], parts[:, n : n + 1], 0.0)
            return total

        def y_weights(col, strip0):
            cells = (source_x - (a * tx - 1)) * 4 + source_y - (b * ty + strip0)
            cells, parts = cells[col : col + 8], share[col : col + 8]
            for x in range(nx):
                wy[8 * x : 8 * x + 8] = spread(cells, parts, x, 4 * (tx + 2))

        def x_weights(first, strip0):
            wide = ty + 16
            cells = (source_x - (a * tx + strip0)) * wide + source_y - (b * ty - 8)
            for i in range(BAND):
                wx[ny * i : ny * i + ny] = spread(cells, share, first + i, 3 * wide)

        @pl.when(b == 0)
        def _():
            y_weights(0, 0)

        @pl.when(b == cy - 1)
        def _():
            y_weights(ny - 8, ty - 4)

        @pl.when(a == 0)
        def _():
            x_weights(0, 0)

        @pl.when(a == cx - 1)
        def _():
            x_weights(nx - BAND, tx - 3)

    def row_sum(rows):
        total = rows[0]
        for row in rows[1:]:
            total = total + row
        return total

    x_windows = {-1: (0, 8, 24), 0: (0, ty + 8, 8), 1: (ty - 8, 2 * ty + 8, 0),
                 2: (2 * ty - 8, ny, 0), 3: (ny - 8, ny, 0)}
    y_windows = {-1: (0, 1, tx + 1), 0: (0, tx + 1, 1), 1: (tx - 1, 2 * tx + 1, 0),
                 2: (2 * tx - 1, nx, 0), 3: (nx - 1, nx, 0)}
    kinds = {-1: 1, 0: 0, 1: 0, 2: 0, 3: 2}

    def x_side(side):
        edge = 0 if side == 0 else cx - 1
        at = XB if side == 0 else XB + tx * (edge % 3) + tx - 3
        return edge, (a == fx + edge // 3) & (b >= fy), at

    def y_side(side):
        edge = 0 if side == 0 else cy - 1
        at = YB if side == 0 else YB + ty * (edge % 3) + ty - 4
        return edge, (b == fy + edge // 3) & (a >= fx), at

    def strip_pack(comps):
        for side in range(2):
            _, on, x_at = x_side(side)

            @pl.when(on)
            def _():
                for c in comps:
                    xpack[c] = S[c, x_at : x_at + 3, YB : YB + ny, :]

            _, on, y_at = y_side(side)

            @pl.when(on)
            def _():
                for c in comps:
                    ypack[c] = S[c, XB : XB + nx, y_at : y_at + 4, :]

    def strip_copies(comps):
        for side in range(2):
            edge, here, _ = x_side(side)
            for j in range(-1, 4):
                lo, hi, dst = x_windows[j]
                child = 3 * (b - fy) + j
                yield here & (child >= 0) & (child < cy), pltpu.make_async_remote_copy(
                    src_ref=xpack.at[comps, :, pl.ds(lo, hi - lo), :],
                    dst_ref=xstrip.at[comps, :, pl.ds(dst, hi - lo), :],
                    send_sem=strip_send.at[0, j + 1], recv_sem=strip_recv.at[0, kinds[j]],
                    device_id=(1, edge, child), device_id_type=MESH,
                )
            edge, here, _ = y_side(side)
            for i in range(-1, 4):
                lo, hi, dst = y_windows[i]
                child = 3 * (a - fx) + i
                yield here & (child >= 0) & (child < cx), pltpu.make_async_remote_copy(
                    src_ref=ypack.at[comps, pl.ds(lo, hi - lo)],
                    dst_ref=ystrip.at[comps, pl.ds(dst, hi - lo)],
                    send_sem=strip_send.at[1, i + 1], recv_sem=strip_recv.at[1, kinds[i]],
                    device_id=(1, child, edge), device_id_type=MESH,
                )

    def strip_start(comps):
        for on, copy in strip_copies(comps):
            @pl.when(on)
            def _():
                copy.start()

    def strips_sent():
        for on, copy in strip_copies(slice(0, 3)):
            @pl.when(on)
            def _():
                copy.wait_send()

    def strip_wait(axis, kind, lo, hi, dst):
        if axis == 0:
            ref = xstrip.at[:, :, pl.ds(dst, hi - lo), :]
        else:
            ref = ystrip.at[:, pl.ds(dst, hi - lo), :, :]
        pltpu.make_async_remote_copy(
            src_ref=ref, dst_ref=ref, send_sem=strip_send.at[0, 0],
            recv_sem=strip_recv.at[axis, kind], device_id=(g, a, b), device_id_type=MESH,
        ).wait_recv()

    def wait_strips(axis, place, count, windows):
        for i in range(3):
            @pl.when(place % 3 == i)
            def _():
                strip_wait(axis, 0, *windows[i])

        @pl.when((place % 3 == 2) & (place < count - 1))
        def _():
            strip_wait(axis, 1, *windows[-1])

        @pl.when((place % 3 == 0) & (place > 0))
        def _():
            strip_wait(axis, 2, *windows[3])

    def relax_at(x, y):
        gx, gy = a * nx + x, b * ny + y
        depth = jnp.minimum(
            jnp.minimum(gx, nx * cx - 1 - gx), jnp.minimum(gy, ny * cy - 1 - gy)
        ).astype(F32)
        return jnp.maximum(1.0 - depth / BAND, 0.0)

    def mixed(weights, source):
        w_high, w_low = split(weights)
        s_high, s_low = split(source)
        return dot(w_high, s_high) + (dot(w_low, s_high) + dot(w_high, s_low))

    def y_edge(col):
        shape = (nx, 8, lev)
        relax = relax_at(
            lax.broadcasted_iota(jnp.int32, shape, 0), col + lax.broadcasted_iota(jnp.int32, shape, 1)
        )
        for c in range(3):
            bound = mixed(wy[...], ystrip[c].reshape(4 * (tx + 2), lev)).reshape(shape)
            at = (c, slice(XB, XB + nx), slice(YB + col, YB + col + 8), slice(None))
            now = S[at]
            S[at] = now + relax * (bound - now)

    def x_edge(first):
        shape = (BAND, ny, lev)
        relax = relax_at(
            first + lax.broadcasted_iota(jnp.int32, shape, 0), lax.broadcasted_iota(jnp.int32, shape, 1)
        )
        for c in range(3):
            bound = mixed(wx[...], xstrip[c].reshape(3 * (ty + 16), lev)).reshape(shape)
            now = saved[c]
            S[c, XB + first : XB + first + BAND, YB : YB + ny, :] = now + relax * (bound - now)

    for k in range(SUBS):
        with jax.named_scope(f"send{k}"):
            send_edges(k)

        @pl.when(g == 1)
        def _():
            if k == 0:
                with jax.named_scope("restrict_weights"):
                    restrict_weights()
            else:
                with jax.named_scope(f"mean{k}"):
                    gather_mean(k - 1)

        last = k == SUBS - 1
        with jax.named_scope(f"inner_winds{k}"):
            inner_winds()
        if last:
            @pl.when(g == 1)
            def _():
                with jax.named_scope("restrict_u"):
                    restrict(1, range(1, quarter))
                fb_start(0)

        with jax.named_scope(f"inner_pressure{k}"):
            inner_pressure()
        if k == 1:
            @pl.when((g == 1) & ((a == 0) | (a == cx - 1) | (b == 0) | (b == cy - 1)))
            def _():
                with jax.named_scope("boundary_weights"):
                    boundary_weights()
        with jax.named_scope(f"receive_y{k}"):
            receive(k, (2, 3))
        edge_winds_y()
        if last:
            @pl.when(g == 1)
            def _():
                with jax.named_scope("restrict_v"):
                    restrict(2, range(quarter))
                fb_start(2)

            @pl.when(g == 0)
            def _():
                strip_pack((2,))
                strip_start(slice(2, 3))
        with jax.named_scope(f"receive_x{k}"):
            receive(k, (0, 1))
        edge_winds_x()
        if last:
            @pl.when(g == 1)
            def _():
                restrict(1, (0,))
                fb_start(1)

            @pl.when(g == 0)
            def _():
                strip_pack((1,))
                strip_start(slice(1, 2))
        with jax.named_scope(f"edge_pressure{k}"):
            edge_pressure()

    def take(i, j, comps):
        first, count = comps[0], len(comps)
        with jax.named_scope(f"piece{i}{j}{first}"):
            piece = fb.at[3 * i + j, first : first + count]
            pltpu.make_async_remote_copy(
                src_ref=piece, dst_ref=piece, send_sem=fb_send.at[0],
                recv_sem=fb_recv.at[3 * i + j, min(first, 1)], device_id=(g, a, b),
                device_id_type=MESH,
            ).wait_recv()
        for c in comps:
            for n in range(quarter):
                got = fb[3 * i + j, c, 3 * n : 3 * n + 3]
                rows = [got[m, :, :lev] for m in range(3)]
                rows.append(jnp.concatenate([got[m, :, lev : lev + slot] for m in range(3)], axis=1))
                for u, value in zip(rows_of(n), rows):
                    at = (c, XB + i * tx + u, slice(YB + j * ty, YB + (j + 1) * ty), slice(None))
                    now = S[at]
                    S[at] = now + FEEDBACK * (value - now)

    @pl.when(g == 1)
    def _():
        with jax.named_scope("restrict_pressure"):
            restrict(0, range(quarter))
        pressure_home().start()
        halo_sent(SUBS - 1)
        x_low, x_high = a == 0, a == cx - 1
        y_low, y_high = b == 0, b == cy - 1

        @pl.when(x_low)
        def _():
            for c in range(3):
                saved[c] = S[c, XB : XB + BAND, YB : YB + ny, :]

        @pl.when(x_high)
        def _():
            for c in range(3):
                saved[c] = S[c, XB + nx - BAND : XB + nx, YB : YB + ny, :]

        @pl.when(x_low | x_high)
        def _():
            xstrip_pad = jnp.zeros((3, 3, 8, lev), F32)

            @pl.when(y_low)
            def _():
                xstrip[:, :, 0:8, :] = xstrip_pad

            if (cy - 1) % 3 == 2:

                @pl.when(y_high)
                def _():
                    xstrip[:, :, ty + 8 : ty + 16, :] = xstrip_pad

        @pl.when(y_low | y_high)
        def _():
            @pl.when(x_low)
            def _():
                ystrip[:, 0:1] = jnp.zeros((3, 1, 4, lev), F32)

            if (cx - 1) % 3 == 2:

                @pl.when(x_high)
                def _():
                    ystrip[:, tx + 1 : tx + 2] = jnp.zeros((3, 1, 4, lev), F32)

            with jax.named_scope("wait_y"):
                wait_strips(1, a, cx, y_windows)

        @pl.when(y_low)
        def _():
            with jax.named_scope("y_low"):
                y_edge(0)

        @pl.when(y_high)
        def _():
            with jax.named_scope("y_high"):
                y_edge(ny - 8)

        @pl.when(x_low | x_high)
        def _():
            with jax.named_scope("wait_x"):
                wait_strips(0, b, cy, x_windows)

        @pl.when(x_low)
        def _():
            with jax.named_scope("x_low_edge"):
                x_edge(0)

        @pl.when(x_high)
        def _():
            with jax.named_scope("x_high_edge"):
                x_edge(nx - BAND)

        for part, comps in ((1, slice(1, 3)), (0, slice(0, 1))):
            piece = rst.at[comps]
            hop(piece, piece, (g, a, b), fb_send.at[part], q_recv.at[0, 0]).wait_send()

    @pl.when(g == 0)
    def _():
        strip_pack((0,))
        strip_start(slice(0, 1))
        with jax.named_scope("pass_parent"):
            pass_on()
        halo_sent(SUBS - 1)
        passed_on()
        winds_of, pressure_of = (1, 2), (0,)
        near = [(i, j) for i in (2, 1) for j in (2, 1, 0)]
        far = [(0, j) for j in (2, 1, 0)]
        order = [(at, winds_of) for at in near] + [(at, pressure_of) for at in near + far]
        order += [(at, winds_of) for at in far]
        for (i, j), comps in order:
            there = (a >= fx) & (b >= fy) & (3 * (a - fx) + i < cx) & (3 * (b - fy) + j < cy)

            @pl.when(there)
            def _():
                take(i, j, comps)

        strips_sent()


def per_device(
    state, courant, vert_inverse, interp_index, interp_weight, restrict_index, restrict_weight
):
    cx, cy = lax.axis_size("gx"), lax.axis_size("gy")
    _, _, nx, ny, lev = state.shape
    tx, ty = nx // 3, ny // 3
    packed = (3 * (tx // 4), ty, 128)
    vmem = lambda *shape: pltpu.VMEM(shape, F32)
    dma = pltpu.SemaphoreType.DMA
    anywhere = pl.BlockSpec(memory_space=pltpu.HBM)
    inside = pl.BlockSpec(memory_space=pltpu.VMEM)
    padded = pl.pallas_call(
        functools.partial(kernel, cx, cy),
        out_shape=vmem(3, nx + 4, ny + 16, lev),
        in_specs=[anywhere] * 7,
        out_specs=inside,
        scratch_shapes=[
            vmem(nx + 2, ny + 16, lev),
            vmem(lev, 1, lev),
            pltpu.VMEM((nx, 4, ny), jnp.int32),
            vmem(nx, 4, ny),
            pltpu.VMEM((9, tx, ty), jnp.int32),
            vmem(9, tx, ty),
            vmem(3, BAND, ny, lev),
            vmem(3, tx, ty, lev),
            vmem(tx, 9, ty, lev),
            vmem(BAND * ny, 3 * (ty + 16)),
            vmem(nx * 8, 4 * (tx + 2)),
            vmem(2, 4, ny, lev),
            vmem(2, nx, 4, lev),
            vmem(2, 4, ny, lev),
            vmem(2, nx, 4, lev),
            vmem(SUBS - 1, 2, 2, ny, lev),
            vmem(SUBS - 1, 2, nx, 2, lev),
            vmem(SUBS - 1, 2, 2, ny, lev),
            vmem(SUBS - 1, 2, nx, 2, lev),
            vmem(3, *packed),
            vmem(9, 3, *packed),
            vmem(3, 3, ty + 16, lev),
            vmem(3, tx + 2, 4, lev),
            dma((7,)),
            dma((4,)),
            dma((2, 4)),
            dma((2, 5)),
            dma((2, 3)),
            dma((2,)),
            dma((9, 2)),
            vmem(3, 2, *packed),
            vmem(3, 3, ny, lev),
            vmem(3, nx, 4, lev),
            dma((3,)),
            dma((3, 3)),
        ],
        compiler_params=pltpu.CompilerParams(
            has_side_effects=True, collective_id=0, vmem_limit_bytes=67043328 - 4 * (3 * (nx + 4) * (ny + 16) * 128) - 2**14
        ),
        name="nest_step",
    )(
        state, courant, vert_inverse.transpose(1, 0, 2),
        interp_index.transpose(0, 2, 1), interp_weight.transpose(0, 2, 1),
        restrict_index.transpose(2, 0, 1), restrict_weight.transpose(2, 0, 1),
    )
    return padded[None, :, XB : XB + nx, YB : YB + ny, :]


def solution(mesh):
    return jax.shard_map(
        per_device,
        mesh=mesh,
        in_specs=(
            P("grp", None, "gx", "gy", None),
            P("grp", "gx", "gy", None),
            P("grp", None, None),
            P("gx", "gy", None),
            P("gx", "gy", None),
            P("gx", "gy", None),
            P("gx", "gy", None),
        ),
        out_specs=P("grp", None, "gx", "gy", None),
        check_vma=False,
    )
```

```python
import functools

import jax
import jax.numpy as jnp
from jax import lax
from jax.experimental import pallas as pl
from jax.experimental.pallas import tpu as pltpu
from jax.sharding import PartitionSpec as P

SUBS = 4
BAND = 5
FEEDBACK = 0.5
MESH = pl.DeviceIdType.MESH
F32 = jnp.float32
XB, YB = 2, 8


def split(a):
    high = a.astype(jnp.bfloat16)
    return high, (a - high.astype(F32)).astype(jnp.bfloat16)


def dot(a, b):
    return jnp.dot(a, b, preferred_element_type=F32)


def dot3(a, b_high, b_low):
    a_high, a_low = split(a)
    return dot(a_high, b_high) + (dot(a_low, b_high) + dot(a_high, b_low))


def third(t):
    return (t * 11) >> 5


def kernel(
    cx, cy,
    state, courant, *rest,
):
    small, (
    S,
    C, inverse, iidx, iwgt, ridx, rwgt, saved, racc, wr, wx, wy, sx0, sy0, rx0, ry0, sx, sy, rx, ry, rst, fb, xstrip, xouter, ystrip,
    load_sem, halo_send, halo_recv, strip_send, strip_recv, fb_send, fb_recv,
    q0, xpack, outer, ypack, q_send, q_recv, outer_send,
    ) = rest[:5], rest[5:]
    g, a, b = lax.axis_index("grp"), lax.axis_index("gx"), lax.axis_index("gy")
    nx, ny, lev = state.shape[2], state.shape[3], state.shape[4]
    tx, ty = nx // 3, ny // 3
    fx, fy = cx // 2, cy // 2
    quarter, slot = tx // 4, lev // 3

    barrier = pltpu.get_barrier_semaphore()
    greeted = []

    def greet(on, device):
        greeted.append(on)

        @pl.when(on)
        def _():
            pl.semaphore_signal(barrier, inc=1, device_id=device, device_id_type=MESH)

    for i in range(-1, 4):
        for j in range(-1, 4):
            child_a, child_b = 3 * (a - fx) + i, 3 * (b - fy) + j
            greet(
                (g == 0) & (a >= fx) & (b >= fy) & (child_a >= 0) & (child_a < cx)
                & (child_b >= 0) & (child_b < cy),
                (1, child_a, child_b),
            )

    def parents(place, first, count):
        own = first + place // 3
        return (
            (place >= 0, own),
            ((place % 3 == 0) & (place > 0), own - 1),
            ((place % 3 == 2) & (own + 1 < count), own + 1),
        )

    for on_a, parent_a in parents(a, fx, cx):
        for on_b, parent_b in parents(b, fy, cy):
            greet((g == 1) & on_a & on_b, (0, parent_a, parent_b))

    loads = [
        pltpu.make_async_copy(
            state.at[0], S.at[:, pl.ds(XB, nx), pl.ds(YB, ny), :], load_sem.at[0]
        ),
        pltpu.make_async_copy(
            courant.at[0], C.at[pl.ds(1, nx), pl.ds(YB, ny), :], load_sem.at[1]
        ),
    ]
    for n, (src, dst) in enumerate(zip(small, (inverse, iidx, iwgt, ridx, rwgt))):
        loads.append(pltpu.make_async_copy(src, dst, load_sem.at[2 + n]))
    for copy in loads:
        copy.start()

    def relay_of(at_a):
        to_a = fx + at_a // 3
        back = (at_a % 3 == 0) & (at_a != to_a)
        on = (at_a % 3 == 2) & (to_a + 1 < cx)
        return to_a, back, on

    to_a, back, on_next = relay_of(a)
    to_b = fy + b // 3
    parent, nest = g == 0, g == 1
    via = back | on_next
    relay_a = jnp.where(back, a, to_a + 1)
    greet(nest & via, (0, relay_a, to_b))
    relayed = []
    next_a = 3 * (a - 1 - fx) + 2
    for from_a, lane, i, here in (
        (a, 0, 0, back), (next_a, 1, 2, (a - 1 >= fx) & (next_a < cx)),
    ):
        for j in range(3):
            from_b = 3 * (b - fy) + j
            on = parent & here & (b >= fy) & (from_b < cy)
            relayed.append((on, 3 * lane + j, i, j, fx + from_a // 3))
            greet(on, (1, from_a, from_b))
        greet(relayed[-3][0], (0, fx + from_a // 3, b))
    for i in range(3):
        from_a = 3 * (a - fx) + i
        on = parent & (a >= fx) & (b >= fy) & (from_a < cx)
        _, from_back, from_next = relay_of(from_a)
        greet(on & from_back, (0, from_a, b))
        greet(on & from_next, (0, a + 1, b))

    greet(a > 0, (g, a - 1, b))
    greet(a < cx - 1, (g, a + 1, b))
    greet(b > 0, (g, a, b - 1))
    greet(b < cy - 1, (g, a, b + 1))
    zrow = jnp.zeros((2, ny, lev), F32)
    S[0, 0:2, YB : YB + ny, :] = zrow
    S[0, XB + nx : XB + nx + 2, YB : YB + ny, :] = zrow
    S[1, 0:2, YB : YB + ny, :] = zrow
    S[1, XB + nx : XB + nx + 2, YB : YB + ny, :] = zrow
    C[0:1, YB : YB + ny, :] = zrow[0:1]
    C[nx + 1 : nx + 2, YB : YB + ny, :] = zrow[0:1]
    outer[...] = jnp.zeros((2, 3, 3, 4, lev), F32)
    zcol = jnp.zeros((nx, 8, lev), F32)
    for c in (0, 2):
        S[c, XB : XB + nx, 0:YB, :] = zcol
        S[c, XB : XB + nx, YB + ny : YB + ny + 8, :] = zcol
    C[1 : 1 + nx, 0:YB, :] = zcol
    C[1 : 1 + nx, YB + ny : YB + ny + 8, :] = zcol
    with jax.named_scope("loads"):
        for copy in loads:
            copy.wait()
    m_high, m_low = split(inverse[:, 0, :])
    with jax.named_scope("greet"):
        pl.semaphore_wait(barrier, sum(on.astype(jnp.int32) for on in greeted))

    dirs = (
        (a > 0, a < cx - 1, (g, a - 1, b)),
        (a < cx - 1, a > 0, (g, a + 1, b)),
        (b > 0, b < cy - 1, (g, a, b - 1)),
        (b < cy - 1, b > 0, (g, a, b + 1)),
    )

    def halo_copy(k, d):
        if k == 0:
            src, dst = (sx0, rx0) if d < 2 else (sy0, ry0)
            src, dst = src.at[d % 2], dst.at[d % 2]
        else:
            src, dst = (sx, rx) if d < 2 else (sy, ry)
            src, dst = src.at[k - 1, d % 2], dst.at[k - 1, d % 2]
        return pltpu.make_async_remote_copy(
            src_ref=src, dst_ref=dst,
            send_sem=halo_send.at[d], recv_sem=halo_recv.at[k % 2, d],
            device_id=dirs[d][2], device_id_type=MESH,
        )

    def halo_sent(k):
        for d in range(4):
            @pl.when(dirs[d][0])
            def _():
                halo_copy(k, d).wait_send()

    def send_edges(k, which):
        rows = slice(XB, XB + nx)
        last_x, last_y = XB + nx, YB + ny
        cols = slice(YB, last_y)
        if k == 0:
            sx0[0, 0:2] = S[0, XB : XB + 2, cols, :]
            sx0[0, 2:3] = S[1, XB : XB + 1, cols, :]
            sx0[0, 3:4] = C[1:2, cols, :]
            sx0[1, 0:2] = S[0, last_x - 2 : last_x, cols, :]
            sx0[1, 2:3] = S[1, last_x - 1 : last_x, cols, :]
            sx0[1, 3:4] = C[nx : nx + 1, cols, :]
            sy0[0, :, 0:2] = S[0, rows, YB : YB + 2, :]
            sy0[0, :, 2:3] = S[2, rows, YB : YB + 1, :]
            sy0[0, :, 3:4] = C[1 : 1 + nx, YB : YB + 1, :]
            sy0[1, :, 0:2] = S[0, rows, last_y - 2 : last_y, :]
            sy0[1, :, 2:3] = S[2, rows, last_y - 1 : last_y, :]
            sy0[1, :, 3:4] = C[1 : 1 + nx, last_y - 1 : last_y, :]
        elif 0 in which:
            sx[k - 1, 0] = S[0, XB : XB + 2, cols, :]
            sx[k - 1, 1] = S[0, last_x - 2 : last_x, cols, :]
        else:
            sy[k - 1, 0] = S[0, rows, YB : YB + 2, :]
            sy[k - 1, 1] = S[0, rows, last_y - 2 : last_y, :]
        for d in which:
            @pl.when(dirs[d][0])
            def _():
                if k > 0:
                    halo_copy(k - 1, d).wait_send()
                halo_copy(k, d).start()

    def receive(k, which):
        cols = slice(YB, YB + ny)
        rows = slice(XB, XB + nx)
        last_x, last_y = XB + nx, YB + ny
        for d in which:
            @pl.when(dirs[d][1])
            def _():
                halo_copy(k, d).wait_recv()
                if d < 2:
                    got = rx0.at[d] if k == 0 else rx.at[k - 1, d]
                    at = last_x if d == 0 else XB - 2
                    S[0, at : at + 2, cols, :] = got[0:2]
                    if k == 0:
                        at = last_x if d == 0 else XB - 1
                        S[1, at : at + 1, cols, :] = got[2:3]
                        C[at - 1 : at, cols, :] = got[3:4]
                else:
                    got = ry0.at[d - 2] if k == 0 else ry.at[k - 1, d - 2]
                    at = last_y if d == 2 else YB - 2
                    S[0, rows, at : at + 2, :] = got[:, 0:2]
                    if k == 0:
                        at = last_y if d == 2 else YB - 1
                        S[2, rows, at : at + 1, :] = got[:, 2:3]
                        C[1 : 1 + nx, at : at + 1, :] = got[:, 3:4]

    cols = slice(YB, YB + ny)

    def u_row(r):
        slope = 0.5 * (S[0, r + 1, cols, :] - S[0, r - 1, cols, :])
        return S[1, r, cols, :] - C[r - 1, cols, :] * slope

    def v_row(r):
        mid = slice(YB + 1, YB + ny - 1)
        slope = 0.5 * (S[0, r, YB + 2 : YB + ny, :] - S[0, r, YB : YB + ny - 2, :])
        return S[2, r, mid, :] - C[r - 1, mid, :] * slope

    def inner_winds():
        group = 4

        def some(us, vs):
            new = [(1, r, cols, u_row(r)) for r in us]
            new += [(2, r, slice(YB + 1, YB + ny - 1), v_row(r)) for r in vs]
            for c, r, at, value in new:
                S[c, r, at, :] = value

        def rows(i, _):
            some(*[[XB + 2 + i * group + j for j in range(group)]] * 2)
            return 0

        first, last = XB, XB + nx - 1
        some((first + 1, last - 1), (first, first + 1, last - 1, last))
        lax.fori_loop(0, (nx - 4) // group, rows, 0)

    def edge_winds_x():
        new = [(r, u_row(r)) for r in (XB - 1, XB, XB + nx - 1, XB + nx)]
        for r, value in new:
            S[1, r, cols, :] = value

    def edge_winds_y():
        rows = slice(XB, XB + nx)
        for y in (YB - 1, YB + ny - 1):
            slope = 0.5 * (S[0, rows, y + 1 : y + 3, :] - S[0, rows, y - 1 : y + 1, :])
            S[2, rows, y : y + 2, :] = S[2, rows, y : y + 2, :] - C[1 : 1 + nx, y : y + 2, :] * slope

    def forced(r, y, width):
        at = slice(y, y + width)
        div = 0.5 * (S[1, r + 1, at, :] - S[1, r - 1, at, :]) + 0.5 * (
            S[2, r, y + 1 : y + width + 1, :] - S[2, r, y - 1 : y + width - 1, :]
        )
        return S[0, r, at, :] - C[r - 1, at, :] * div

    def solved(parts):
        return dot3(jnp.concatenate(parts, axis=0), m_high, m_low)

    def inner_pressure():
        group = 8

        def rows(i, _):
            first = XB + 2 + i * group
            new = solved([forced(first + j, YB, ny) for j in range(group)])
            for j in range(group):
                S[0, first + j, YB + 2 : YB + ny - 2, :] = new[j * ny + 2 : (j + 1) * ny - 2]
            return 0

        lax.fori_loop(0, (nx - 4) // group, rows, 0)

    def edge_rows():
        rows = (XB, XB + 1, XB + nx - 2, XB + nx - 1)
        new = solved([forced(r, YB, ny) for r in rows])
        for n, r in enumerate(rows):
            S[0, r, cols, :] = new[n * ny : (n + 1) * ny]

    def edge_columns():
        sides = [(r, y) for y in (YB, YB + ny - 8) for r in range(XB + 2, XB + nx - 2)]
        new = solved([forced(r, y, 8) for r, y in sides])
        for n, (r, y) in enumerate(sides):
            skip = 0 if y == YB else 6
            S[0, r, y + skip : y + skip + 2, :] = new[8 * n + skip : 8 * n + skip + 2]

    def hop(src, dst, device, send, recv):
        return pltpu.make_async_remote_copy(
            src_ref=src, dst_ref=dst, send_sem=send, recv_sem=recv,
            device_id=device, device_id_type=MESH,
        )

    chunks = ((1, slice(3, 3 * quarter)), (2, slice(0, 3 * quarter)), (1, slice(0, 3)))

    def home(src, c, part, i, j, device, send):
        n = 3 * i + j
        return hop(src, fb.at[n, c, part], device, send, fb_recv.at[n, min(c, 1)])

    def pressure_home():
        whole = slice(0, 3 * quarter)
        return home(rst.at[0], 0, whole, a % 3, b % 3, (0, to_a, to_b), fb_send.at[0])

    def fb_start(n):
        c, part = chunks[n]
        mine, sem = rst.at[c, part], fb_send.at[1]
        around = via if n < 2 else back

        @pl.when(jnp.logical_not(around))
        def _():
            home(mine, c, part, a % 3, b % 3, (0, to_a, to_b), sem).start()

        @pl.when(around)
        def _():
            at = jnp.where(back, 0, 3) + b % 3
            hop(mine, q0.at[at, c - 1, part], (0, relay_a, to_b), sem, q_recv.at[at, n]).start()

    def pass_on():
        for n, (c, part) in enumerate(chunks):
            for on, at, i, j, home_a in relayed[: 6 if n < 2 else 3]:
                @pl.when(on)
                def _():
                    piece = q0.at[at, c - 1, part]
                    hop(piece, piece, (g, a, b), q_send.at[at], q_recv.at[at, n]).wait_recv()
                    home(piece, c, part, i, j, (0, home_a, b), q_send.at[at]).start()

    def passed_on():
        for on, at, _, _, _ in relayed:
            @pl.when(on)
            def _():
                sent = [q0.at[at]] if at < 3 else [q0.at[at, 0, chunks[0][1]], q0.at[at, 1]]
                for piece in sent:
                    hop(piece, piece, (g, a, b), q_send.at[at], q_recv.at[0, 0]).wait_send()

    def rows_of(i):
        if i == 0:
            return 0, tx - 1, 1, 2
        return tuple(4 * i - 1 + m for m in range(4))

    def mixed_row(c, u):
        total = None
        for t in range(9):
            part = wr[u, t] * S[c, XB + 3 * u + t // 3, pl.ds(YB + t % 3, ty, stride=3), :]
            total = part if total is None else total + part
        return total

    def gather_mean(k):
        def rows(u, _):
            new = [mixed_row(c, u) for c in range(3)]
            for c in range(3):
                racc[c, u] = new[c] if k == 0 else racc[c, u] + new[c]
            return 0

        lax.fori_loop(0, tx, rows, 0)

    def restrict(c, groups):
        spare = jnp.zeros((ty, 128 - lev - slot), F32)
        for i in groups:
            own = [racc[c, u] + mixed_row(c, u) for u in rows_of(i)]
            for m in range(3):
                part = own[3][:, m * slot : (m + 1) * slot]
                rst[c, 3 * i + m] = jnp.concatenate([own[m], part, spare], axis=1)

    def restrict_weights():
        terms = range(ridx.shape[0])
        w = [rwgt[k] for k in terms]
        scale = (1.0 / SUBS) / row_sum(w)
        shares = [part * scale for part in w]
        index = [ridx[k] for k in terms]
        for t in range(9):
            at = row_sum([jnp.where(index[k] == t, shares[k], 0.0) for k in terms]).T
            for u in range(tx):
                wr[u, t] = jnp.broadcast_to(at[:, u : u + 1], (ty, lev))

    def boundary_weights():
        share = iwgt[...] / jnp.sum(iwgt[...], axis=1, keepdims=True)
        share = share.reshape(nx * 4, ny).T
        index = iidx[...].astype(F32).reshape(nx * 4, ny).T.astype(jnp.int32)
        over = third(index)
        shape = index.shape
        x3 = (lax.broadcasted_iota(jnp.int32, shape, 1) * 171) >> 11
        y3 = (lax.broadcasted_iota(jnp.int32, shape, 0) * 171) >> 9
        source_x = jnp.clip(a * tx + x3 + over - 1, 0, cx * tx - 1)
        source_y = jnp.clip(b * ty + y3 + (index - 3 * over) - 1, 0, cy * ty - 1)

        def spread(cells, parts, x, depth):
            places = lax.broadcasted_iota(jnp.int32, (cells.shape[0], depth), 1)
            total = jnp.zeros(places.shape, F32)
            for n in range(4 * x, 4 * x + 4):
                total = total + jnp.where(places == cells[:, n : n + 1], parts[:, n : n + 1], 0.0)
            return total

        def y_weights(col, strip0):
            cells = (source_x - (a * tx - 1)) * 4 + source_y - (b * ty + strip0)
            cells, parts = cells[col : col + 8], share[col : col + 8]
            for x in range(nx):
                wy[8 * x : 8 * x + 8] = spread(cells, parts, x, 4 * (tx + 2))

        def x_weights(first, strip0):
            row, column = source_x - (a * tx + strip0), source_y - b * ty
            cells = jnp.where(
                column < 0, 3 * ty + row, jnp.where(column < ty, row * ty + column, 3 * ty + 4 + row)
            )
            for i in range(BAND):
                wx[ny * i : ny * i + ny] = spread(cells, share, first + i, 3 * ty + 8)

        @pl.when(b == 0)
        def _():
            y_weights(0, 0)

        @pl.when(b == cy - 1)
        def _():
            y_weights(ny - 8, ty - 4)

        @pl.when(a == 0)
        def _():
            x_weights(0, 0)

        @pl.when(a == cx - 1)
        def _():
            x_weights(nx - BAND, tx - 3)

    def row_sum(rows):
        total = rows[0]
        for row in rows[1:]:
            total = total + row
        return total

    y_windows = {-1: (0, 1, tx + 1), 0: (0, tx + 1, 1), 1: (tx - 1, 2 * tx + 1, 0),
                 2: (2 * tx - 1, nx, 0), 3: (nx - 1, nx, 0)}
    kinds = {-1: 1, 0: 0, 1: 0, 2: 0, 3: 2}

    def x_side(side):
        edge = 0 if side == 0 else cx - 1
        at = XB if side == 0 else XB + tx * (edge % 3) + tx - 3
        return edge, (a == fx + edge // 3) & (b >= fy), at

    def y_side(side):
        edge = 0 if side == 0 else cy - 1
        at = YB if side == 0 else YB + ty * (edge % 3) + ty - 4
        return edge, (b == fy + edge // 3) & (a >= fx), at

    def strip_pack(comps):
        for side in range(2):
            _, on, x_at = x_side(side)

            @pl.when(on)
            def _():
                for c in comps:
                    xpack[c] = S[c, x_at : x_at + 3, YB : YB + ny, :]
                    for j in range(3):
                        for side_y, y in ((1, j * ty), (0, j * ty + ty - 1)):
                            outer[side_y, j, c, 0:3] = S[c, x_at : x_at + 3, YB + y, :]

            _, on, y_at = y_side(side)

            @pl.when(on)
            def _():
                for c in comps:
                    ypack[c] = S[c, XB : XB + nx, y_at : y_at + 4, :]

    def strip_copies(comps):
        for side in range(2):
            edge, here, _ = x_side(side)
            for j in range(3):
                child = 3 * (b - fy) + j
                yield here & (child < cy), pltpu.make_async_remote_copy(
                    src_ref=xpack.at[comps, :, pl.ds(j * ty, ty), :], dst_ref=xstrip.at[comps],
                    send_sem=strip_send.at[0, j], recv_sem=strip_recv.at[0, 0],
                    device_id=(1, edge, child), device_id_type=MESH,
                )
                if comps.start > 0:
                    continue
                for side_y, beside in ((0, child + 1), (1, child - 1)):
                    yield here & (child < cy) & (beside >= 0) & (beside < cy), pltpu.make_async_remote_copy(
                        src_ref=outer.at[side_y, j], dst_ref=xouter.at[side_y],
                        send_sem=outer_send.at[side_y, j], recv_sem=strip_recv.at[0, 1 + side_y],
                        device_id=(1, edge, beside), device_id_type=MESH,
                    )
            edge, here, _ = y_side(side)
            for i in range(-1, 4):
                lo, hi, dst = y_windows[i]
                child = 3 * (a - fx) + i
                yield here & (child >= 0) & (child < cx), pltpu.make_async_remote_copy(
                    src_ref=ypack.at[comps, pl.ds(lo, hi - lo)],
                    dst_ref=ystrip.at[comps, pl.ds(dst, hi - lo)],
                    send_sem=strip_send.at[1, i + 1], recv_sem=strip_recv.at[1, kinds[i]],
                    device_id=(1, child, edge), device_id_type=MESH,
                )

    def strip_start(comps):
        for on, copy in strip_copies(comps):
            @pl.when(on)
            def _():
                copy.start()

    def strips_sent():
        for on, copy in strip_copies(slice(0, 3)):
            @pl.when(on)
            def _():
                copy.wait_send()

    def strip_wait(ref, kind):
        pltpu.make_async_remote_copy(
            src_ref=ref, dst_ref=ref, send_sem=strip_send.at[0, 0],
            recv_sem=strip_recv.at[kind], device_id=(g, a, b), device_id_type=MESH,
        ).wait_recv()

    def wait_y_strips():
        def rows(kind, lo, hi, dst):
            strip_wait(ystrip.at[:, pl.ds(dst, hi - lo), :, :], (1, kind))

        for i in range(3):
            @pl.when(a % 3 == i)
            def _():
                rows(0, *y_windows[i])

        @pl.when((a % 3 == 2) & (a < cx - 1))
        def _():
            rows(1, *y_windows[-1])

        @pl.when((a % 3 == 0) & (a > 0))
        def _():
            rows(2, *y_windows[3])

    def wait_x_strips():
        strip_wait(xstrip, (0, 0))

        @pl.when(b > 0)
        def _():
            strip_wait(xouter.at[0], (0, 1))

        @pl.when(b < cy - 1)
        def _():
            strip_wait(xouter.at[1], (0, 2))

    def relax_at(x, y):
        gx, gy = a * nx + x, b * ny + y
        depth = jnp.minimum(
            jnp.minimum(gx, nx * cx - 1 - gx), jnp.minimum(gy, ny * cy - 1 - gy)
        ).astype(F32)
        return jnp.maximum(1.0 - depth / BAND, 0.0)

    def mixed(weights, source):
        w_high, w_low = split(weights)
        s_high, s_low = split(source)
        return dot(w_high, s_high) + (dot(w_low, s_high) + dot(w_high, s_low))

    def y_edge(col):
        shape = (nx, 8, lev)
        relax = relax_at(
            lax.broadcasted_iota(jnp.int32, shape, 0), col + lax.broadcasted_iota(jnp.int32, shape, 1)
        )
        for c in range(3):
            bound = mixed(wy[...], ystrip[c].reshape(4 * (tx + 2), lev)).reshape(shape)
            at = (c, slice(XB, XB + nx), slice(YB + col, YB + col + 8), slice(None))
            now = S[at]
            S[at] = now + relax * (bound - now)

    def x_edge(first):
        shape = (BAND, ny, lev)
        relax = relax_at(
            first + lax.broadcasted_iota(jnp.int32, shape, 0), lax.broadcasted_iota(jnp.int32, shape, 1)
        )
        for c in range(3):
            source = jnp.concatenate(
                [xstrip[c].reshape(3 * ty, lev), xouter[0, c], xouter[1, c]], axis=0
            )
            bound = mixed(wx[...], source).reshape(shape)
            now = saved[c]
            S[c, XB + first : XB + first + BAND, YB : YB + ny, :] = now + relax * (bound - now)

    for k in range(SUBS):
        if k == 0:
            send_edges(0, (0, 1, 2, 3))

        @pl.when(g == 1)
        def _():
            if k == 0:
                with jax.named_scope("restrict_weights"):
                    restrict_weights()
            else:
                with jax.named_scope(f"mean{k}"):
                    gather_mean(k - 1)

        last = k == SUBS - 1
        with jax.named_scope(f"inner_winds{k}"):
            inner_winds()
        if last:
            @pl.when(g == 1)
            def _():
                with jax.named_scope("restrict_u"):
                    restrict(1, range(1, quarter))
                fb_start(0)

        with jax.named_scope(f"inner_pressure{k}"):
            inner_pressure()
        if k == 1:
            @pl.when((g == 1) & ((a == 0) | (a == cx - 1) | (b == 0) | (b == cy - 1)))
            def _():
                with jax.named_scope("boundary_weights"):
                    boundary_weights()
        with jax.named_scope(f"receive_y{k}"):
            receive(k, (2, 3))
        edge_winds_y()
        if last:
            @pl.when(g == 1)
            def _():
                with jax.named_scope("restrict_v"):
                    restrict(2, range(quarter))
                fb_start(1)

            @pl.when(g == 0)
            def _():
                strip_pack((2,))
                strip_start(slice(2, 3))
        with jax.named_scope(f"receive_x{k}"):
            receive(k, (0, 1))
        edge_winds_x()
        if last:
            @pl.when(g == 1)
            def _():
                restrict(1, (0,))
                fb_start(2)

            @pl.when(g == 0)
            def _():
                strip_pack((1,))
                strip_start(slice(1, 2))
        with jax.named_scope(f"edge_rows{k}"):
            edge_rows()
            if not last:
                send_edges(k + 1, (0, 1))
        with jax.named_scope(f"edge_columns{k}"):
            edge_columns()
            if not last:
                send_edges(k + 1, (2, 3))

    def take(i, j, comps):
        first, count = comps[0], len(comps)
        with jax.named_scope(f"piece{i}{j}{first}"):
            piece = fb.at[3 * i + j, first : first + count]
            pltpu.make_async_remote_copy(
                src_ref=piece, dst_ref=piece, send_sem=fb_send.at[0],
                recv_sem=fb_recv.at[3 * i + j, min(first, 1)], device_id=(g, a, b),
                device_id_type=MESH,
            ).wait_recv()
        for c in comps:
            for n in range(quarter):
                got = fb[3 * i + j, c, 3 * n : 3 * n + 3]
                rows = [got[m, :, :lev] for m in range(3)]
                rows.append(jnp.concatenate([got[m, :, lev : lev + slot] for m in range(3)], axis=1))
                for u, value in zip(rows_of(n), rows):
                    at = (c, XB + i * tx + u, slice(YB + j * ty, YB + (j + 1) * ty), slice(None))
                    now = S[at]
                    S[at] = now + FEEDBACK * (value - now)

    @pl.when(g == 1)
    def _():
        with jax.named_scope("restrict_pressure"):
            restrict(0, range(quarter))
        pressure_home().start()
        halo_sent(SUBS - 1)
        x_low, x_high = a == 0, a == cx - 1
        y_low, y_high = b == 0, b == cy - 1

        @pl.when(x_low)
        def _():
            for c in range(3):
                saved[c] = S[c, XB : XB + BAND, YB : YB + ny, :]

        @pl.when(x_high)
        def _():
            for c in range(3):
                saved[c] = S[c, XB + nx - BAND : XB + nx, YB : YB + ny, :]

        @pl.when(x_low | x_high)
        def _():
            @pl.when(y_low)
            def _():
                xouter[0] = jnp.zeros((3, 4, lev), F32)

            @pl.when(y_high)
            def _():
                xouter[1] = jnp.zeros((3, 4, lev), F32)

        @pl.when(y_low | y_high)
        def _():
            @pl.when(x_low)
            def _():
                ystrip[:, 0:1] = jnp.zeros((3, 1, 4, lev), F32)

            if (cx - 1) % 3 == 2:

                @pl.when(x_high)
                def _():
                    ystrip[:, tx + 1 : tx + 2] = jnp.zeros((3, 1, 4, lev), F32)

            with jax.named_scope("wait_y"):
                wait_y_strips()

        @pl.when(y_low)
        def _():
            with jax.named_scope("y_low"):
                y_edge(0)

        @pl.when(y_high)
        def _():
            with jax.named_scope("y_high"):
                y_edge(ny - 8)

        @pl.when(x_low | x_high)
        def _():
            with jax.named_scope("wait_x"):
                wait_x_strips()

        @pl.when(x_low)
        def _():
            with jax.named_scope("x_low_edge"):
                x_edge(0)

        @pl.when(x_high)
        def _():
            with jax.named_scope("x_high_edge"):
                x_edge(nx - BAND)

        for part, comps in ((1, slice(1, 3)), (0, slice(0, 1))):
            piece = rst.at[comps]
            hop(piece, piece, (g, a, b), fb_send.at[part], q_recv.at[0, 0]).wait_send()

    @pl.when(g == 0)
    def _():
        strip_pack((0,))
        strip_start(slice(0, 1))
        with jax.named_scope("pass_parent"):
            pass_on()
        halo_sent(SUBS - 1)
        passed_on()
        winds_of, pressure_of = (1, 2), (0,)
        tiles = [[(i, j) for j in (2, 0, 1)] for i in range(3)]
        order = [(at, winds_of) for at in tiles[1]] + [(at, pressure_of) for at in tiles[1]]
        order += [(at, winds_of) for at in tiles[2]] + [(at, pressure_of) for at in tiles[0]]
        order += [(at, pressure_of) for at in tiles[2][:2]] + [(at, winds_of) for at in tiles[0]]
        order += [(at, pressure_of) for at in tiles[2][2:]]
        for (i, j), comps in order:
            there = (a >= fx) & (b >= fy) & (3 * (a - fx) + i < cx) & (3 * (b - fy) + j < cy)

            @pl.when(there)
            def _():
                take(i, j, comps)

        strips_sent()


def per_device(
    state, courant, vert_inverse, interp_index, interp_weight, restrict_index, restrict_weight
):
    cx, cy = lax.axis_size("gx"), lax.axis_size("gy")
    _, _, nx, ny, lev = state.shape
    tx, ty = nx // 3, ny // 3
    packed = (3 * (tx // 4), ty, 128)
    vmem = lambda *shape: pltpu.VMEM(shape, F32)
    dma = pltpu.SemaphoreType.DMA
    anywhere = pl.BlockSpec(memory_space=pltpu.HBM)
    inside = pl.BlockSpec(memory_space=pltpu.VMEM)
    padded = pl.pallas_call(
        functools.partial(kernel, cx, cy),
        out_shape=vmem(3, nx + 4, ny + 16, lev),
        in_specs=[anywhere] * 7,
        out_specs=inside,
        scratch_shapes=[
            vmem(nx + 2, ny + 16, lev),
            vmem(lev, 1, lev),
            pltpu.VMEM((nx, 4, ny), jnp.int32),
            vmem(nx, 4, ny),
            pltpu.VMEM((9, tx, ty), jnp.int32),
            vmem(9, tx, ty),
            vmem(3, BAND, ny, lev),
            vmem(3, tx, ty, lev),
            vmem(tx, 9, ty, lev),
            vmem(BAND * ny, 3 * ty + 8),
            vmem(nx * 8, 4 * (tx + 2)),
            vmem(2, 4, ny, lev),
            vmem(2, nx, 4, lev),
            vmem(2, 4, ny, lev),
            vmem(2, nx, 4, lev),
            vmem(SUBS - 1, 2, 2, ny, lev),
            vmem(SUBS - 1, 2, nx, 2, lev),
            vmem(SUBS - 1, 2, 2, ny, lev),
            vmem(SUBS - 1, 2, nx, 2, lev),
            vmem(3, *packed),
            vmem(9, 3, *packed),
            vmem(3, 3, ty, lev),
            vmem(2, 3, 4, lev),
            vmem(3, tx + 2, 4, lev),
            dma((7,)),
            dma((4,)),
            dma((2, 4)),
            dma((2, 5)),
            dma((2, 3)),
            dma((2,)),
            dma((9, 2)),
            vmem(6, 2, *packed),
            vmem(3, 3, ny, lev),
            vmem(2, 3, 3, 4, lev),
            vmem(3, nx, 4, lev),
            dma((6,)),
            dma((6, 3)),
            dma((2, 3)),
        ],
        compiler_params=pltpu.CompilerParams(
            has_side_effects=True, collective_id=0, vmem_limit_bytes=67043328 - 4 * (3 * (nx + 4) * (ny + 16) * 128) - 2**14
        ),
        name="nest_step",
    )(
        state, courant, vert_inverse.transpose(1, 0, 2),
        interp_index.transpose(0, 2, 1), interp_weight.transpose(0, 2, 1),
        restrict_index.transpose(2, 0, 1), restrict_weight.transpose(2, 0, 1),
    )
    return padded[None, :, XB : XB + nx, YB : YB + ny, :]


def solution(mesh):
    return jax.shard_map(
        per_device,
        mesh=mesh,
        in_specs=(
            P("grp", None, "gx", "gy", None),
            P("grp", "gx", "gy", None),
            P("grp", None, None),
            P("gx", "gy", None),
            P("gx", "gy", None),
            P("gx", "gy", None),
            P("gx", "gy", None),
        ),
        out_specs=P("grp", None, "gx", "gy", None),
        check_vma=False,
    )
```

```python
import functools

import jax
import jax.numpy as jnp
from jax import lax
from jax.experimental import pallas as pl
from jax.experimental.pallas import tpu as pltpu
from jax.sharding import PartitionSpec as P

SUBS = 4
BAND = 5
FEEDBACK = 0.5
MESH = pl.DeviceIdType.MESH
F32 = jnp.float32
XB, YB = 2, 8


def split(a):
    high = a.astype(jnp.bfloat16)
    return high, (a - high.astype(F32)).astype(jnp.bfloat16)


def dot(a, b):
    return jnp.dot(a, b, preferred_element_type=F32)


def dot3(a, b_high, b_low):
    a_high, a_low = split(a)
    return dot(a_high, b_high) + (dot(a_low, b_high) + dot(a_high, b_low))


def third(t):
    return (t * 11) >> 5


def kernel(
    cx, cy,
    state, courant, *rest,
):
    small, (
    S,
    C, inverse, iidx, iwgt, ridx, rwgt, saved, racc, wr, wx, wy, sx0, sy0, rx0, ry0, sx, sy, rx, ry, rst, fb, xstrip, xouter, ystrip,
    load_sem, halo_send, halo_recv, strip_send, strip_recv, fb_send, fb_recv,
    q0, xpack, outer, ypack, q_send, q_recv, outer_send,
    ) = rest[:5], rest[5:]
    g, a, b = lax.axis_index("grp"), lax.axis_index("gx"), lax.axis_index("gy")
    nx, ny, lev = state.shape[2], state.shape[3], state.shape[4]
    tx, ty = nx // 3, ny // 3
    fx, fy = cx // 2, cy // 2
    quarter, slot = tx // 4, lev // 3

    barrier = pltpu.get_barrier_semaphore()
    greeted = []

    def greet(on, device):
        greeted.append(on)

        @pl.when(on)
        def _():
            pl.semaphore_signal(barrier, inc=1, device_id=device, device_id_type=MESH)

    for i in range(-1, 4):
        for j in range(-1, 4):
            child_a, child_b = 3 * (a - fx) + i, 3 * (b - fy) + j
            greet(
                (g == 0) & (a >= fx) & (b >= fy) & (child_a >= 0) & (child_a < cx)
                & (child_b >= 0) & (child_b < cy),
                (1, child_a, child_b),
            )

    def parents(place, first, count):
        own = first + place // 3
        return (
            (place >= 0, own),
            ((place % 3 == 0) & (place > 0), own - 1),
            ((place % 3 == 2) & (own + 1 < count), own + 1),
        )

    for on_a, parent_a in parents(a, fx, cx):
        for on_b, parent_b in parents(b, fy, cy):
            greet((g == 1) & on_a & on_b, (0, parent_a, parent_b))

    loads = [
        pltpu.make_async_copy(
            state.at[0], S.at[:, pl.ds(XB, nx), pl.ds(YB, ny), :], load_sem.at[0]
        ),
        pltpu.make_async_copy(
            courant.at[0], C.at[pl.ds(1, nx), pl.ds(YB, ny), :], load_sem.at[1]
        ),
    ]
    for n, (src, dst) in enumerate(zip(small, (inverse, iidx, iwgt, ridx, rwgt))):
        loads.append(pltpu.make_async_copy(src, dst, load_sem.at[2 + n]))
    for copy in loads:
        copy.start()

    def relay_of(at_a):
        to_a = fx + at_a // 3
        back = (at_a % 3 == 0) & (at_a != to_a)
        on = (at_a % 3 == 2) & (to_a + 1 < cx)
        return to_a, back, on

    to_a, back, on_next = relay_of(a)
    to_b = fy + b // 3
    parent, nest = g == 0, g == 1
    via = back | on_next
    relay_a = jnp.where(back, a, to_a + 1)
    greet(nest & via, (0, relay_a, to_b))
    relayed = []
    next_a = 3 * (a - 1 - fx) + 2
    for from_a, lane, i, here in (
        (a, 0, 0, back), (next_a, 1, 2, (a - 1 >= fx) & (next_a < cx)),
    ):
        for j in range(3):
            from_b = 3 * (b - fy) + j
            on = parent & here & (b >= fy) & (from_b < cy)
            relayed.append((on, 3 * lane + j, i, j, fx + from_a // 3))
            greet(on, (1, from_a, from_b))
        greet(relayed[-3][0], (0, fx + from_a // 3, b))
    for i in range(3):
        from_a = 3 * (a - fx) + i
        on = parent & (a >= fx) & (b >= fy) & (from_a < cx)
        _, from_back, from_next = relay_of(from_a)
        greet(on & from_back, (0, from_a, b))
        greet(on & from_next, (0, a + 1, b))

    greet(a > 0, (g, a - 1, b))
    greet(a < cx - 1, (g, a + 1, b))
    greet(b > 0, (g, a, b - 1))
    greet(b < cy - 1, (g, a, b + 1))
    zrow = jnp.zeros((2, ny, lev), F32)
    S[0, 0:2, YB : YB + ny, :] = zrow
    S[0, XB + nx : XB + nx + 2, YB : YB + ny, :] = zrow
    S[1, 0:2, YB : YB + ny, :] = zrow
    S[1, XB + nx : XB + nx + 2, YB : YB + ny, :] = zrow
    C[0:1, YB : YB + ny, :] = zrow[0:1]
    C[nx + 1 : nx + 2, YB : YB + ny, :] = zrow[0:1]
    outer[...] = jnp.zeros((2, 3, 3, 4, lev), F32)
    zcol = jnp.zeros((nx, 8, lev), F32)
    for c in (0, 2):
        S[c, XB : XB + nx, 0:YB, :] = zcol
        S[c, XB : XB + nx, YB + ny : YB + ny + 8, :] = zcol
    C[1 : 1 + nx, 0:YB, :] = zcol
    C[1 : 1 + nx, YB + ny : YB + ny + 8, :] = zcol
    with jax.named_scope("loads"):
        for copy in loads:
            copy.wait()
    m_high, m_low = split(inverse[:, 0, :])
    with jax.named_scope("greet"):
        pl.semaphore_wait(barrier, sum(on.astype(jnp.int32) for on in greeted))

    dirs = (
        (a > 0, a < cx - 1, (g, a - 1, b)),
        (a < cx - 1, a > 0, (g, a + 1, b)),
        (b > 0, b < cy - 1, (g, a, b - 1)),
        (b < cy - 1, b > 0, (g, a, b + 1)),
    )

    def halo_copy(k, d):
        if k == 0:
            src, dst = (sx0, rx0) if d < 2 else (sy0, ry0)
            src, dst = src.at[d % 2], dst.at[d % 2]
        else:
            src, dst = (sx, rx) if d < 2 else (sy, ry)
            src, dst = src.at[k - 1, d % 2], dst.at[k - 1, d % 2]
        return pltpu.make_async_remote_copy(
            src_ref=src, dst_ref=dst,
            send_sem=halo_send.at[d], recv_sem=halo_recv.at[k % 2, d],
            device_id=dirs[d][2], device_id_type=MESH,
        )

    def halo_sent(k):
        for d in range(4):
            @pl.when(dirs[d][0])
            def _():
                halo_copy(k, d).wait_send()

    def send_edges(k, which):
        rows = slice(XB, XB + nx)
        last_x, last_y = XB + nx, YB + ny
        cols = slice(YB, last_y)
        if k == 0:
            sx0[0, 0:2] = S[0, XB : XB + 2, cols, :]
            sx0[0, 2:3] = S[1, XB : XB + 1, cols, :]
            sx0[0, 3:4] = C[1:2, cols, :]
            sx0[1, 0:2] = S[0, last_x - 2 : last_x, cols, :]
            sx0[1, 2:3] = S[1, last_x - 1 : last_x, cols, :]
            sx0[1, 3:4] = C[nx : nx + 1, cols, :]
            sy0[0, :, 0:2] = S[0, rows, YB : YB + 2, :]
            sy0[0, :, 2:3] = S[2, rows, YB : YB + 1, :]
            sy0[0, :, 3:4] = C[1 : 1 + nx, YB : YB + 1, :]
            sy0[1, :, 0:2] = S[0, rows, last_y - 2 : last_y, :]
            sy0[1, :, 2:3] = S[2, rows, last_y - 1 : last_y, :]
            sy0[1, :, 3:4] = C[1 : 1 + nx, last_y - 1 : last_y, :]
        elif 0 in which:
            sx[k - 1, 0] = S[0, XB : XB + 2, cols, :]
            sx[k - 1, 1] = S[0, last_x - 2 : last_x, cols, :]
        else:
            sy[k - 1, 0] = S[0, rows, YB : YB + 2, :]
            sy[k - 1, 1] = S[0, rows, last_y - 2 : last_y, :]
        for d in which:
            @pl.when(dirs[d][0])
            def _():
                if k > 0:
                    halo_copy(k - 1, d).wait_send()
                halo_copy(k, d).start()

    def receive(k, which):
        cols = slice(YB, YB + ny)
        rows = slice(XB, XB + nx)
        last_x, last_y = XB + nx, YB + ny
        for d in which:
            @pl.when(dirs[d][1])
            def _():
                halo_copy(k, d).wait_recv()
                if d < 2:
                    got = rx0.at[d] if k == 0 else rx.at[k - 1, d]
                    at = last_x if d == 0 else XB - 2
                    S[0, at : at + 2, cols, :] = got[0:2]
                    if k == 0:
                        at = last_x if d == 0 else XB - 1
                        S[1, at : at + 1, cols, :] = got[2:3]
                        C[at - 1 : at, cols, :] = got[3:4]
                else:
                    got = ry0.at[d - 2] if k == 0 else ry.at[k - 1, d - 2]
                    at = last_y if d == 2 else YB - 2
                    S[0, rows, at : at + 2, :] = got[:, 0:2]
                    if k == 0:
                        at = last_y if d == 2 else YB - 1
                        S[2, rows, at : at + 1, :] = got[:, 2:3]
                        C[1 : 1 + nx, at : at + 1, :] = got[:, 3:4]

    cols = slice(YB, YB + ny)

    def u_row(r):
        slope = 0.5 * (S[0, r + 1, cols, :] - S[0, r - 1, cols, :])
        return S[1, r, cols, :] - C[r - 1, cols, :] * slope

    def v_row(r):
        mid = slice(YB + 1, YB + ny - 1)
        slope = 0.5 * (S[0, r, YB + 2 : YB + ny, :] - S[0, r, YB : YB + ny - 2, :])
        return S[2, r, mid, :] - C[r - 1, mid, :] * slope

    def inner_winds():
        group = 4

        def some(us, vs):
            new = [(1, r, cols, u_row(r)) for r in us]
            new += [(2, r, slice(YB + 1, YB + ny - 1), v_row(r)) for r in vs]
            for c, r, at, value in new:
                S[c, r, at, :] = value

        def rows(i, _):
            some(*[[XB + 2 + i * group + j for j in range(group)]] * 2)
            return 0

        first, last = XB, XB + nx - 1
        some((first + 1, last - 1), (first, first + 1, last - 1, last))
        lax.fori_loop(0, (nx - 4) // group, rows, 0)

    def edge_winds_x():
        new = [(r, u_row(r)) for r in (XB - 1, XB, XB + nx - 1, XB + nx)]
        for r, value in new:
            S[1, r, cols, :] = value

    def edge_winds_y():
        rows = slice(XB, XB + nx)
        for y in (YB - 1, YB + ny - 1):
            slope = 0.5 * (S[0, rows, y + 1 : y + 3, :] - S[0, rows, y - 1 : y + 1, :])
            S[2, rows, y : y + 2, :] = S[2, rows, y : y + 2, :] - C[1 : 1 + nx, y : y + 2, :] * slope

    def forced(r, y, width):
        at = slice(y, y + width)
        div = 0.5 * (S[1, r + 1, at, :] - S[1, r - 1, at, :]) + 0.5 * (
            S[2, r, y + 1 : y + width + 1, :] - S[2, r, y - 1 : y + width - 1, :]
        )
        return S[0, r, at, :] - C[r - 1, at, :] * div

    def solved(parts):
        return dot3(jnp.concatenate(parts, axis=0), m_high, m_low)

    def inner_pressure():
        group = 8

        def rows(i, _):
            first = XB + 2 + i * group
            new = solved([forced(first + j, YB, ny) for j in range(group)])
            for j in range(group):
                S[0, first + j, YB + 2 : YB + ny - 2, :] = new[j * ny + 2 : (j + 1) * ny - 2]
            return 0

        lax.fori_loop(0, (nx - 4) // group, rows, 0)

    def edge_rows():
        rows = (XB, XB + 1, XB + nx - 2, XB + nx - 1)
        new = solved([forced(r, YB, ny) for r in rows])
        for n, r in enumerate(rows):
            S[0, r, cols, :] = new[n * ny : (n + 1) * ny]

    def edge_columns():
        sides = [(r, y) for y in (YB, YB + ny - 8) for r in range(XB + 2, XB + nx - 2)]
        new = solved([forced(r, y, 8) for r, y in sides])
        for n, (r, y) in enumerate(sides):
            skip = 0 if y == YB else 6
            S[0, r, y + skip : y + skip + 2, :] = new[8 * n + skip : 8 * n + skip + 2]

    def hop(src, dst, device, send, recv):
        return pltpu.make_async_remote_copy(
            src_ref=src, dst_ref=dst, send_sem=send, recv_sem=recv,
            device_id=device, device_id_type=MESH,
        )

    chunks = ((1, slice(3, 3 * quarter)), (2, slice(0, 3 * quarter)), (1, slice(0, 3)))

    def home(src, c, part, i, j, device, send):
        n = 3 * i + j
        return hop(src, fb.at[n, c, part], device, send, fb_recv.at[n, min(c, 1)])

    def pressure_home(part):
        return home(rst.at[0, part], 0, part, a % 3, b % 3, (0, to_a, to_b), fb_send.at[0])

    def fb_start(n):
        c, part = chunks[n]
        mine, sem = rst.at[c, part], fb_send.at[1]
        around = via if n < 2 else back

        @pl.when(jnp.logical_not(around))
        def _():
            home(mine, c, part, a % 3, b % 3, (0, to_a, to_b), sem).start()

        @pl.when(around)
        def _():
            at = jnp.where(back, 0, 3) + b % 3
            hop(mine, q0.at[at, c - 1, part], (0, relay_a, to_b), sem, q_recv.at[at, n]).start()

    def pass_on():
        for n, (c, part) in enumerate(chunks):
            for on, at, i, j, home_a in relayed[: 6 if n < 2 else 3]:
                @pl.when(on)
                def _():
                    piece = q0.at[at, c - 1, part]
                    hop(piece, piece, (g, a, b), q_send.at[at], q_recv.at[at, n]).wait_recv()
                    home(piece, c, part, i, j, (0, home_a, b), q_send.at[at]).start()

    def passed_on():
        for on, at, _, _, _ in relayed:
            @pl.when(on)
            def _():
                sent = [q0.at[at]] if at < 3 else [q0.at[at, 0, chunks[0][1]], q0.at[at, 1]]
                for piece in sent:
                    hop(piece, piece, (g, a, b), q_send.at[at], q_recv.at[0, 0]).wait_send()

    def rows_of(i):
        if i == 0:
            return 0, tx - 1, 1, 2
        return tuple(4 * i - 1 + m for m in range(4))

    def mixed_row(c, u):
        total = None
        for t in range(9):
            part = wr[u, t] * S[c, XB + 3 * u + t // 3, pl.ds(YB + t % 3, ty, stride=3), :]
            total = part if total is None else total + part
        return total

    def gather_mean(k):
        def rows(u, _):
            new = [mixed_row(c, u) for c in range(3)]
            for c in range(3):
                racc[c, u] = new[c] if k == 0 else racc[c, u] + new[c]
            return 0

        lax.fori_loop(0, tx, rows, 0)

    def restrict(c, groups):
        spare = jnp.zeros((ty, 128 - lev - slot), F32)
        for i in groups:
            own = [racc[c, u] + mixed_row(c, u) for u in rows_of(i)]
            for m in range(3):
                part = own[3][:, m * slot : (m + 1) * slot]
                rst[c, 3 * i + m] = jnp.concatenate([own[m], part, spare], axis=1)

    def restrict_weights():
        terms = range(ridx.shape[0])
        w = [rwgt[k] for k in terms]
        scale = (1.0 / SUBS) / row_sum(w)
        shares = [part * scale for part in w]
        index = [ridx[k] for k in terms]
        for t in range(9):
            at = row_sum([jnp.where(index[k] == t, shares[k], 0.0) for k in terms]).T
            for u in range(tx):
                wr[u, t] = jnp.broadcast_to(at[:, u : u + 1], (ty, lev))

    def boundary_weights():
        share = iwgt[...] / jnp.sum(iwgt[...], axis=1, keepdims=True)
        share = share.reshape(nx * 4, ny).T
        index = iidx[...].astype(F32).reshape(nx * 4, ny).T.astype(jnp.int32)
        over = third(index)
        shape = index.shape
        x3 = (lax.broadcasted_iota(jnp.int32, shape, 1) * 171) >> 11
        y3 = (lax.broadcasted_iota(jnp.int32, shape, 0) * 171) >> 9
        source_x = jnp.clip(a * tx + x3 + over - 1, 0, cx * tx - 1)
        source_y = jnp.clip(b * ty + y3 + (index - 3 * over) - 1, 0, cy * ty - 1)

        def spread(cells, parts, x, depth):
            places = lax.broadcasted_iota(jnp.int32, (cells.shape[0], depth), 1)
            total = jnp.zeros(places.shape, F32)
            for n in range(4 * x, 4 * x + 4):
                total = total + jnp.where(places == cells[:, n : n + 1], parts[:, n : n + 1], 0.0)
            return total

        def y_weights(col, strip0):
            cells = (source_x - (a * tx - 1)) * 4 + source_y - (b * ty + strip0)
            cells, parts = cells[col : col + 8], share[col : col + 8]
            for x in range(nx):
                wy[8 * x : 8 * x + 8] = spread(cells, parts, x, 4 * (tx + 2))

        def x_weights(first, strip0):
            row, column = source_x - (a * tx + strip0), source_y - b * ty
            cells = jnp.where(
                column < 0, 3 * ty + row, jnp.where(column < ty, row * ty + column, 3 * ty + 4 + row)
            )
            for i in range(BAND):
                wx[ny * i : ny * i + ny] = spread(cells, share, first + i, 3 * ty + 8)

        @pl.when(b == 0)
        def _():
            y_weights(0, 0)

        @pl.when(b == cy - 1)
        def _():
            y_weights(ny - 8, ty - 4)

        @pl.when(a == 0)
        def _():
            x_weights(0, 0)

        @pl.when(a == cx - 1)
        def _():
            x_weights(nx - BAND, tx - 3)

    def row_sum(rows):
        total = rows[0]
        for row in rows[1:]:
            total = total + row
        return total

    y_windows = {-1: (0, 1, tx + 1), 0: (0, tx + 1, 1), 1: (tx - 1, 2 * tx + 1, 0),
                 2: (2 * tx - 1, nx, 0), 3: (nx - 1, nx, 0)}
    kinds = {-1: 1, 0: 0, 1: 0, 2: 0, 3: 2}

    def x_side(side):
        edge = 0 if side == 0 else cx - 1
        at = XB if side == 0 else XB + tx * (edge % 3) + tx - 3
        return edge, (a == fx + edge // 3) & (b >= fy), at

    def y_side(side):
        edge = 0 if side == 0 else cy - 1
        at = YB if side == 0 else YB + ty * (edge % 3) + ty - 4
        return edge, (b == fy + edge // 3) & (a >= fx), at

    def strip_pack(comps):
        for side in range(2):
            _, on, x_at = x_side(side)

            @pl.when(on)
            def _():
                for c in comps:
                    xpack[c] = S[c, x_at : x_at + 3, YB : YB + ny, :]
                    for j in range(3):
                        for side_y, y in ((1, j * ty), (0, j * ty + ty - 1)):
                            outer[side_y, j, c, 0:3] = S[c, x_at : x_at + 3, YB + y, :]

            _, on, y_at = y_side(side)

            @pl.when(on)
            def _():
                for c in comps:
                    ypack[c] = S[c, XB : XB + nx, y_at : y_at + 4, :]

    def strip_copies(comps):
        for side in range(2):
            edge, here, _ = x_side(side)
            for j in range(3):
                child = 3 * (b - fy) + j
                yield here & (child < cy), pltpu.make_async_remote_copy(
                    src_ref=xpack.at[comps, :, pl.ds(j * ty, ty), :], dst_ref=xstrip.at[comps],
                    send_sem=strip_send.at[0, j], recv_sem=strip_recv.at[0, 0],
                    device_id=(1, edge, child), device_id_type=MESH,
                )
                if comps.start > 0:
                    continue
                for side_y, beside in ((0, child + 1), (1, child - 1)):
                    yield here & (child < cy) & (beside >= 0) & (beside < cy), pltpu.make_async_remote_copy(
                        src_ref=outer.at[side_y, j], dst_ref=xouter.at[side_y],
                        send_sem=outer_send.at[side_y, j], recv_sem=strip_recv.at[0, 1 + side_y],
                        device_id=(1, edge, beside), device_id_type=MESH,
                    )
            edge, here, _ = y_side(side)
            for i in range(-1, 4):
                lo, hi, dst = y_windows[i]
                child = 3 * (a - fx) + i
                yield here & (child >= 0) & (child < cx), pltpu.make_async_remote_copy(
                    src_ref=ypack.at[comps, pl.ds(lo, hi - lo)],
                    dst_ref=ystrip.at[comps, pl.ds(dst, hi - lo)],
                    send_sem=strip_send.at[1, i + 1], recv_sem=strip_recv.at[1, kinds[i]],
                    device_id=(1, child, edge), device_id_type=MESH,
                )

    def strip_start(comps):
        for on, copy in strip_copies(comps):
            @pl.when(on)
            def _():
                copy.start()

    def strips_sent():
        for on, copy in strip_copies(slice(0, 3)):
            @pl.when(on)
            def _():
                copy.wait_send()

    def strip_wait(ref, kind):
        pltpu.make_async_remote_copy(
            src_ref=ref, dst_ref=ref, send_sem=strip_send.at[0, 0],
            recv_sem=strip_recv.at[kind], device_id=(g, a, b), device_id_type=MESH,
        ).wait_recv()

    def wait_y_strips():
        def rows(kind, lo, hi, dst):
            strip_wait(ystrip.at[:, pl.ds(dst, hi - lo), :, :], (1, kind))

        for i in range(3):
            @pl.when(a % 3 == i)
            def _():
                rows(0, *y_windows[i])

        @pl.when((a % 3 == 2) & (a < cx - 1))
        def _():
            rows(1, *y_windows[-1])

        @pl.when((a % 3 == 0) & (a > 0))
        def _():
            rows(2, *y_windows[3])

    def wait_x_strips():
        strip_wait(xstrip, (0, 0))

        @pl.when(b > 0)
        def _():
            strip_wait(xouter.at[0], (0, 1))

        @pl.when(b < cy - 1)
        def _():
            strip_wait(xouter.at[1], (0, 2))

    def relax_at(x, y):
        gx, gy = a * nx + x, b * ny + y
        depth = jnp.minimum(
            jnp.minimum(gx, nx * cx - 1 - gx), jnp.minimum(gy, ny * cy - 1 - gy)
        ).astype(F32)
        return jnp.maximum(1.0 - depth / BAND, 0.0)

    def mixed(weights, source):
        w_high, w_low = split(weights)
        s_high, s_low = split(source)
        return dot(w_high, s_high) + (dot(w_low, s_high) + dot(w_high, s_low))

    def y_edge(col):
        shape = (nx, 8, lev)
        relax = relax_at(
            lax.broadcasted_iota(jnp.int32, shape, 0), col + lax.broadcasted_iota(jnp.int32, shape, 1)
        )
        for c in range(3):
            bound = mixed(wy[...], ystrip[c].reshape(4 * (tx + 2), lev)).reshape(shape)
            at = (c, slice(XB, XB + nx), slice(YB + col, YB + col + 8), slice(None))
            now = S[at]
            S[at] = now + relax * (bound - now)

    def x_edge(first):
        shape = (BAND, ny, lev)
        relax = relax_at(
            first + lax.broadcasted_iota(jnp.int32, shape, 0), lax.broadcasted_iota(jnp.int32, shape, 1)
        )
        for c in range(3):
            source = jnp.concatenate(
                [xstrip[c].reshape(3 * ty, lev), xouter[0, c], xouter[1, c]], axis=0
            )
            bound = mixed(wx[...], source).reshape(shape)
            now = saved[c]
            S[c, XB + first : XB + first + BAND, YB : YB + ny, :] = now + relax * (bound - now)

    for k in range(SUBS):
        if k == 0:
            send_edges(0, (0, 1, 2, 3))

        @pl.when(g == 1)
        def _():
            if k == 0:
                with jax.named_scope("restrict_weights"):
                    restrict_weights()
            else:
                with jax.named_scope(f"mean{k}"):
                    gather_mean(k - 1)

        last = k == SUBS - 1
        with jax.named_scope(f"inner_winds{k}"):
            inner_winds()
        if last:
            @pl.when(g == 1)
            def _():
                with jax.named_scope("restrict_u"):
                    restrict(1, range(1, quarter))
                fb_start(0)

        with jax.named_scope(f"inner_pressure{k}"):
            inner_pressure()
        if k == 1:
            @pl.when((g == 1) & ((a == 0) | (a == cx - 1) | (b == 0) | (b == cy - 1)))
            def _():
                with jax.named_scope("boundary_weights"):
                    boundary_weights()
        with jax.named_scope(f"receive_y{k}"):
            receive(k, (2, 3))
        edge_winds_y()
        if last:
            @pl.when(g == 1)
            def _():
                with jax.named_scope("restrict_v"):
                    restrict(2, range(quarter))
                fb_start(1)

            @pl.when(g == 0)
            def _():
                strip_pack((2,))
                strip_start(slice(2, 3))
        outer_tile = (b == 0) | (b == cy - 1)

        def columns():
            with jax.named_scope(f"edge_columns{k}"):
                edge_columns()

        if last:
            columns()

            @pl.when(g == 1)
            def _():
                restrict(0, range(1, quarter))
                pressure_home(slice(3, 3 * quarter)).start()
        else:
            pl.when(outer_tile)(columns)
        with jax.named_scope(f"receive_x{k}"):
            receive(k, (0, 1))
        edge_winds_x()
        if last:
            @pl.when(g == 1)
            def _():
                restrict(1, (0,))
                fb_start(2)

            @pl.when(g == 0)
            def _():
                strip_pack((1,))
                strip_start(slice(1, 2))
        with jax.named_scope(f"edge_rows{k}"):
            edge_rows()
            if not last:
                send_edges(k + 1, (0, 1))
        if not last:
            pl.when(jnp.logical_not(outer_tile))(columns)
            send_edges(k + 1, (2, 3))

    def take(i, j, comps):
        first, count = comps[0], len(comps)
        with jax.named_scope(f"piece{i}{j}{first}"):
            piece = fb.at[3 * i + j, first : first + count]
            pltpu.make_async_remote_copy(
                src_ref=piece, dst_ref=piece, send_sem=fb_send.at[0],
                recv_sem=fb_recv.at[3 * i + j, min(first, 1)], device_id=(g, a, b),
                device_id_type=MESH,
            ).wait_recv()
        for c in comps:
            for n in range(quarter):
                got = fb[3 * i + j, c, 3 * n : 3 * n + 3]
                rows = [got[m, :, :lev] for m in range(3)]
                rows.append(jnp.concatenate([got[m, :, lev : lev + slot] for m in range(3)], axis=1))
                for u, value in zip(rows_of(n), rows):
                    at = (c, XB + i * tx + u, slice(YB + j * ty, YB + (j + 1) * ty), slice(None))
                    now = S[at]
                    S[at] = now + FEEDBACK * (value - now)

    @pl.when(g == 1)
    def _():
        with jax.named_scope("restrict_pressure"):
            restrict(0, (0,))
        pressure_home(slice(0, 3)).start()
        halo_sent(SUBS - 1)
        x_low, x_high = a == 0, a == cx - 1
        y_low, y_high = b == 0, b == cy - 1

        @pl.when(x_low)
        def _():
            for c in range(3):
                saved[c] = S[c, XB : XB + BAND, YB : YB + ny, :]

        @pl.when(x_high)
        def _():
            for c in range(3):
                saved[c] = S[c, XB + nx - BAND : XB + nx, YB : YB + ny, :]

        @pl.when(x_low | x_high)
        def _():
            @pl.when(y_low)
            def _():
                xouter[0] = jnp.zeros((3, 4, lev), F32)

            @pl.when(y_high)
            def _():
                xouter[1] = jnp.zeros((3, 4, lev), F32)

        @pl.when(y_low | y_high)
        def _():
            @pl.when(x_low)
            def _():
                ystrip[:, 0:1] = jnp.zeros((3, 1, 4, lev), F32)

            if (cx - 1) % 3 == 2:

                @pl.when(x_high)
                def _():
                    ystrip[:, tx + 1 : tx + 2] = jnp.zeros((3, 1, 4, lev), F32)

            with jax.named_scope("wait_y"):
                wait_y_strips()

        @pl.when(y_low)
        def _():
            with jax.named_scope("y_low"):
                y_edge(0)

        @pl.when(y_high)
        def _():
            with jax.named_scope("y_high"):
                y_edge(ny - 8)

        @pl.when(x_low | x_high)
        def _():
            with jax.named_scope("wait_x"):
                wait_x_strips()

        @pl.when(x_low)
        def _():
            with jax.named_scope("x_low_edge"):
                x_edge(0)

        @pl.when(x_high)
        def _():
            with jax.named_scope("x_high_edge"):
                x_edge(nx - BAND)

        for part, comps in ((1, slice(1, 3)), (0, slice(0, 1))):
            piece = rst.at[comps]
            hop(piece, piece, (g, a, b), fb_send.at[part], q_recv.at[0, 0]).wait_send()

    @pl.when(g == 0)
    def _():
        strip_pack((0,))
        strip_start(slice(0, 1))
        with jax.named_scope("pass_parent"):
            pass_on()
        halo_sent(SUBS - 1)
        passed_on()
        winds_of, pressure_of = (1, 2), (0,)
        tiles = [[(i, j) for j in (2, 0, 1)] for i in range(3)]
        order = [(at, winds_of) for at in tiles[1]] + [(at, pressure_of) for at in tiles[1]]
        order += [(at, winds_of) for at in tiles[2]] + [(at, pressure_of) for at in tiles[0]]
        order += [(at, pressure_of) for at in tiles[2][:2]] + [(at, winds_of) for at in tiles[0]]
        order += [(at, pressure_of) for at in tiles[2][2:]]
        for (i, j), comps in order:
            there = (a >= fx) & (b >= fy) & (3 * (a - fx) + i < cx) & (3 * (b - fy) + j < cy)

            @pl.when(there)
            def _():
                take(i, j, comps)

        strips_sent()


def store(padded, out, sem):
    nx, ny = out.shape[2], out.shape[3]
    copy = pltpu.make_async_copy(
        padded.at[:, pl.ds(XB, nx), pl.ds(YB, ny), :], out.at[0], sem.at[0]
    )
    copy.start()
    copy.wait()


def per_device(
    state, courant, vert_inverse, interp_index, interp_weight, restrict_index, restrict_weight
):
    cx, cy = lax.axis_size("gx"), lax.axis_size("gy")
    _, _, nx, ny, lev = state.shape
    tx, ty = nx // 3, ny // 3
    packed = (3 * (tx // 4), ty, 128)
    vmem = lambda *shape: pltpu.VMEM(shape, F32)
    dma = pltpu.SemaphoreType.DMA
    anywhere = pl.BlockSpec(memory_space=pltpu.HBM)
    inside = pl.BlockSpec(memory_space=pltpu.VMEM)
    padded = pl.pallas_call(
        functools.partial(kernel, cx, cy),
        out_shape=vmem(3, nx + 4, ny + 16, lev),
        in_specs=[anywhere] * 7,
        out_specs=inside,
        scratch_shapes=[
            vmem(nx + 2, ny + 16, lev),
            vmem(lev, 1, lev),
            pltpu.VMEM((nx, 4, ny), jnp.int32),
            vmem(nx, 4, ny),
            pltpu.VMEM((9, tx, ty), jnp.int32),
            vmem(9, tx, ty),
            vmem(3, BAND, ny, lev),
            vmem(3, tx, ty, lev),
            vmem(tx, 9, ty, lev),
            vmem(BAND * ny, 3 * ty + 8),
            vmem(nx * 8, 4 * (tx + 2)),
            vmem(2, 4, ny, lev),
            vmem(2, nx, 4, lev),
            vmem(2, 4, ny, lev),
            vmem(2, nx, 4, lev),
            vmem(SUBS - 1, 2, 2, ny, lev),
            vmem(SUBS - 1, 2, nx, 2, lev),
            vmem(SUBS - 1, 2, 2, ny, lev),
            vmem(SUBS - 1, 2, nx, 2, lev),
            vmem(3, *packed),
            vmem(9, 3, *packed),
            vmem(3, 3, ty, lev),
            vmem(2, 3, 4, lev),
            vmem(3, tx + 2, 4, lev),
            dma((7,)),
            dma((4,)),
            dma((2, 4)),
            dma((2, 5)),
            dma((2, 3)),
            dma((2,)),
            dma((9, 2)),
            vmem(6, 2, *packed),
            vmem(3, 3, ny, lev),
            vmem(2, 3, 3, 4, lev),
            vmem(3, nx, 4, lev),
            dma((6,)),
            dma((6, 3)),
            dma((2, 3)),
        ],
        compiler_params=pltpu.CompilerParams(
            has_side_effects=True, collective_id=0, vmem_limit_bytes=67043328 - 4 * (3 * (nx + 4) * (ny + 16) * 128) - 2**14
        ),
        name="nest_step",
    )(
        state, courant, vert_inverse.transpose(1, 0, 2),
        interp_index.transpose(0, 2, 1), interp_weight.transpose(0, 2, 1),
        restrict_index.transpose(2, 0, 1), restrict_weight.transpose(2, 0, 1),
    )
    return pl.pallas_call(
        store, out_shape=jax.ShapeDtypeStruct(state.shape, F32), in_specs=[inside], out_specs=anywhere,
        scratch_shapes=[dma((1,))], name="store",
        compiler_params=pltpu.CompilerParams(vmem_limit_bytes=2**20),
    )(padded)


def solution(mesh):
    return jax.shard_map(
        per_device,
        mesh=mesh,
        in_specs=(
            P("grp", None, "gx", "gy", None),
            P("grp", "gx", "gy", None),
            P("grp", None, None),
            P("gx", "gy", None),
            P("gx", "gy", None),
            P("gx", "gy", None),
            P("gx", "gy", None),
        ),
        out_specs=P("grp", None, "gx", "gy", None),
        check_vma=False,
    )
```

```python
import functools

import jax
import jax.numpy as jnp
from jax import lax
from jax.experimental import pallas as pl
from jax.experimental.pallas import tpu as pltpu
from jax.sharding import PartitionSpec as P

SUBS = 4
BAND = 5
FEEDBACK = 0.5
MESH = pl.DeviceIdType.MESH
F32 = jnp.float32
XB, YB = 2, 8


def split(a):
    high = a.astype(jnp.bfloat16)
    return high, (a - high.astype(F32)).astype(jnp.bfloat16)


def dot(a, b):
    return jnp.dot(a, b, preferred_element_type=F32)


def dot3(a, b_high, b_low):
    a_high, a_low = split(a)
    return dot(a_high, b_high) + (dot(a_low, b_high) + dot(a_high, b_low))


def third(t):
    return (t * 11) >> 5


def kernel(
    cx, cy,
    state, courant, *rest,
):
    small, (
    S,
    C, inverse, iidx, iwgt, ridx, rwgt, saved, racc, wr, wx, wy, sx0, sy0, rx0, ry0, sx, sy, rx, ry, rst, fb, xstrip, xouter, ystrip,
    load_sem, halo_send, halo_recv, strip_send, strip_recv, fb_send, fb_recv,
    q0, xpack, outer, ypack, q_send, q_recv, outer_send,
    ) = rest[:5], rest[5:]
    g, a, b = lax.axis_index("grp"), lax.axis_index("gx"), lax.axis_index("gy")
    nx, ny, lev = state.shape[2], state.shape[3], state.shape[4]
    tx, ty = nx // 3, ny // 3
    fx, fy = cx // 2, cy // 2
    quarter, slot = tx // 4, lev // 3

    barrier = pltpu.get_barrier_semaphore()
    greeted = []

    def greet(on, device):
        greeted.append(on)

        @pl.when(on)
        def _():
            pl.semaphore_signal(barrier, inc=1, device_id=device, device_id_type=MESH)

    for i in range(-1, 4):
        for j in range(-1, 4):
            child_a, child_b = 3 * (a - fx) + i, 3 * (b - fy) + j
            greet(
                (g == 0) & (a >= fx) & (b >= fy) & (child_a >= 0) & (child_a < cx)
                & (child_b >= 0) & (child_b < cy),
                (1, child_a, child_b),
            )

    def parents(place, first, count):
        own = first + place // 3
        return (
            (place >= 0, own),
            ((place % 3 == 0) & (place > 0), own - 1),
            ((place % 3 == 2) & (own + 1 < count), own + 1),
        )

    for on_a, parent_a in parents(a, fx, cx):
        for on_b, parent_b in parents(b, fy, cy):
            greet((g == 1) & on_a & on_b, (0, parent_a, parent_b))

    loads = [
        pltpu.make_async_copy(
            state.at[0], S.at[:, pl.ds(XB, nx), pl.ds(YB, ny), :], load_sem.at[0]
        ),
        pltpu.make_async_copy(
            courant.at[0], C.at[pl.ds(1, nx), pl.ds(YB, ny), :], load_sem.at[1]
        ),
    ]
    for n, (src, dst) in enumerate(zip(small, (inverse, iidx, iwgt, ridx, rwgt))):
        loads.append(pltpu.make_async_copy(src, dst, load_sem.at[2 + n]))
    for copy in loads:
        copy.start()

    def relay_of(at_a):
        to_a = fx + at_a // 3
        back = (at_a % 3 == 0) & (at_a != to_a)
        on = (at_a % 3 == 2) & (to_a + 1 < cx)
        return to_a, back, on

    to_a, back, on_next = relay_of(a)
    to_b = fy + b // 3
    parent, nest = g == 0, g == 1
    via = back | on_next
    relay_a = jnp.where(back, a, to_a + 1)
    greet(nest & via, (0, relay_a, to_b))
    relayed = []
    next_a = 3 * (a - 1 - fx) + 2
    for from_a, lane, i, here in (
        (a, 0, 0, back), (next_a, 1, 2, (a - 1 >= fx) & (next_a < cx)),
    ):
        for j in range(3):
            from_b = 3 * (b - fy) + j
            on = parent & here & (b >= fy) & (from_b < cy)
            relayed.append((on, 3 * lane + j, i, j, fx + from_a // 3))
            greet(on, (1, from_a, from_b))
        greet(relayed[-3][0], (0, fx + from_a // 3, b))
    for i in range(3):
        from_a = 3 * (a - fx) + i
        on = parent & (a >= fx) & (b >= fy) & (from_a < cx)
        _, from_back, from_next = relay_of(from_a)
        greet(on & from_back, (0, from_a, b))
        greet(on & from_next, (0, a + 1, b))

    greet(a > 0, (g, a - 1, b))
    greet(a < cx - 1, (g, a + 1, b))
    greet(b > 0, (g, a, b - 1))
    greet(b < cy - 1, (g, a, b + 1))
    zrow = jnp.zeros((2, ny, lev), F32)
    S[0, 0:2, YB : YB + ny, :] = zrow
    S[0, XB + nx : XB + nx + 2, YB : YB + ny, :] = zrow
    S[1, 0:2, YB : YB + ny, :] = zrow
    S[1, XB + nx : XB + nx + 2, YB : YB + ny, :] = zrow
    C[0:1, YB : YB + ny, :] = zrow[0:1]
    C[nx + 1 : nx + 2, YB : YB + ny, :] = zrow[0:1]
    outer[...] = jnp.zeros((2, 3, 3, 4, lev), F32)
    zcol = jnp.zeros((nx, 8, lev), F32)
    for c in (0, 2):
        S[c, XB : XB + nx, 0:YB, :] = zcol
        S[c, XB : XB + nx, YB + ny : YB + ny + 8, :] = zcol
    C[1 : 1 + nx, 0:YB, :] = zcol
    C[1 : 1 + nx, YB + ny : YB + ny + 8, :] = zcol
    with jax.named_scope("loads"):
        for copy in loads:
            copy.wait()
    m_high, m_low = split(inverse[:, 0, :])
    with jax.named_scope("greet"):
        pl.semaphore_wait(barrier, sum(on.astype(jnp.int32) for on in greeted))

    dirs = (
        (a > 0, a < cx - 1, (g, a - 1, b)),
        (a < cx - 1, a > 0, (g, a + 1, b)),
        (b > 0, b < cy - 1, (g, a, b - 1)),
        (b < cy - 1, b > 0, (g, a, b + 1)),
    )

    def halo_copy(k, d):
        if k == 0:
            src, dst = (sx0, rx0) if d < 2 else (sy0, ry0)
            src, dst = src.at[d % 2], dst.at[d % 2]
        else:
            src, dst = (sx, rx) if d < 2 else (sy, ry)
            src, dst = src.at[k - 1, d % 2], dst.at[k - 1, d % 2]
        return pltpu.make_async_remote_copy(
            src_ref=src, dst_ref=dst,
            send_sem=halo_send.at[d], recv_sem=halo_recv.at[k % 2, d],
            device_id=dirs[d][2], device_id_type=MESH,
        )

    def halo_sent(k):
        for d in range(4):
            @pl.when(dirs[d][0])
            def _():
                halo_copy(k, d).wait_send()

    def send_edges(k, which):
        rows = slice(XB, XB + nx)
        last_x, last_y = XB + nx, YB + ny
        cols = slice(YB, last_y)
        if k == 0:
            sx0[0, 0:2] = S[0, XB : XB + 2, cols, :]
            sx0[0, 2:3] = S[1, XB : XB + 1, cols, :]
            sx0[0, 3:4] = C[1:2, cols, :]
            sx0[1, 0:2] = S[0, last_x - 2 : last_x, cols, :]
            sx0[1, 2:3] = S[1, last_x - 1 : last_x, cols, :]
            sx0[1, 3:4] = C[nx : nx + 1, cols, :]
            sy0[0, :, 0:2] = S[0, rows, YB : YB + 2, :]
            sy0[0, :, 2:3] = S[2, rows, YB : YB + 1, :]
            sy0[0, :, 3:4] = C[1 : 1 + nx, YB : YB + 1, :]
            sy0[1, :, 0:2] = S[0, rows, last_y - 2 : last_y, :]
            sy0[1, :, 2:3] = S[2, rows, last_y - 1 : last_y, :]
            sy0[1, :, 3:4] = C[1 : 1 + nx, last_y - 1 : last_y, :]
        elif 0 in which:
            sx[k - 1, 0] = S[0, XB : XB + 2, cols, :]
            sx[k - 1, 1] = S[0, last_x - 2 : last_x, cols, :]
        else:
            sy[k - 1, 0] = S[0, rows, YB : YB + 2, :]
            sy[k - 1, 1] = S[0, rows, last_y - 2 : last_y, :]
        for d in which:
            @pl.when(dirs[d][0])
            def _():
                if k > 0:
                    halo_copy(k - 1, d).wait_send()
                halo_copy(k, d).start()

    def receive(k, which):
        cols = slice(YB, YB + ny)
        rows = slice(XB, XB + nx)
        last_x, last_y = XB + nx, YB + ny
        for d in which:
            @pl.when(dirs[d][1])
            def _():
                halo_copy(k, d).wait_recv()
                if d < 2:
                    got = rx0.at[d] if k == 0 else rx.at[k - 1, d]
                    at = last_x if d == 0 else XB - 2
                    S[0, at : at + 2, cols, :] = got[0:2]
                    if k == 0:
                        at = last_x if d == 0 else XB - 1
                        S[1, at : at + 1, cols, :] = got[2:3]
                        C[at - 1 : at, cols, :] = got[3:4]
                else:
                    got = ry0.at[d - 2] if k == 0 else ry.at[k - 1, d - 2]
                    at = last_y if d == 2 else YB - 2
                    S[0, rows, at : at + 2, :] = got[:, 0:2]
                    if k == 0:
                        at = last_y if d == 2 else YB - 1
                        S[2, rows, at : at + 1, :] = got[:, 2:3]
                        C[1 : 1 + nx, at : at + 1, :] = got[:, 3:4]

    cols = slice(YB, YB + ny)

    def u_row(r):
        slope = 0.5 * (S[0, r + 1, cols, :] - S[0, r - 1, cols, :])
        return S[1, r, cols, :] - C[r - 1, cols, :] * slope

    def v_row(r):
        mid = slice(YB + 1, YB + ny - 1)
        slope = 0.5 * (S[0, r, YB + 2 : YB + ny, :] - S[0, r, YB : YB + ny - 2, :])
        return S[2, r, mid, :] - C[r - 1, mid, :] * slope

    def inner_winds():
        group = 4

        def some(us, vs):
            new = [(1, r, cols, u_row(r)) for r in us]
            new += [(2, r, slice(YB + 1, YB + ny - 1), v_row(r)) for r in vs]
            for c, r, at, value in new:
                S[c, r, at, :] = value

        def rows(i, _):
            some(*[[XB + 2 + i * group + j for j in range(group)]] * 2)
            return 0

        first, last = XB, XB + nx - 1
        some((first + 1, last - 1), (first, first + 1, last - 1, last))
        lax.fori_loop(0, (nx - 4) // group, rows, 0)

    def edge_winds_x():
        new = [(r, u_row(r)) for r in (XB - 1, XB, XB + nx - 1, XB + nx)]
        for r, value in new:
            S[1, r, cols, :] = value

    def edge_winds_y():
        rows = slice(XB, XB + nx)
        for y in (YB - 1, YB + ny - 1):
            slope = 0.5 * (S[0, rows, y + 1 : y + 3, :] - S[0, rows, y - 1 : y + 1, :])
            S[2, rows, y : y + 2, :] = S[2, rows, y : y + 2, :] - C[1 : 1 + nx, y : y + 2, :] * slope

    def forced(r, y, width):
        at = slice(y, y + width)
        div = 0.5 * (S[1, r + 1, at, :] - S[1, r - 1, at, :]) + 0.5 * (
            S[2, r, y + 1 : y + width + 1, :] - S[2, r, y - 1 : y + width - 1, :]
        )
        return S[0, r, at, :] - C[r - 1, at, :] * div

    def solved(parts):
        return dot3(jnp.concatenate(parts, axis=0), m_high, m_low)

    def inner_pressure():
        group = 8

        def rows(i, _):
            first = XB + 2 + i * group
            new = solved([forced(first + j, YB, ny) for j in range(group)])
            for j in range(group):
                S[0, first + j, YB + 2 : YB + ny - 2, :] = new[j * ny + 2 : (j + 1) * ny - 2]
            return 0

        lax.fori_loop(0, (nx - 4) // group, rows, 0)

    def edge_rows():
        rows = (XB, XB + 1, XB + nx - 2, XB + nx - 1)
        new = solved([forced(r, YB, ny) for r in rows])
        for n, r in enumerate(rows):
            S[0, r, cols, :] = new[n * ny : (n + 1) * ny]

    def edge_columns():
        sides = [(r, y) for y in (YB, YB + ny - 8) for r in range(XB + 2, XB + nx - 2)]
        new = solved([forced(r, y, 8) for r, y in sides])
        for n, (r, y) in enumerate(sides):
            skip = 0 if y == YB else 6
            S[0, r, y + skip : y + skip + 2, :] = new[8 * n + skip : 8 * n + skip + 2]

    def hop(src, dst, device, send, recv):
        return pltpu.make_async_remote_copy(
            src_ref=src, dst_ref=dst, send_sem=send, recv_sem=recv,
            device_id=device, device_id_type=MESH,
        )

    chunks = ((1, slice(3, 3 * quarter)), (2, slice(0, 3 * quarter)), (1, slice(0, 3)))

    def home(src, c, part, i, j, device, send):
        n = 3 * i + j
        return hop(src, fb.at[n, c, part], device, send, fb_recv.at[i, min(c, 1)])

    def pressure_home(part):
        return home(rst.at[0, part], 0, part, a % 3, b % 3, (0, to_a, to_b), fb_send.at[0])

    def q_slot(at, n):
        return 6 * n + at

    def fb_start(n):
        c, part = chunks[n]
        mine, sem = rst.at[c, part], fb_send.at[1]
        around = via if n < 2 else back

        @pl.when(jnp.logical_not(around))
        def _():
            home(mine, c, part, a % 3, b % 3, (0, to_a, to_b), sem).start()

        @pl.when(around)
        def _():
            at = jnp.where(back, 0, 3) + b % 3
            hop(mine, q0.at[at, c - 1, part], (0, relay_a, to_b), sem, q_recv.at[q_slot(at, n)]).start()

    def pass_on():
        for n, (c, part) in enumerate(chunks):
            for on, at, i, j, home_a in relayed[: 6 if n < 2 else 3]:
                @pl.when(on)
                def _():
                    piece = q0.at[at, c - 1, part]
                    hop(piece, piece, (g, a, b), q_send.at[at], q_recv.at[q_slot(at, n)]).wait_recv()
                    home(piece, c, part, i, j, (0, home_a, b), q_send.at[at]).start()

    def passed_on():
        for on, at, _, _, _ in relayed:
            @pl.when(on)
            def _():
                sent = [q0.at[at]] if at < 3 else [q0.at[at, 0, chunks[0][1]], q0.at[at, 1]]
                for piece in sent:
                    hop(piece, piece, (g, a, b), q_send.at[at], q_recv.at[0]).wait_send()

    def rows_of(i):
        if i == 0:
            return 0, tx - 1, 1, 2
        return tuple(4 * i - 1 + m for m in range(4))

    def mixed_row(c, u):
        total = None
        for t in range(9):
            part = wr[u, t] * S[c, XB + 3 * u + t // 3, pl.ds(YB + t % 3, ty, stride=3), :]
            total = part if total is None else total + part
        return total

    def gather_mean(k):
        def rows(u, _):
            new = [mixed_row(c, u) for c in range(3)]
            for c in range(3):
                racc[c, u] = new[c] if k == 0 else racc[c, u] + new[c]
            return 0

        lax.fori_loop(0, tx, rows, 0)

    def restrict(c, groups):
        spare = jnp.zeros((ty, 128 - lev - slot), F32)
        for i in groups:
            own = [racc[c, u] + mixed_row(c, u) for u in rows_of(i)]
            for m in range(3):
                part = own[3][:, m * slot : (m + 1) * slot]
                rst[c, 3 * i + m] = jnp.concatenate([own[m], part, spare], axis=1)

    def restrict_weights():
        terms = range(ridx.shape[0])
        w = [rwgt[k] for k in terms]
        scale = (1.0 / SUBS) / row_sum(w)
        shares = [part * scale for part in w]
        index = [ridx[k] for k in terms]
        for t in range(9):
            at = row_sum([jnp.where(index[k] == t, shares[k], 0.0) for k in terms]).T
            for u in range(tx):
                wr[u, t] = jnp.broadcast_to(at[:, u : u + 1], (ty, lev))

    def boundary_weights():
        share = iwgt[...] / jnp.sum(iwgt[...], axis=1, keepdims=True)
        share = share.reshape(nx * 4, ny).T
        index = iidx[...].astype(F32).reshape(nx * 4, ny).T.astype(jnp.int32)
        over = third(index)
        shape = index.shape
        x3 = (lax.broadcasted_iota(jnp.int32, shape, 1) * 171) >> 11
        y3 = (lax.broadcasted_iota(jnp.int32, shape, 0) * 171) >> 9
        source_x = jnp.clip(a * tx + x3 + over - 1, 0, cx * tx - 1)
        source_y = jnp.clip(b * ty + y3 + (index - 3 * over) - 1, 0, cy * ty - 1)

        def spread(cells, parts, x, depth):
            places = lax.broadcasted_iota(jnp.int32, (cells.shape[0], depth), 1)
            total = jnp.zeros(places.shape, F32)
            for n in range(4 * x, 4 * x + 4):
                total = total + jnp.where(places == cells[:, n : n + 1], parts[:, n : n + 1], 0.0)
            return total

        def y_weights(col, strip0):
            cells = (source_x - (a * tx - 1)) * 4 + source_y - (b * ty + strip0)
            cells, parts = cells[col : col + 8], share[col : col + 8]
            for x in range(nx):
                wy[8 * x : 8 * x + 8] = spread(cells, parts, x, 4 * (tx + 2))

        def x_weights(first, strip0):
            row, column = source_x - (a * tx + strip0), source_y - b * ty
            cells = jnp.where(
                column < 0, 3 * ty + row, jnp.where(column < ty, row * ty + column, 3 * ty + 4 + row)
            )
            for i in range(BAND):
                wx[ny * i : ny * i + ny] = spread(cells, share, first + i, 3 * ty + 8)

        @pl.when(b == 0)
        def _():
            y_weights(0, 0)

        @pl.when(b == cy - 1)
        def _():
            y_weights(ny - 8, ty - 4)

        @pl.when(a == 0)
        def _():
            x_weights(0, 0)

        @pl.when(a == cx - 1)
        def _():
            x_weights(nx - BAND, tx - 3)

    def row_sum(rows):
        total = rows[0]
        for row in rows[1:]:
            total = total + row
        return total

    y_windows = {-1: (0, 1, tx + 1), 0: (0, tx + 1, 1), 1: (tx - 1, 2 * tx + 1, 0),
                 2: (2 * tx - 1, nx, 0), 3: (nx - 1, nx, 0)}
    kinds = {-1: 1, 0: 0, 1: 0, 2: 0, 3: 2}

    def x_side(side):
        edge = 0 if side == 0 else cx - 1
        at = XB if side == 0 else XB + tx * (edge % 3) + tx - 3
        return edge, (a == fx + edge // 3) & (b >= fy), at

    def y_side(side):
        edge = 0 if side == 0 else cy - 1
        at = YB if side == 0 else YB + ty * (edge % 3) + ty - 4
        return edge, (b == fy + edge // 3) & (a >= fx), at

    def strip_pack(comps):
        for side in range(2):
            _, on, x_at = x_side(side)

            @pl.when(on)
            def _():
                for c in comps:
                    xpack[c] = S[c, x_at : x_at + 3, YB : YB + ny, :]
                    for j in range(3):
                        for side_y, y in ((1, j * ty), (0, j * ty + ty - 1)):
                            outer[side_y, j, c, 0:3] = S[c, x_at : x_at + 3, YB + y, :]

            _, on, y_at = y_side(side)

            @pl.when(on)
            def _():
                for c in comps:
                    ypack[c] = S[c, XB : XB + nx, y_at : y_at + 4, :]

    def strip_copies(comps):
        for side in range(2):
            edge, here, _ = x_side(side)
            for j in range(3):
                child = 3 * (b - fy) + j
                yield here & (child < cy), pltpu.make_async_remote_copy(
                    src_ref=xpack.at[comps, :, pl.ds(j * ty, ty), :], dst_ref=xstrip.at[comps],
                    send_sem=strip_send.at[j], recv_sem=strip_recv.at[0, 0],
                    device_id=(1, edge, child), device_id_type=MESH,
                )
                if comps.start > 0:
                    continue
                for side_y, beside in ((0, child + 1), (1, child - 1)):
                    yield here & (child < cy) & (beside >= 0) & (beside < cy), pltpu.make_async_remote_copy(
                        src_ref=outer.at[side_y, j], dst_ref=xouter.at[side_y],
                        send_sem=outer_send.at[side_y, j], recv_sem=strip_recv.at[0, 1 + side_y],
                        device_id=(1, edge, beside), device_id_type=MESH,
                    )
            edge, here, _ = y_side(side)
            for i in range(-1, 4):
                lo, hi, dst = y_windows[i]
                child = 3 * (a - fx) + i
                yield here & (child >= 0) & (child < cx), pltpu.make_async_remote_copy(
                    src_ref=ypack.at[comps, pl.ds(lo, hi - lo)],
                    dst_ref=ystrip.at[comps, pl.ds(dst, hi - lo)],
                    send_sem=strip_send.at[4 + i], recv_sem=strip_recv.at[1, kinds[i]],
                    device_id=(1, child, edge), device_id_type=MESH,
                )

    def strip_start(comps):
        for on, copy in strip_copies(comps):
            @pl.when(on)
            def _():
                copy.start()

    def strips_sent():
        for on, copy in strip_copies(slice(0, 3)):
            @pl.when(on)
            def _():
                copy.wait_send()

    def strip_wait(ref, kind):
        pltpu.make_async_remote_copy(
            src_ref=ref, dst_ref=ref, send_sem=strip_send.at[0],
            recv_sem=strip_recv.at[kind], device_id=(g, a, b), device_id_type=MESH,
        ).wait_recv()

    def wait_y_strips():
        def rows(kind, lo, hi, dst):
            strip_wait(ystrip.at[:, pl.ds(dst, hi - lo), :, :], (1, kind))

        for i in range(3):
            @pl.when(a % 3 == i)
            def _():
                rows(0, *y_windows[i])

        @pl.when((a % 3 == 2) & (a < cx - 1))
        def _():
            rows(1, *y_windows[-1])

        @pl.when((a % 3 == 0) & (a > 0))
        def _():
            rows(2, *y_windows[3])

    def wait_x_strips():
        strip_wait(xstrip, (0, 0))

        @pl.when(b > 0)
        def _():
            strip_wait(xouter.at[0], (0, 1))

        @pl.when(b < cy - 1)
        def _():
            strip_wait(xouter.at[1], (0, 2))

    def relax_at(x, y):
        gx, gy = a * nx + x, b * ny + y
        depth = jnp.minimum(
            jnp.minimum(gx, nx * cx - 1 - gx), jnp.minimum(gy, ny * cy - 1 - gy)
        ).astype(F32)
        return jnp.maximum(1.0 - depth / BAND, 0.0)

    def mixed(weights, source):
        w_high, w_low = split(weights)
        s_high, s_low = split(source)
        return dot(w_high, s_high) + (dot(w_low, s_high) + dot(w_high, s_low))

    def y_edge(col):
        shape = (nx, 8, lev)
        relax = relax_at(
            lax.broadcasted_iota(jnp.int32, shape, 0), col + lax.broadcasted_iota(jnp.int32, shape, 1)
        )
        for c in range(3):
            bound = mixed(wy[...], ystrip[c].reshape(4 * (tx + 2), lev)).reshape(shape)
            at = (c, slice(XB, XB + nx), slice(YB + col, YB + col + 8), slice(None))
            now = S[at]
            S[at] = now + relax * (bound - now)

    def x_edge(first):
        shape = (BAND, ny, lev)
        relax = relax_at(
            first + lax.broadcasted_iota(jnp.int32, shape, 0), lax.broadcasted_iota(jnp.int32, shape, 1)
        )
        for c in range(3):
            source = jnp.concatenate(
                [xstrip[c].reshape(3 * ty, lev), xouter[0, c], xouter[1, c]], axis=0
            )
            bound = mixed(wx[...], source).reshape(shape)
            now = saved[c]
            S[c, XB + first : XB + first + BAND, YB : YB + ny, :] = now + relax * (bound - now)

    for k in range(SUBS):
        if k == 0:
            send_edges(0, (0, 1, 2, 3))

        @pl.when(g == 1)
        def _():
            if k == 0:
                with jax.named_scope("restrict_weights"):
                    restrict_weights()
            else:
                with jax.named_scope(f"mean{k}"):
                    gather_mean(k - 1)

        last = k == SUBS - 1
        with jax.named_scope(f"inner_winds{k}"):
            inner_winds()
        if last:
            @pl.when(g == 1)
            def _():
                with jax.named_scope("restrict_u"):
                    restrict(1, range(1, quarter))
                fb_start(0)

        with jax.named_scope(f"inner_pressure{k}"):
            inner_pressure()
        if k == 1:
            @pl.when((g == 1) & ((a == 0) | (a == cx - 1) | (b == 0) | (b == cy - 1)))
            def _():
                with jax.named_scope("boundary_weights"):
                    boundary_weights()
        with jax.named_scope(f"receive_y{k}"):
            receive(k, (2, 3))
        edge_winds_y()
        if last:
            @pl.when(g == 1)
            def _():
                with jax.named_scope("restrict_v"):
                    restrict(2, range(quarter))
                fb_start(1)

            @pl.when(g == 0)
            def _():
                strip_pack((2,))
                strip_start(slice(2, 3))
        outer_tile = (b == 0) | (b == cy - 1)

        def columns():
            with jax.named_scope(f"edge_columns{k}"):
                edge_columns()

        if last:
            columns()

            @pl.when(g == 1)
            def _():
                restrict(0, range(1, quarter))
                pressure_home(slice(3, 3 * quarter)).start()
        else:
            pl.when(outer_tile)(columns)
        with jax.named_scope(f"receive_x{k}"):
            receive(k, (0, 1))
        edge_winds_x()
        if last:
            @pl.when(g == 1)
            def _():
                restrict(1, (0,))
                fb_start(2)

            @pl.when(g == 0)
            def _():
                strip_pack((1,))
                strip_start(slice(1, 2))
        with jax.named_scope(f"edge_rows{k}"):
            edge_rows()
            if not last:
                send_edges(k + 1, (0, 1))
        if not last:
            pl.when(jnp.logical_not(outer_tile))(columns)
            send_edges(k + 1, (2, 3))

    def arrived(i, comps):
        first = comps[0]
        for count in range(1, 4):
            here = (a >= fx) & (b >= fy) & (3 * (a - fx) + i < cx)

            @pl.when(here & (jnp.minimum(cy - 3 * (b - fy), 3) == count))
            def _():
                row = fb.at[3 * i : 3 * i + count, first : first + len(comps)]
                hop(row, row, (g, a, b), fb_send.at[0], fb_recv.at[i, min(first, 1)]).wait_recv()

    def take(i, j, comps):
        for c in comps:
            for n in range(quarter):
                got = fb[3 * i + j, c, 3 * n : 3 * n + 3]
                rows = [got[m, :, :lev] for m in range(3)]
                rows.append(jnp.concatenate([got[m, :, lev : lev + slot] for m in range(3)], axis=1))
                for u, value in zip(rows_of(n), rows):
                    at = (c, XB + i * tx + u, slice(YB + j * ty, YB + (j + 1) * ty), slice(None))
                    now = S[at]
                    S[at] = now + FEEDBACK * (value - now)

    @pl.when(g == 1)
    def _():
        with jax.named_scope("restrict_pressure"):
            restrict(0, (0,))
        pressure_home(slice(0, 3)).start()
        halo_sent(SUBS - 1)
        x_low, x_high = a == 0, a == cx - 1
        y_low, y_high = b == 0, b == cy - 1

        @pl.when(x_low)
        def _():
            for c in range(3):
                saved[c] = S[c, XB : XB + BAND, YB : YB + ny, :]

        @pl.when(x_high)
        def _():
            for c in range(3):
                saved[c] = S[c, XB + nx - BAND : XB + nx, YB : YB + ny, :]

        @pl.when(x_low | x_high)
        def _():
            @pl.when(y_low)
            def _():
                xouter[0] = jnp.zeros((3, 4, lev), F32)

            @pl.when(y_high)
            def _():
                xouter[1] = jnp.zeros((3, 4, lev), F32)

        @pl.when(y_low | y_high)
        def _():
            @pl.when(x_low)
            def _():
                ystrip[:, 0:1] = jnp.zeros((3, 1, 4, lev), F32)

            if (cx - 1) % 3 == 2:

                @pl.when(x_high)
                def _():
                    ystrip[:, tx + 1 : tx + 2] = jnp.zeros((3, 1, 4, lev), F32)

            with jax.named_scope("wait_y"):
                wait_y_strips()

        @pl.when(y_low)
        def _():
            with jax.named_scope("y_low"):
                y_edge(0)

        @pl.when(y_high)
        def _():
            with jax.named_scope("y_high"):
                y_edge(ny - 8)

        @pl.when(x_low | x_high)
        def _():
            with jax.named_scope("wait_x"):
                wait_x_strips()

        @pl.when(x_low)
        def _():
            with jax.named_scope("x_low_edge"):
                x_edge(0)

        @pl.when(x_high)
        def _():
            with jax.named_scope("x_high_edge"):
                x_edge(nx - BAND)

        for part, comps in ((1, slice(1, 3)), (0, slice(0, 1))):
            piece = rst.at[comps]
            hop(piece, piece, (g, a, b), fb_send.at[part], q_recv.at[0]).wait_send()

    @pl.when(g == 0)
    def _():
        strip_pack((0,))
        strip_start(slice(0, 1))
        with jax.named_scope("pass_parent"):
            pass_on()
        halo_sent(SUBS - 1)
        passed_on()
        winds_of, pressure_of = (1, 2), (0,)
        for i, comps in (
            (1, winds_of), (1, pressure_of), (2, winds_of), (0, pressure_of), (2, pressure_of), (0, winds_of)
        ):
            with jax.named_scope(f"row{i}{comps[0]}"):
                arrived(i, comps)
            for j in range(3):
                there = (a >= fx) & (b >= fy) & (3 * (a - fx) + i < cx) & (3 * (b - fy) + j < cy)

                @pl.when(there)
                def _():
                    take(i, j, comps)

        strips_sent()


def store(padded, out, sem):
    nx, ny = out.shape[2], out.shape[3]
    copy = pltpu.make_async_copy(
        padded.at[:, pl.ds(XB, nx), pl.ds(YB, ny), :], out.at[0], sem.at[0]
    )
    copy.start()
    copy.wait()


def per_device(
    state, courant, vert_inverse, interp_index, interp_weight, restrict_index, restrict_weight
):
    cx, cy = lax.axis_size("gx"), lax.axis_size("gy")
    _, _, nx, ny, lev = state.shape
    tx, ty = nx // 3, ny // 3
    packed = (3 * (tx // 4), ty, 128)
    vmem = lambda *shape: pltpu.VMEM(shape, F32)
    dma = pltpu.SemaphoreType.DMA
    anywhere = pl.BlockSpec(memory_space=pltpu.HBM)
    inside = pl.BlockSpec(memory_space=pltpu.VMEM)
    padded = pl.pallas_call(
        functools.partial(kernel, cx, cy),
        out_shape=vmem(3, nx + 4, ny + 16, lev),
        in_specs=[anywhere] * 7,
        out_specs=inside,
        scratch_shapes=[
            vmem(nx + 2, ny + 16, lev),
            vmem(lev, 1, lev),
            pltpu.VMEM((nx, 4, ny), jnp.int32),
            vmem(nx, 4, ny),
            pltpu.VMEM((9, tx, ty), jnp.int32),
            vmem(9, tx, ty),
            vmem(3, BAND, ny, lev),
            vmem(3, tx, ty, lev),
            vmem(tx, 9, ty, lev),
            vmem(BAND * ny, 3 * ty + 8),
            vmem(nx * 8, 4 * (tx + 2)),
            vmem(2, 4, ny, lev),
            vmem(2, nx, 4, lev),
            vmem(2, 4, ny, lev),
            vmem(2, nx, 4, lev),
            vmem(SUBS - 1, 2, 2, ny, lev),
            vmem(SUBS - 1, 2, nx, 2, lev),
            vmem(SUBS - 1, 2, 2, ny, lev),
            vmem(SUBS - 1, 2, nx, 2, lev),
            vmem(3, *packed),
            vmem(9, 3, *packed),
            vmem(3, 3, ty, lev),
            vmem(2, 3, 4, lev),
            vmem(3, tx + 2, 4, lev),
            dma((7,)),
            dma((4,)),
            dma((2, 4)),
            dma((8,)),
            dma((2, 3)),
            dma((2,)),
            dma((3, 2)),
            vmem(6, 2, *packed),
            vmem(3, 3, ny, lev),
            vmem(2, 3, 3, 4, lev),
            vmem(3, nx, 4, lev),
            dma((6,)),
            dma((15,)),
            dma((2, 3)),
        ],
        compiler_params=pltpu.CompilerParams(
            has_side_effects=True, collective_id=0, vmem_limit_bytes=67043328 - 4 * (3 * (nx + 4) * (ny + 16) * 128) - 2**14
        ),
        name="nest_step",
    )(
        state, courant, vert_inverse.transpose(1, 0, 2),
        interp_index.transpose(0, 2, 1), interp_weight.transpose(0, 2, 1),
        restrict_index.transpose(2, 0, 1), restrict_weight.transpose(2, 0, 1),
    )
    return pl.pallas_call(
        store, out_shape=jax.ShapeDtypeStruct(state.shape, F32), in_specs=[inside], out_specs=anywhere,
        scratch_shapes=[dma((1,))], name="store",
        compiler_params=pltpu.CompilerParams(vmem_limit_bytes=2**20),
    )(padded)


def solution(mesh):
    return jax.shard_map(
        per_device,
        mesh=mesh,
        in_specs=(
            P("grp", None, "gx", "gy", None),
            P("grp", "gx", "gy", None),
            P("grp", None, None),
            P("gx", "gy", None),
            P("gx", "gy", None),
            P("gx", "gy", None),
            P("gx", "gy", None),
        ),
        out_specs=P("grp", None, "gx", "gy", None),
        check_vma=False,
    )
```

```python
import functools

import jax
import jax.numpy as jnp
from jax import lax
from jax.experimental import pallas as pl
from jax.experimental.pallas import tpu as pltpu
from jax.sharding import PartitionSpec as P

SUBS = 4
BAND = 5
FEEDBACK = 0.5
MESH = pl.DeviceIdType.MESH
F32 = jnp.float32
XB, YB = 2, 8


def split(a):
    high = a.astype(jnp.bfloat16)
    return high, (a - high.astype(F32)).astype(jnp.bfloat16)


def dot(a, b):
    return jnp.dot(a, b, preferred_element_type=F32)


def dot3(a, b_high, b_low):
    a_high, a_low = split(a)
    return dot(a_high, b_high) + (dot(a_low, b_high) + dot(a_high, b_low))


def third(t):
    return (t * 11) >> 5


def kernel(
    cx, cy,
    state, courant, *rest,
):
    small, (
    S,
    C, inverse, iidx, iwgt, ridx, rwgt, saved, racc, wr, wx, wy, sx0, sy0, rx0, ry0, sx, sy, rx, ry, rst, fb, xstrip, xouter, ystrip,
    load_sem, halo_send, halo_recv, strip_send, strip_recv, fb_send, fb_recv,
    q0, xpack, outer, ypack, q_send, q_recv, outer_send,
    ) = rest[:5], rest[5:]
    g, a, b = lax.axis_index("grp"), lax.axis_index("gx"), lax.axis_index("gy")
    nx, ny, lev = state.shape[2], state.shape[3], state.shape[4]
    tx, ty = nx // 3, ny // 3
    fx, fy = cx // 2, cy // 2
    quarter, slot = tx // 4, lev // 3

    barrier = pltpu.get_barrier_semaphore()
    greeted = []

    def greet(on, device):
        greeted.append(on)

        @pl.when(on)
        def _():
            pl.semaphore_signal(barrier, inc=1, device_id=device, device_id_type=MESH)

    for i in range(-1, 4):
        for j in range(-1, 4):
            child_a, child_b = 3 * (a - fx) + i, 3 * (b - fy) + j
            greet(
                (g == 0) & (a >= fx) & (b >= fy) & (child_a >= 0) & (child_a < cx)
                & (child_b >= 0) & (child_b < cy),
                (1, child_a, child_b),
            )

    def parents(place, first, count):
        own = first + place // 3
        return (
            (place >= 0, own),
            ((place % 3 == 0) & (place > 0), own - 1),
            ((place % 3 == 2) & (own + 1 < count), own + 1),
        )

    for on_a, parent_a in parents(a, fx, cx):
        for on_b, parent_b in parents(b, fy, cy):
            greet((g == 1) & on_a & on_b, (0, parent_a, parent_b))

    loads = [
        pltpu.make_async_copy(
            state.at[0], S.at[:, pl.ds(XB, nx), pl.ds(YB, ny), :], load_sem.at[0]
        ),
        pltpu.make_async_copy(
            courant.at[0], C.at[pl.ds(1, nx), pl.ds(YB, ny), :], load_sem.at[1]
        ),
    ]
    for n, (src, dst) in enumerate(zip(small, (inverse, iidx, iwgt, ridx, rwgt))):
        loads.append(pltpu.make_async_copy(src, dst, load_sem.at[2 + n]))
    for copy in loads:
        copy.start()

    def relay_of(at_a):
        to_a = fx + at_a // 3
        back = (at_a % 3 == 0) & (at_a != to_a)
        on = (at_a % 3 == 2) & (to_a + 1 < cx)
        return to_a, back, on

    to_a, back, on_next = relay_of(a)
    to_b = fy + b // 3
    parent, nest = g == 0, g == 1
    via = back | on_next
    relay_a = jnp.where(back, a, to_a + 1)
    greet(nest & via, (0, relay_a, to_b))
    relayed = []
    next_a = 3 * (a - 1 - fx) + 2
    for from_a, lane, i, here in (
        (a, 0, 0, back), (next_a, 1, 2, (a - 1 >= fx) & (next_a < cx)),
    ):
        for j in range(3):
            from_b = 3 * (b - fy) + j
            on = parent & here & (b >= fy) & (from_b < cy)
            relayed.append((on, 3 * lane + j, i, j, fx + from_a // 3))
            greet(on, (1, from_a, from_b))
        greet(relayed[-3][0], (0, fx + from_a // 3, b))
    for i in range(3):
        from_a = 3 * (a - fx) + i
        on = parent & (a >= fx) & (b >= fy) & (from_a < cx)
        _, from_back, from_next = relay_of(from_a)
        greet(on & from_back, (0, from_a, b))
        greet(on & from_next, (0, a + 1, b))

    greet(a > 0, (g, a - 1, b))
    greet(a < cx - 1, (g, a + 1, b))
    greet(b > 0, (g, a, b - 1))
    greet(b < cy - 1, (g, a, b + 1))
    zrow = jnp.zeros((2, ny, lev), F32)
    S[0, 0:2, YB : YB + ny, :] = zrow
    S[0, XB + nx : XB + nx + 2, YB : YB + ny, :] = zrow
    S[1, 0:2, YB : YB + ny, :] = zrow
    S[1, XB + nx : XB + nx + 2, YB : YB + ny, :] = zrow
    C[0:1, YB : YB + ny, :] = zrow[0:1]
    C[nx + 1 : nx + 2, YB : YB + ny, :] = zrow[0:1]
    outer[...] = jnp.zeros((2, 3, 3, 4, lev), F32)
    zcol = jnp.zeros((nx, 8, lev), F32)
    for c in (0, 2):
        S[c, XB : XB + nx, 0:YB, :] = zcol
        S[c, XB : XB + nx, YB + ny : YB + ny + 8, :] = zcol
    C[1 : 1 + nx, 0:YB, :] = zcol
    C[1 : 1 + nx, YB + ny : YB + ny + 8, :] = zcol
    with jax.named_scope("loads"):
        for copy in loads:
            copy.wait()
    m_high, m_low = split(inverse[:, 0, :])
    with jax.named_scope("greet"):
        pl.semaphore_wait(barrier, sum(on.astype(jnp.int32) for on in greeted))

    dirs = (
        (a > 0, a < cx - 1, (g, a - 1, b)),
        (a < cx - 1, a > 0, (g, a + 1, b)),
        (b > 0, b < cy - 1, (g, a, b - 1)),
        (b < cy - 1, b > 0, (g, a, b + 1)),
    )

    def halo_copy(k, d):
        if k == 0:
            src, dst = (sx0, rx0) if d < 2 else (sy0, ry0)
            src, dst = src.at[d % 2], dst.at[d % 2]
        else:
            src, dst = (sx, rx) if d < 2 else (sy, ry)
            src, dst = src.at[k - 1, d % 2], dst.at[k - 1, d % 2]
        return pltpu.make_async_remote_copy(
            src_ref=src, dst_ref=dst,
            send_sem=halo_send.at[d], recv_sem=halo_recv.at[k % 2, d],
            device_id=dirs[d][2], device_id_type=MESH,
        )

    def halo_sent(k):
        for d in range(4):
            @pl.when(dirs[d][0])
            def _():
                halo_copy(k, d).wait_send()

    def send_edges(k, which):
        rows = slice(XB, XB + nx)
        last_x, last_y = XB + nx, YB + ny
        cols = slice(YB, last_y)
        if k == 0:
            sx0[0, 0:2] = S[0, XB : XB + 2, cols, :]
            sx0[0, 2:3] = S[1, XB : XB + 1, cols, :]
            sx0[0, 3:4] = C[1:2, cols, :]
            sx0[1, 0:2] = S[0, last_x - 2 : last_x, cols, :]
            sx0[1, 2:3] = S[1, last_x - 1 : last_x, cols, :]
            sx0[1, 3:4] = C[nx : nx + 1, cols, :]
            sy0[0, :, 0:2] = S[0, rows, YB : YB + 2, :]
            sy0[0, :, 2:3] = S[2, rows, YB : YB + 1, :]
            sy0[0, :, 3:4] = C[1 : 1 + nx, YB : YB + 1, :]
            sy0[1, :, 0:2] = S[0, rows, last_y - 2 : last_y, :]
            sy0[1, :, 2:3] = S[2, rows, last_y - 1 : last_y, :]
            sy0[1, :, 3:4] = C[1 : 1 + nx, last_y - 1 : last_y, :]
        elif 0 in which:
            sx[k - 1, 0] = S[0, XB : XB + 2, cols, :]
            sx[k - 1, 1] = S[0, last_x - 2 : last_x, cols, :]
        else:
            sy[k - 1, 0] = S[0, rows, YB : YB + 2, :]
            sy[k - 1, 1] = S[0, rows, last_y - 2 : last_y, :]
        for d in which:
            @pl.when(dirs[d][0])
            def _():
                if k > 0:
                    halo_copy(k - 1, d).wait_send()
                halo_copy(k, d).start()

    def receive(k, which):
        cols = slice(YB, YB + ny)
        rows = slice(XB, XB + nx)
        last_x, last_y = XB + nx, YB + ny
        for d in which:
            @pl.when(dirs[d][1])
            def _():
                halo_copy(k, d).wait_recv()
                if d < 2:
                    got = rx0.at[d] if k == 0 else rx.at[k - 1, d]
                    at = last_x if d == 0 else XB - 2
                    S[0, at : at + 2, cols, :] = got[0:2]
                    if k == 0:
                        at = last_x if d == 0 else XB - 1
                        S[1, at : at + 1, cols, :] = got[2:3]
                        C[at - 1 : at, cols, :] = got[3:4]
                else:
                    got = ry0.at[d - 2] if k == 0 else ry.at[k - 1, d - 2]
                    at = last_y if d == 2 else YB - 2
                    S[0, rows, at : at + 2, :] = got[:, 0:2]
                    if k == 0:
                        at = last_y if d == 2 else YB - 1
                        S[2, rows, at : at + 1, :] = got[:, 2:3]
                        C[1 : 1 + nx, at : at + 1, :] = got[:, 3:4]

    cols = slice(YB, YB + ny)

    def u_row(r):
        slope = 0.5 * (S[0, r + 1, cols, :] - S[0, r - 1, cols, :])
        return S[1, r, cols, :] - C[r - 1, cols, :] * slope

    def v_row(r):
        mid = slice(YB + 1, YB + ny - 1)
        slope = 0.5 * (S[0, r, YB + 2 : YB + ny, :] - S[0, r, YB : YB + ny - 2, :])
        return S[2, r, mid, :] - C[r - 1, mid, :] * slope

    def inner_winds():
        group = 4

        def some(us, vs):
            new = [(1, r, cols, u_row(r)) for r in us]
            new += [(2, r, slice(YB + 1, YB + ny - 1), v_row(r)) for r in vs]
            for c, r, at, value in new:
                S[c, r, at, :] = value

        def rows(i, _):
            some(*[[XB + 2 + i * group + j for j in range(group)]] * 2)
            return 0

        first, last = XB, XB + nx - 1
        some((first + 1, last - 1), (first, first + 1, last - 1, last))
        lax.fori_loop(0, (nx - 4) // group, rows, 0)

    def edge_winds_x():
        new = [(r, u_row(r)) for r in (XB - 1, XB, XB + nx - 1, XB + nx)]
        for r, value in new:
            S[1, r, cols, :] = value

    def edge_winds_y():
        rows = slice(XB, XB + nx)
        for y in (YB - 1, YB + ny - 1):
            slope = 0.5 * (S[0, rows, y + 1 : y + 3, :] - S[0, rows, y - 1 : y + 1, :])
            S[2, rows, y : y + 2, :] = S[2, rows, y : y + 2, :] - C[1 : 1 + nx, y : y + 2, :] * slope

    def forced(r, y, width):
        at = slice(y, y + width)
        div = 0.5 * (S[1, r + 1, at, :] - S[1, r - 1, at, :]) + 0.5 * (
            S[2, r, y + 1 : y + width + 1, :] - S[2, r, y - 1 : y + width - 1, :]
        )
        return S[0, r, at, :] - C[r - 1, at, :] * div

    def solved(parts):
        return dot3(jnp.concatenate(parts, axis=0), m_high, m_low)

    def inner_pressure():
        group = 8

        def rows(i, _):
            first = XB + 2 + i * group
            new = solved([forced(first + j, YB, ny) for j in range(group)])
            for j in range(group):
                S[0, first + j, YB + 2 : YB + ny - 2, :] = new[j * ny + 2 : (j + 1) * ny - 2]
            return 0

        lax.fori_loop(0, (nx - 4) // group, rows, 0)

    def edge_rows():
        rows = (XB, XB + 1, XB + nx - 2, XB + nx - 1)
        new = solved([forced(r, YB, ny) for r in rows])
        for n, r in enumerate(rows):
            S[0, r, cols, :] = new[n * ny : (n + 1) * ny]

    def edge_columns():
        sides = [(r, y) for y in (YB, YB + ny - 8) for r in range(XB + 2, XB + nx - 2)]
        new = solved([forced(r, y, 8) for r, y in sides])
        for n, (r, y) in enumerate(sides):
            skip = 0 if y == YB else 6
            S[0, r, y + skip : y + skip + 2, :] = new[8 * n + skip : 8 * n + skip + 2]

    def hop(src, dst, device, send, recv):
        return pltpu.make_async_remote_copy(
            src_ref=src, dst_ref=dst, send_sem=send, recv_sem=recv,
            device_id=device, device_id_type=MESH,
        )

    chunks = ((1, slice(3, 3 * quarter)), (2, slice(0, 3 * quarter)), (1, slice(0, 3)))

    def home(src, c, part, i, j, device, send):
        n = 3 * i + j
        return hop(src, fb.at[n, c, part], device, send, fb_recv.at[i, min(c, 1)])

    def pressure_home(part):
        return home(rst.at[0, part], 0, part, a % 3, b % 3, (0, to_a, to_b), fb_send.at[0])

    def q_slot(at, n):
        return 6 * n + at

    def fb_start(n):
        c, part = chunks[n]
        mine, sem = rst.at[c, part], fb_send.at[1]
        around = via if n < 2 else back

        @pl.when(jnp.logical_not(around))
        def _():
            home(mine, c, part, a % 3, b % 3, (0, to_a, to_b), sem).start()

        @pl.when(around)
        def _():
            at = jnp.where(back, 0, 3) + b % 3
            hop(mine, q0.at[at, c - 1, part], (0, relay_a, to_b), sem, q_recv.at[q_slot(at, n)]).start()

    def pass_on():
        for n, (c, part) in enumerate(chunks):
            for on, at, i, j, home_a in relayed[: 6 if n < 2 else 3]:
                @pl.when(on)
                def _():
                    piece = q0.at[at, c - 1, part]
                    hop(piece, piece, (g, a, b), q_send.at[at], q_recv.at[q_slot(at, n)]).wait_recv()
                    home(piece, c, part, i, j, (0, home_a, b), q_send.at[at]).start()

    def passed_on():
        for on, at, _, _, _ in relayed:
            @pl.when(on)
            def _():
                sent = [q0.at[at]] if at < 3 else [q0.at[at, 0, chunks[0][1]], q0.at[at, 1]]
                for piece in sent:
                    hop(piece, piece, (g, a, b), q_send.at[at], q_recv.at[0]).wait_send()

    def rows_of(i):
        if i == 0:
            return 0, tx - 1, 1, 2
        return tuple(4 * i - 1 + m for m in range(4))

    def mixed_row(c, u):
        total = None
        for t in range(9):
            part = wr[u, t] * S[c, XB + 3 * u + t // 3, pl.ds(YB + t % 3, ty, stride=3), :]
            total = part if total is None else total + part
        return total

    def gather_mean(k):
        def rows(u, _):
            new = [mixed_row(c, u) for c in range(3)]
            for c in range(3):
                racc[c, u] = new[c] if k == 0 else racc[c, u] + new[c]
            return 0

        lax.fori_loop(0, tx, rows, 0)

    def restrict(c, groups):
        spare = jnp.zeros((ty, 128 - lev - slot), F32)
        for i in groups:
            own = [racc[c, u] + mixed_row(c, u) for u in rows_of(i)]
            for m in range(3):
                part = own[3][:, m * slot : (m + 1) * slot]
                rst[c, 3 * i + m] = jnp.concatenate([own[m], part, spare], axis=1)

    def restrict_weights():
        terms = range(ridx.shape[0])
        w = [rwgt[k] for k in terms]
        scale = (1.0 / SUBS) / row_sum(w)
        shares = [part * scale for part in w]
        index = [ridx[k] for k in terms]
        for t in range(9):
            at = row_sum([jnp.where(index[k] == t, shares[k], 0.0) for k in terms]).T
            for u in range(tx):
                wr[u, t] = jnp.broadcast_to(at[:, u : u + 1], (ty, lev))

    def boundary_weights():
        share = iwgt[...] / jnp.sum(iwgt[...], axis=1, keepdims=True)
        share = share.reshape(nx * 4, ny).T
        index = iidx[...].astype(F32).reshape(nx * 4, ny).T.astype(jnp.int32)
        over = third(index)
        shape = index.shape
        x3 = (lax.broadcasted_iota(jnp.int32, shape, 1) * 171) >> 11
        y3 = (lax.broadcasted_iota(jnp.int32, shape, 0) * 171) >> 9
        source_x = jnp.clip(a * tx + x3 + over - 1, 0, cx * tx - 1)
        source_y = jnp.clip(b * ty + y3 + (index - 3 * over) - 1, 0, cy * ty - 1)

        def spread(cells, parts, x, depth):
            places = lax.broadcasted_iota(jnp.int32, (cells.shape[0], depth), 1)
            total = jnp.zeros(places.shape, F32)
            for n in range(4 * x, 4 * x + 4):
                total = total + jnp.where(places == cells[:, n : n + 1], parts[:, n : n + 1], 0.0)
            return total

        def y_weights(col, strip0):
            cells = (source_x - (a * tx - 1)) * 4 + source_y - (b * ty + strip0)
            cells, parts = cells[col : col + 8], share[col : col + 8]
            for x in range(nx):
                wy[8 * x : 8 * x + 8] = spread(cells, parts, x, 4 * (tx + 2))

        def x_weights(first, strip0):
            row, column = source_x - (a * tx + strip0), source_y - b * ty
            cells = jnp.where(
                column < 0, 3 * ty + row, jnp.where(column < ty, row * ty + column, 3 * ty + 4 + row)
            )
            for i in range(BAND):
                wx[ny * i : ny * i + ny] = spread(cells, share, first + i, 3 * ty + 8)

        @pl.when(b == 0)
        def _():
            y_weights(0, 0)

        @pl.when(b == cy - 1)
        def _():
            y_weights(ny - 8, ty - 4)

        @pl.when(a == 0)
        def _():
            x_weights(0, 0)

        @pl.when(a == cx - 1)
        def _():
            x_weights(nx - BAND, tx - 3)

    def row_sum(rows):
        total = rows[0]
        for row in rows[1:]:
            total = total + row
        return total

    y_windows = {-1: (0, 1, tx + 1), 0: (0, tx + 1, 1), 1: (tx - 1, 2 * tx + 1, 0),
                 2: (2 * tx - 1, nx, 0), 3: (nx - 1, nx, 0)}
    kinds = {-1: 1, 0: 0, 1: 0, 2: 0, 3: 2}

    def x_side(side):
        edge = 0 if side == 0 else cx - 1
        at = XB if side == 0 else XB + tx * (edge % 3) + tx - 3
        return edge, (a == fx + edge // 3) & (b >= fy), at

    def y_side(side):
        edge = 0 if side == 0 else cy - 1
        at = YB if side == 0 else YB + ty * (edge % 3) + ty - 4
        return edge, (b == fy + edge // 3) & (a >= fx), at

    def strip_pack(comps):
        for side in range(2):
            _, on, x_at = x_side(side)

            @pl.when(on)
            def _():
                for c in comps:
                    xpack[c] = S[c, x_at : x_at + 3, YB : YB + ny, :]
                    for j in range(3):
                        for side_y, y in ((1, j * ty), (0, j * ty + ty - 1)):
                            outer[side_y, j, c, 0:3] = S[c, x_at : x_at + 3, YB + y, :]

            _, on, y_at = y_side(side)

            @pl.when(on)
            def _():
                for c in comps:
                    ypack[c] = S[c, XB : XB + nx, y_at : y_at + 4, :]

    def strip_copies(comps):
        for side in range(2):
            edge, here, _ = x_side(side)
            for j in range(3):
                child = 3 * (b - fy) + j
                yield here & (child < cy), pltpu.make_async_remote_copy(
                    src_ref=xpack.at[comps, :, pl.ds(j * ty, ty), :], dst_ref=xstrip.at[comps],
                    send_sem=strip_send.at[j], recv_sem=strip_recv.at[0, 0],
                    device_id=(1, edge, child), device_id_type=MESH,
                )
                if comps.start > 0:
                    continue
                for side_y, beside in ((0, child + 1), (1, child - 1)):
                    yield here & (child < cy) & (beside >= 0) & (beside < cy), pltpu.make_async_remote_copy(
                        src_ref=outer.at[side_y, j], dst_ref=xouter.at[side_y],
                        send_sem=outer_send.at[side_y, j], recv_sem=strip_recv.at[0, 1 + side_y],
                        device_id=(1, edge, beside), device_id_type=MESH,
                    )
            edge, here, _ = y_side(side)
            for i in range(-1, 4):
                lo, hi, dst = y_windows[i]
                child = 3 * (a - fx) + i
                yield here & (child >= 0) & (child < cx), pltpu.make_async_remote_copy(
                    src_ref=ypack.at[comps, pl.ds(lo, hi - lo)],
                    dst_ref=ystrip.at[comps, pl.ds(dst, hi - lo)],
                    send_sem=strip_send.at[4 + i], recv_sem=strip_recv.at[1, kinds[i]],
                    device_id=(1, child, edge), device_id_type=MESH,
                )

    def strip_start(comps):
        for on, copy in strip_copies(comps):
            @pl.when(on)
            def _():
                copy.start()

    def strips_sent():
        for on, copy in strip_copies(slice(0, 3)):
            @pl.when(on)
            def _():
                copy.wait_send()

    def strip_wait(ref, kind):
        pltpu.make_async_remote_copy(
            src_ref=ref, dst_ref=ref, send_sem=strip_send.at[0],
            recv_sem=strip_recv.at[kind], device_id=(g, a, b), device_id_type=MESH,
        ).wait_recv()

    def wait_y_strips():
        def rows(kind, lo, hi, dst):
            strip_wait(ystrip.at[:, pl.ds(dst, hi - lo), :, :], (1, kind))

        for i in range(3):
            @pl.when(a % 3 == i)
            def _():
                rows(0, *y_windows[i])

        @pl.when((a % 3 == 2) & (a < cx - 1))
        def _():
            rows(1, *y_windows[-1])

        @pl.when((a % 3 == 0) & (a > 0))
        def _():
            rows(2, *y_windows[3])

    def wait_x_strips():
        strip_wait(xstrip, (0, 0))

        @pl.when(b > 0)
        def _():
            strip_wait(xouter.at[0], (0, 1))

        @pl.when(b < cy - 1)
        def _():
            strip_wait(xouter.at[1], (0, 2))

    def relax_at(x, y):
        gx, gy = a * nx + x, b * ny + y
        depth = jnp.minimum(
            jnp.minimum(gx, nx * cx - 1 - gx), jnp.minimum(gy, ny * cy - 1 - gy)
        ).astype(F32)
        return jnp.maximum(1.0 - depth / BAND, 0.0)

    def mixed(weights, source):
        w_high, w_low = split(weights)
        s_high, s_low = split(source)
        return dot(w_high, s_high) + (dot(w_low, s_high) + dot(w_high, s_low))

    def y_edge(col):
        shape = (nx, 8, lev)
        relax = relax_at(
            lax.broadcasted_iota(jnp.int32, shape, 0), col + lax.broadcasted_iota(jnp.int32, shape, 1)
        )
        for c in range(3):
            bound = mixed(wy[...], ystrip[c].reshape(4 * (tx + 2), lev)).reshape(shape)
            at = (c, slice(XB, XB + nx), slice(YB + col, YB + col + 8), slice(None))
            now = S[at]
            S[at] = now + relax * (bound - now)

    def x_edge(first):
        shape = (BAND, ny, lev)
        relax = relax_at(
            first + lax.broadcasted_iota(jnp.int32, shape, 0), lax.broadcasted_iota(jnp.int32, shape, 1)
        )
        for c in range(3):
            source = jnp.concatenate(
                [xstrip[c].reshape(3 * ty, lev), xouter[0, c], xouter[1, c]], axis=0
            )
            bound = mixed(wx[...], source).reshape(shape)
            now = saved[c]
            S[c, XB + first : XB + first + BAND, YB : YB + ny, :] = now + relax * (bound - now)

    for k in range(SUBS):
        if k == 0:
            send_edges(0, (0, 1, 2, 3))

        @pl.when(g == 1)
        def _():
            if k == 0:
                with jax.named_scope("restrict_weights"):
                    restrict_weights()
            else:
                with jax.named_scope(f"mean{k}"):
                    gather_mean(k - 1)

        last = k == SUBS - 1
        with jax.named_scope(f"inner_winds{k}"):
            inner_winds()
        if last:
            @pl.when(g == 1)
            def _():
                with jax.named_scope("restrict_u"):
                    restrict(1, range(1, quarter))
                fb_start(0)

        with jax.named_scope(f"inner_pressure{k}"):
            inner_pressure()
        with jax.named_scope(f"receive_y{k}"):
            receive(k, (2, 3))
        edge_winds_y()
        if last:
            @pl.when(g == 1)
            def _():
                with jax.named_scope("restrict_v"):
                    restrict(2, range(quarter))
                fb_start(1)

            @pl.when(g == 0)
            def _():
                strip_pack((2,))
                strip_start(slice(2, 3))
        outer_tile = (b == 0) | (b == cy - 1)

        def columns():
            with jax.named_scope(f"edge_columns{k}"):
                edge_columns()

        if last:
            columns()

            @pl.when(g == 1)
            def _():
                restrict(0, range(1, quarter))
                pressure_home(slice(3, 3 * quarter)).start()
        else:
            pl.when(outer_tile)(columns)
        with jax.named_scope(f"receive_x{k}"):
            receive(k, (0, 1))
        edge_winds_x()
        if last:
            @pl.when(g == 1)
            def _():
                restrict(1, (0,))
                fb_start(2)

            @pl.when(g == 0)
            def _():
                strip_pack((1,))
                strip_start(slice(1, 2))
        with jax.named_scope(f"edge_rows{k}"):
            edge_rows()
            if not last:
                send_edges(k + 1, (0, 1))
        if not last:
            pl.when(jnp.logical_not(outer_tile))(columns)
            send_edges(k + 1, (2, 3))

    def arrived(i, comps):
        first = comps[0]
        for count in range(1, 4):
            here = (a >= fx) & (b >= fy) & (3 * (a - fx) + i < cx)

            @pl.when(here & (jnp.minimum(cy - 3 * (b - fy), 3) == count))
            def _():
                row = fb.at[3 * i : 3 * i + count, first : first + len(comps)]
                hop(row, row, (g, a, b), fb_send.at[0], fb_recv.at[i, min(first, 1)]).wait_recv()

    def take(i, j, comps):
        for c in comps:
            for n in range(quarter):
                got = fb[3 * i + j, c, 3 * n : 3 * n + 3]
                rows = [got[m, :, :lev] for m in range(3)]
                rows.append(jnp.concatenate([got[m, :, lev : lev + slot] for m in range(3)], axis=1))
                for u, value in zip(rows_of(n), rows):
                    at = (c, XB + i * tx + u, slice(YB + j * ty, YB + (j + 1) * ty), slice(None))
                    now = S[at]
                    S[at] = now + FEEDBACK * (value - now)

    @pl.when(g == 1)
    def _():
        with jax.named_scope("restrict_pressure"):
            restrict(0, (0,))
        pressure_home(slice(0, 3)).start()

        @pl.when((a == 0) | (a == cx - 1) | (b == 0) | (b == cy - 1))
        def _():
            with jax.named_scope("boundary_weights"):
                boundary_weights()

        halo_sent(SUBS - 1)
        x_low, x_high = a == 0, a == cx - 1
        y_low, y_high = b == 0, b == cy - 1

        @pl.when(x_low)
        def _():
            for c in range(3):
                saved[c] = S[c, XB : XB + BAND, YB : YB + ny, :]

        @pl.when(x_high)
        def _():
            for c in range(3):
                saved[c] = S[c, XB + nx - BAND : XB + nx, YB : YB + ny, :]

        @pl.when(x_low | x_high)
        def _():
            @pl.when(y_low)
            def _():
                xouter[0] = jnp.zeros((3, 4, lev), F32)

            @pl.when(y_high)
            def _():
                xouter[1] = jnp.zeros((3, 4, lev), F32)

        @pl.when(y_low | y_high)
        def _():
            @pl.when(x_low)
            def _():
                ystrip[:, 0:1] = jnp.zeros((3, 1, 4, lev), F32)

            if (cx - 1) % 3 == 2:

                @pl.when(x_high)
                def _():
                    ystrip[:, tx + 1 : tx + 2] = jnp.zeros((3, 1, 4, lev), F32)

            with jax.named_scope("wait_y"):
                wait_y_strips()

        @pl.when(y_low)
        def _():
            with jax.named_scope("y_low"):
                y_edge(0)

        @pl.when(y_high)
        def _():
            with jax.named_scope("y_high"):
                y_edge(ny - 8)

        @pl.when(x_low | x_high)
        def _():
            with jax.named_scope("wait_x"):
                wait_x_strips()

        @pl.when(x_low)
        def _():
            with jax.named_scope("x_low_edge"):
                x_edge(0)

        @pl.when(x_high)
        def _():
            with jax.named_scope("x_high_edge"):
                x_edge(nx - BAND)

        for part, comps in ((1, slice(1, 3)), (0, slice(0, 1))):
            piece = rst.at[comps]
            hop(piece, piece, (g, a, b), fb_send.at[part], q_recv.at[0]).wait_send()

    @pl.when(g == 0)
    def _():
        strip_pack((0,))
        strip_start(slice(0, 1))
        with jax.named_scope("pass_parent"):
            pass_on()
        halo_sent(SUBS - 1)
        passed_on()
        winds_of, pressure_of = (1, 2), (0,)
        for i, comps in (
            (1, winds_of), (1, pressure_of), (2, winds_of), (0, pressure_of), (2, pressure_of), (0, winds_of)
        ):
            with jax.named_scope(f"row{i}{comps[0]}"):
                arrived(i, comps)
            for j in range(3):
                there = (a >= fx) & (b >= fy) & (3 * (a - fx) + i < cx) & (3 * (b - fy) + j < cy)

                @pl.when(there)
                def _():
                    take(i, j, comps)

        strips_sent()


def store(padded, out, sem):
    nx, ny = out.shape[2], out.shape[3]
    copy = pltpu.make_async_copy(
        padded.at[:, pl.ds(XB, nx), pl.ds(YB, ny), :], out.at[0], sem.at[0]
    )
    copy.start()
    copy.wait()


def per_device(
    state, courant, vert_inverse, interp_index, interp_weight, restrict_index, restrict_weight
):
    cx, cy = lax.axis_size("gx"), lax.axis_size("gy")
    _, _, nx, ny, lev = state.shape
    tx, ty = nx // 3, ny // 3
    packed = (3 * (tx // 4), ty, 128)
    vmem = lambda *shape: pltpu.VMEM(shape, F32)
    dma = pltpu.SemaphoreType.DMA
    anywhere = pl.BlockSpec(memory_space=pltpu.HBM)
    inside = pl.BlockSpec(memory_space=pltpu.VMEM)
    padded = pl.pallas_call(
        functools.partial(kernel, cx, cy),
        out_shape=vmem(3, nx + 4, ny + 16, lev),
        in_specs=[anywhere] * 7,
        out_specs=inside,
        scratch_shapes=[
            vmem(nx + 2, ny + 16, lev),
            vmem(lev, 1, lev),
            pltpu.VMEM((nx, 4, ny), jnp.int32),
            vmem(nx, 4, ny),
            pltpu.VMEM((9, tx, ty), jnp.int32),
            vmem(9, tx, ty),
            vmem(3, BAND, ny, lev),
            vmem(3, tx, ty, lev),
            vmem(tx, 9, ty, lev),
            vmem(BAND * ny, 3 * ty + 8),
            vmem(nx * 8, 4 * (tx + 2)),
            vmem(2, 4, ny, lev),
            vmem(2, nx, 4, lev),
            vmem(2, 4, ny, lev),
            vmem(2, nx, 4, lev),
            vmem(SUBS - 1, 2, 2, ny, lev),
            vmem(SUBS - 1, 2, nx, 2, lev),
            vmem(SUBS - 1, 2, 2, ny, lev),
            vmem(SUBS - 1, 2, nx, 2, lev),
            vmem(3, *packed),
            vmem(9, 3, *packed),
            vmem(3, 3, ty, lev),
            vmem(2, 3, 4, lev),
            vmem(3, tx + 2, 4, lev),
            dma((7,)),
            dma((4,)),
            dma((2, 4)),
            dma((8,)),
            dma((2, 3)),
            dma((2,)),
            dma((3, 2)),
            vmem(6, 2, *packed),
            vmem(3, 3, ny, lev),
            vmem(2, 3, 3, 4, lev),
            vmem(3, nx, 4, lev),
            dma((6,)),
            dma((15,)),
            dma((2, 3)),
        ],
        compiler_params=pltpu.CompilerParams(
            has_side_effects=True, collective_id=0, vmem_limit_bytes=67043328 - 4 * (3 * (nx + 4) * (ny + 16) * 128) - 2**14
        ),
        name="nest_step",
    )(
        state, courant, vert_inverse.transpose(1, 0, 2),
        interp_index.transpose(0, 2, 1), interp_weight.transpose(0, 2, 1),
        restrict_index.transpose(2, 0, 1), restrict_weight.transpose(2, 0, 1),
    )
    return pl.pallas_call(
        store, out_shape=jax.ShapeDtypeStruct(state.shape, F32), in_specs=[inside], out_specs=anywhere,
        scratch_shapes=[dma((1,))], name="store",
        compiler_params=pltpu.CompilerParams(vmem_limit_bytes=2**20),
    )(padded)


def solution(mesh):
    return jax.shard_map(
        per_device,
        mesh=mesh,
        in_specs=(
            P("grp", None, "gx", "gy", None),
            P("grp", "gx", "gy", None),
            P("grp", None, None),
            P("gx", "gy", None),
            P("gx", "gy", None),
            P("gx", "gy", None),
            P("gx", "gy", None),
        ),
        out_specs=P("grp", None, "gx", "gy", None),
        check_vma=False,
    )
```
